128 devices in a mesh: data: 1, cp: 128 (over z, y, x, core).
Axes of the slice: x: 4, y: 4, z: 4, core: 2. Of those that a mesh axis runs over, the one named last changes fastest.
Arguments:
- q: bfloat16 [65536, 1, 128], P(('data', 'cp'))
- k: bfloat16 [65536, 1, 128], P(('data', 'cp'))
- v: bfloat16 [65536, 1, 128], P(('data', 'cp'))
- o: bfloat16 [65536, 1, 128], P(('data', 'cp'))
- dout: bfloat16 [65536, 1, 128], P(('data', 'cp'))
- lse: float32 [1, 65536], P(None, ('data', 'cp'))
Outputs:
- output 1: bfloat16 [65536, 1, 128], P(('data', 'cp'))
- output 2: bfloat16 [65536, 1, 128], P(('data', 'cp'))
- output 3: bfloat16 [65536, 1, 128], P(('data', 'cp'))
All inputs are finite; a program needn't handle non-finite values.
Results may differ from the reference program's by a relative error of at most 0.00164.
Values are sent between devices in bfloat16 or wider.
A program may use at most 1 GiB of HBM per device.

```python
import math
import jax
import jax.numpy as jnp
from jax import lax

C = 512
CP = 128
HEADS = 1
HEAD = 128
QB = 128

T = C * CP
SCALE = 1.0 / math.sqrt(HEAD)


def positions():
    r = jnp.arange(T, dtype=jnp.int32)
    return (r % C) * CP + r // C


def _head_forward(q, k, v, pos):
    def blk(b):
        qb = lax.dynamic_slice_in_dim(q, b * QB, QB)
        pb = lax.dynamic_slice_in_dim(pos, b * QB, QB)
        s = jnp.dot(qb, k.T, preferred_element_type=jnp.float32) * SCALE
        s = jnp.where(pos[None, :] <= pb[:, None], s, -jnp.inf)
        mx = jnp.max(s, axis=1, keepdims=True)
        e = jnp.exp(s - mx)
        l = jnp.sum(e, axis=1, keepdims=True)
        o = jnp.dot((e / l).astype(jnp.bfloat16), v, preferred_element_type=jnp.float32)
        return o.astype(jnp.bfloat16), (mx + jnp.log(l))[:, 0]
    o, lse = lax.map(blk, jnp.arange(T // QB))
    return o.reshape(T, HEAD), lse.reshape(T)


def _forward(q, k, v):
    pos = positions()
    o, lse = lax.map(lambda a: _head_forward(a[0], a[1], a[2], pos),
                     (q.transpose(1, 0, 2), k.transpose(1, 0, 2), v.transpose(1, 0, 2)))
    return o.transpose(1, 0, 2), lse


def setup_inputs(seed: int = 0, part: int = 0) -> dict:
    key = jax.random.fold_in(jax.random.PRNGKey(seed), part)
    kq, kk, km, kv, kd = jax.random.split(key, 5)
    shape = (T, HEADS, HEAD)
    q = jax.random.normal(kq, shape, jnp.float32).astype(jnp.bfloat16)
    k = jax.random.normal(kk, shape, jnp.float32).astype(jnp.bfloat16)
    mu = jax.random.normal(km, (1, HEADS, HEAD), jnp.float32)
    v = (0.8 * mu + 0.6 * jax.random.normal(kv, shape, jnp.float32)).astype(jnp.bfloat16)
    o, lse = _forward(q, k, v)
    dout = (0.8 * o.astype(jnp.float32) + 0.6 * jax.random.normal(kd, shape, jnp.float32)).astype(jnp.bfloat16)
    return {'q': q, 'k': k, 'v': v, 'o': o, 'dout': dout, 'lse': lse}


def reference(q, k, v, o, dout, lse):
    pos = positions()
    dd = jnp.sum(dout.astype(jnp.float32) * o.astype(jnp.float32), axis=-1)

    def head(a):
        qh, kh, vh, doh, lh, dh = a

        def step(carry, b):
            dk, dv = carry
            qb = lax.dynamic_slice_in_dim(qh, b * QB, QB)
            dob = lax.dynamic_slice_in_dim(doh, b * QB, QB)
            lb = lax.dynamic_slice_in_dim(lh, b * QB, QB)
            db = lax.dynamic_slice_in_dim(dh, b * QB, QB)
            pb = lax.dynamic_slice_in_dim(pos, b * QB, QB)
            s = jnp.dot(qb, kh.T, preferred_element_type=jnp.float32) * SCALE
            mask = pos[None, :] <= pb[:, None]
            p = jnp.where(mask, jnp.exp(s - lb[:, None]), 0.0)
            dv = dv + jnp.dot(p.astype(jnp.bfloat16).T, dob, preferred_element_type=jnp.float32)
            dp = jnp.dot(dob, vh.T, preferred_element_type=jnp.float32)
            ds = (p * (dp - db[:, None])).astype(jnp.bfloat16)
            dqb = jnp.dot(ds, kh, preferred_element_type=jnp.float32) * SCALE
            dk = dk + jnp.dot(ds.T, qb, preferred_element_type=jnp.float32) * SCALE
            return (dk, dv), dqb

        z = jnp.zeros((T, HEAD), jnp.float32)
        (dk, dv), dq = lax.scan(step, (z, z), jnp.arange(T // QB))
        return dq.reshape(T, HEAD), dk, dv

    dq, dk, dv = lax.map(head, (q.transpose(1, 0, 2), k.transpose(1, 0, 2), v.transpose(1, 0, 2),
                                dout.transpose(1, 0, 2), lse, dd.T))
    return (dq.transpose(1, 0, 2).astype(jnp.bfloat16),
            dk.transpose(1, 0, 2).astype(jnp.bfloat16),
            dv.transpose(1, 0, 2).astype(jnp.bfloat16))
```

```python
import functools
import math

import jax
import jax.numpy as jnp
from jax import lax
from jax.experimental import pallas as pl
from jax.experimental.pallas import tpu as pltpu
from jax.sharding import PartitionSpec as P

F32, BF16 = jnp.float32, jnp.bfloat16
MESH = pl.DeviceIdType.MESH
ROWS, HD = 512, 128
L = 32
NC = ROWS // L
NG, GR = 8, 64
NQ, NK = 16, 8
BQ, BK = NQ * L, NK * L
KQ, KR = 4, 128
SCALE = HD ** -0.5
LOG2E = math.log2(math.e)


def dg(a, b, ca, cb):
    return lax.dot_general(a, b, (((ca,), (cb,)), ((), ())), preferred_element_type=F32)


def kernel(q_ref, k_ref, v_ref, o_ref, do_ref, lse_ref, dq_ref, dk_ref, dv_ref,
           qd, kv, ld, lb, db, thr, kt, vt, qt, dot, p_a, p_b, p_c, ds_a, ds_b, ds_c, dqt, dkt, dvt,
           pq, rb, sa, ra, pk, rd, sz, rz,
           lda_s, lda_r, ldb_s, ldb_r, qa_s, qa_r, qb_s, qb_r, kz_s, kz_r, kd_s, kd_r,
           rb_s, rb_r, ra_s, ra_r, rd_s, rd_r, rz_s, rz_r):
    me = lax.axis_index('cp')
    core = lax.rem(me, 2)
    x = lax.rem(lax.div(me, 2), 4)
    y = lax.rem(lax.div(me, 8), 4)
    z = lax.div(me, 32)
    a = x + core * (y - x)
    b = y + core * (x - y)
    step_a, step_b = 2 + 6 * core, 8 - 6 * core

    def dev_q(b_, a_):
        return z * 32 + b_ * step_b + a_ * step_a + core

    def dev_k(z_, c_):
        return z_ * 32 + y * 8 + x * 2 + c_

    def turn(i, d):
        return lax.rem(i + d, 4)

    def remote(src, dst, ss, rs, dev):
        return pltpu.make_async_remote_copy(src_ref=src, dst_ref=dst, send_sem=ss, recv_sem=rs,
                                            device_id={'cp': dev}, device_id_type=MESH)

    D3 = (1, 2, 3)
    slot = b * 4 + a

    def ld_a(d):
        return remote(ld.at[slot], ld.at[slot], lda_s.at[d - 1], lda_r.at[d - 1], dev_q(b, turn(a, d)))

    def ld_b(d):
        r = ld.at[pl.ds(b * 4, 4)]
        return remote(r, r, ldb_s.at[d - 1], ldb_r.at[d - 1], dev_q(turn(b, d), a))

    def q_a(g, d):
        r = qd.at[slot, :, pl.ds(pl.multiple_of(g * GR, GR), GR), :]
        return remote(r, r, qa_s.at[g, d - 1], qa_r.at[g, d - 1], dev_q(b, turn(a, d)))

    def q_b(g, d):
        r = qd.at[pl.ds(b * 4, 4), :, pl.ds(pl.multiple_of(g * GR, GR), GR), :]
        return remote(r, r, qb_s.at[g, d - 1], qb_r.at[g, d - 1], dev_q(turn(b, d), a))

    def k_z(j, d):
        r = kv.at[core, z, :, pl.ds(pl.multiple_of(j * KR, KR), KR), :]
        return remote(r, r, kz_s.at[j, d - 1], kz_r.at[j, d - 1], dev_k(turn(z, d), core))

    def k_d(j, d):
        r = kv.at[core, turn(z, 4 - d), :, pl.ds(pl.multiple_of(j * KR, KR), KR), :]
        return remote(r, r, kd_s.at[j, d], kd_r.at[j, d], dev_k(z, 1 - core))

    def r_b(g, d):
        return remote(pq.at[g, pl.ds(turn(b, d) * 4, 4)], rb.at[g, d - 1], rb_s.at[g, d - 1], rb_r.at[g, d - 1],
                      dev_q(turn(b, d), a))

    def r_a(g, d):
        return remote(sa.at[g, turn(a, d)], ra.at[g, d - 1], ra_s.at[g, d - 1], ra_r.at[g, d - 1],
                      dev_q(b, turn(a, d)))

    def r_d(g):
        return remote(pk.at[g, 1 - core], rd.at[g], rd_s.at[g], rd_r.at[g], dev_k(z, 1 - core))

    def r_z(g, d):
        return remote(sz.at[g, turn(z, d)], rz.at[g, d - 1], rz_s.at[g, d - 1], rz_r.at[g, d - 1],
                      dev_k(turn(z, d), core))

    qd[slot, 0] = q_ref[...]
    qd[slot, 1] = do_ref[...]
    kv[core, z, 0] = k_ref[...]
    kv[core, z, 1] = v_ref[...]
    for j in range(4):
        rows_j = pl.ds(j * 128, 128)
        d_j = jnp.sum(do_ref[rows_j, :].astype(F32) * o_ref[rows_j, :].astype(F32), axis=1, keepdims=True)
        ld[slot, pl.ds(j, 1), :] = lse_ref[:, rows_j] * LOG2E
        ld[slot, pl.ds(4 + j, 1), :] = jnp.broadcast_to(d_j, (128, 128)).T[:1]

    barrier = pltpu.get_barrier_semaphore()
    peers = [dev_q(b, turn(a, d)) for d in D3] + [dev_q(turn(b, d), a) for d in D3]
    peers += [dev_k(turn(z, d), core) for d in D3] + [dev_k(z, 1 - core)]
    for p in peers:
        pl.semaphore_signal(barrier, inc=1, device_id={'cp': p}, device_id_type=MESH)
    pl.semaphore_wait(barrier, len(peers))

    for d in D3:
        ld_a(d).start()
    for d in D3:
        q_a(NG - 1, d).start()
    for j in range(KQ):
        for d in D3:
            k_z(j, d).start()
        k_d(j, 0).start()

    def start_a(i, _):
        for d in D3:
            q_a(NG - 2 - i, d).start()
        return 0
    lax.fori_loop(0, NG - 1, start_a, 0)

    for d in D3:
        ld_a(d).wait_recv()
    for d in D3:
        ld_b(d).start()

    qi = lax.broadcasted_iota(jnp.int32, (BQ, 1), 0)
    ki = lax.broadcasted_iota(jnp.int32, (1, BK), 1)
    qpos = (qi & (L - 1)) * 128 + dev_q(qi >> 7, (qi >> 5) & 3)
    kpos = (ki & (L - 1)) * 128 + dev_k((ki >> 5) & 3, ki >> 7)
    thr[0] = jnp.full((BQ, BK), jnp.inf, F32)
    thr[1] = jnp.where(kpos <= qpos, jnp.inf, -jnp.inf).astype(F32)
    dkt[...] = jnp.zeros_like(dkt)
    dvt[...] = jnp.zeros_like(dvt)
    dqt[...] = jnp.zeros_like(dqt)

    def pass_a(i, _):
        g = NG - 1 - i
        for d in D3:
            q_a(g, d).wait_recv()
        for d in D3:
            q_b(g, d).start()
        return 0
    lax.fori_loop(0, 2, pass_a, 0)

    for d in D3:
        ld_b(d).wait_recv()

    def prep_l(i, _):
        for j in range(4):
            rows_j = pl.ds(j * 128, 128)
            lb[i, rows_j, :] = jnp.broadcast_to(ld[i, pl.ds(j, 1), :], (128, 128)).T
            db[i, rows_j, :] = jnp.broadcast_to(ld[i, pl.ds(4 + j, 1), :], (128, 128)).T
        return 0

    def pass_k(j, _):
        for d in D3:
            k_z(j, d).wait_recv()
        for d in D3:
            k_d(j, d).start()
        return 0
    lax.fori_loop(0, KQ, pass_k, 0)
    lax.fori_loop(0, NQ, prep_l, 0)
    lax.fori_loop(2, NG, pass_a, 0)

    def rows_q(which, r):
        return qd[:, which, pl.ds(pl.multiple_of(r * L, L), L), :].reshape(BQ, HD)

    def rows_k(which, c):
        return kv[:, :, which, pl.ds(pl.multiple_of(c * L, L), L), :].reshape(BK, HD)

    def rows_f(ref, r):
        return ref[:, pl.ds(pl.multiple_of(r * L, L), L), :].reshape(BQ, HD)

    def prep_k(c, _):
        kt[c] = rows_k(0, c).T
        vt[c] = rows_k(1, c).T
        return 0

    def take_k(j, _):
        for d in (0, 1, 2, 3):
            k_d(j, d).wait_recv()
        lax.fori_loop(j * (KR // L), (j + 1) * (KR // L), prep_k, 0)
        return 0
    lax.fori_loop(0, KQ, take_k, 0)

    def a_mm(r, c):
        return dg(rows_q(0, r), kt[c], 1, 0), dg(rows_q(1, r), vt[c], 1, 0)

    def a_vpu(r, sdp, diag, p_s, ds_s):
        s, dp = sdp
        lbr, dbr = rows_f(lb, r), rows_f(db, r)
        t = s * (SCALE * LOG2E) - jnp.concatenate([lbr, lbr], axis=1)
        p = jnp.exp2(jnp.minimum(t, thr[diag]))
        p_s[...] = p.astype(BF16)
        ds_s[...] = (p * (dp - jnp.concatenate([dbr, dbr], axis=1))).astype(BF16)

    def b_mm(c, h, p_s, ds_s):
        p, ds = p_s[...], ds_s[...]
        dqt[h] += dg(kt[c], ds, 1, 1)
        return dg(dot[h], p, 1, 0), dg(qt[h], ds, 1, 0)

    def q_prep(r, h):
        qt[h] = rows_q(0, r).T
        dot[h] = rows_q(1, r).T

    def finish_q(g, h):
        pq[g, :, pl.ds(h * L, L), :] = dqt[h].T.reshape(NQ, L, HD)
        dqt[h] = jnp.zeros((HD, BQ), F32)

    def finish_k(g, h):
        r = 2 * g + h
        pk[g, :, :, 0, pl.ds(h * L, L), :] = dkt[r].T.reshape(2, 4, L, HD)
        pk[g, :, :, 1, pl.ds(h * L, L), :] = dvt[r].T.reshape(2, 4, L, HD)

    def one(c, r0, d0):
        sdp = a_mm(r0, c + 1)
        dv, dk = b_mm(c, 0, p_a, ds_a)
        a_vpu(r0, sdp, d0, p_a, ds_a)
        sdp = a_mm(r0 + 1, c + 1)
        dv1, dk1 = b_mm(c, 1, p_b, ds_b)
        a_vpu(r0 + 1, sdp, 0, p_b, ds_b)
        dvt[c] += dv + dv1
        dkt[c] += dk + dk1

    def inner(r0):
        def two(j, _):
            c = 2 * j
            one(c, r0, 0)
            one(c + 1, r0, lax.div(c + 2, r0))
            return 0
        lax.fori_loop(0, lax.div(r0, 2), two, 0)

    def tail(g, nxt):
        r0, r1 = 2 * g, 2 * g + 1
        sdp = a_mm(r1, r1)
        dv, dk = b_mm(r0, 0, p_a, ds_a)
        a_vpu(r1, sdp, 1, p_c, ds_c)
        if nxt:
            sdp = a_mm(r0 - 2, 0)
        dv1, dk1 = b_mm(r0, 1, p_b, ds_b)
        if nxt:
            a_vpu(r0 - 2, sdp, lax.div(2, r0), p_a, ds_a)
        dvt[r0] += dv + dv1
        dkt[r0] += dk + dk1
        if nxt:
            sdp = a_mm(r0 - 1, 0)
        dv, dk = b_mm(r1, 1, p_c, ds_c)
        if nxt:
            a_vpu(r0 - 1, sdp, 0, p_b, ds_b)
        dvt[r1] += dv
        dkt[r1] += dk
        finish_q(g, 0)
        finish_k(g, 0)
        finish_q(g, 1)
        finish_k(g, 1)
        if nxt:
            q_prep(r0 - 2, 0)
            q_prep(r0 - 1, 1)

    def rs1(g):
        for d in D3:
            r_b(g, d).start()
        r_d(g).start()

    def rs2(g):
        r_d(g).wait_recv()
        sz[g] = pk[g, core] + rd[g]
        for d in D3:
            r_z(g, d).start()
        for d in D3:
            r_b(g, d).wait_recv()
        sa[g] = pq[g, pl.ds(b * 4, 4)] + rb[g, 0] + rb[g, 1] + rb[g, 2]
        for d in D3:
            r_a(g, d).start()

    def rs3(g):
        for d in D3:
            r_z(g, d).wait_recv()
        rows_g = pl.ds(pl.multiple_of(g * GR, GR), GR)
        dkv = sz[g, z] + rz[g, 0] + rz[g, 1] + rz[g, 2]
        dk_ref[rows_g, :] = (dkv[0] * SCALE).astype(BF16)
        dv_ref[rows_g, :] = dkv[1].astype(BF16)
        for d in D3:
            r_a(g, d).wait_recv()
        dq = sa[g, a] + ra[g, 0] + ra[g, 1] + ra[g, 2]
        dq_ref[rows_g, :] = (dq * SCALE).astype(BF16)

    def take_q(g):
        for d in D3:
            q_b(g, d).wait_recv()

    take_q(NG - 1)
    q_prep(NC - 2, 0)
    q_prep(NC - 1, 1)
    a_vpu(NC - 2, a_mm(NC - 2, 0), 0, p_a, ds_a)
    a_vpu(NC - 1, a_mm(NC - 1, 0), 0, p_b, ds_b)

    def superstep(i, _):
        g = NG - 1 - i
        inner(2 * g)
        take_q(g - 1)
        tail(g, True)
        rs1(g)

        @pl.when(i >= 1)
        def _():
            rs2(g + 1)

        @pl.when(i >= 2)
        def _():
            rs3(g + 2)
        return 0
    lax.fori_loop(0, NG - 1, superstep, 0)
    tail(0, False)
    rs1(0)
    rs2(1)
    rs3(2)
    rs2(0)
    rs3(1)
    rs3(0)

    for d in D3:
        ld_a(d).wait_send()
        ld_b(d).wait_send()

    def sent_k(j, _):
        for d in D3:
            k_z(j, d).wait_send()
        for d in (0, 1, 2, 3):
            k_d(j, d).wait_send()
        return 0
    lax.fori_loop(0, KQ, sent_k, 0)

    def sent(g, _):
        r_d(g).wait_send()
        for d in D3:
            for f in (q_a, q_b, r_b, r_a, r_z):
                f(g, d).wait_send()
        return 0
    lax.fori_loop(0, NG, sent, 0)


def local(q, k, v, o, dout, lse):
    flat = (ROWS, HD)
    vm = pl.BlockSpec(memory_space=pltpu.VMEM)
    V, DMA = pltpu.VMEM, pltpu.SemaphoreType.DMA
    scratch = [
        V((NQ, 2, ROWS, HD), BF16), V((2, 4, 2, ROWS, HD), BF16), V((NQ, 8, 128), F32),
        V((NQ, ROWS, HD), F32), V((NQ, ROWS, HD), F32), V((2, BQ, BK), F32),
        V((NC, HD, BK), BF16), V((NC, HD, BK), BF16), V((2, HD, BQ), BF16), V((2, HD, BQ), BF16),
        *[V((BQ, BK), BF16)] * 6,
        V((2, HD, BQ), F32), V((NC, HD, BK), F32), V((NC, HD, BK), F32),
        V((NG, NQ, GR, HD), F32), V((NG, 3, 4, GR, HD), F32), V((NG, 4, GR, HD), F32), V((NG, 3, GR, HD), F32),
        V((NG, 2, 4, 2, GR, HD), F32), V((NG, 4, 2, GR, HD), F32), V((NG, 4, 2, GR, HD), F32),
        V((NG, 3, 2, GR, HD), F32),
        *[DMA((3,))] * 4, *[DMA((NG, 3))] * 4, *[DMA((KQ, 3))] * 2, *[DMA((KQ, 4))] * 2,
        *[DMA((NG, 3))] * 4, *[DMA((NG,))] * 2, *[DMA((NG, 3))] * 2,
    ]
    outs = pl.pallas_call(
        kernel,
        out_shape=[jax.ShapeDtypeStruct(flat, BF16)] * 3,
        in_specs=[vm] * 6, out_specs=[vm] * 3,
        scratch_shapes=scratch,
        compiler_params=pltpu.CompilerParams(collective_id=0, has_side_effects=True, vmem_limit_bytes=62 << 20),
    )(*[t.reshape(flat) for t in (q, k, v, o, dout)], lse)
    return tuple(t.reshape(ROWS, 1, HD) for t in outs)


def solution(mesh):
    rows = P(('data', 'cp'))
    cols = P(None, ('data', 'cp'))
    return jax.shard_map(local, mesh=mesh, in_specs=(rows, rows, rows, rows, rows, cols),
                         out_specs=(rows, rows, rows), check_vma=False)
```

```python
import functools
import math

import jax
import jax.numpy as jnp
from jax import lax
from jax.experimental import pallas as pl
from jax.experimental.pallas import tpu as pltpu
from jax.sharding import PartitionSpec as P

F32, BF16 = jnp.float32, jnp.bfloat16
MESH = pl.DeviceIdType.MESH
ROWS, HD = 512, 128
L = 32
NC = ROWS // L
NG, GR = 8, 64
NQ, NK = 16, 8
BQ, BK = NQ * L, NK * L
KQ, KR = 4, 128
SCALE = HD ** -0.5
LOG2E = math.log2(math.e)


def dg(a, b, ca, cb):
    return lax.dot_general(a, b, (((ca,), (cb,)), ((), ())), preferred_element_type=F32)


def kernel(q_hbm, k_hbm, v_hbm, o_hbm, do_hbm, lse_hbm, dq_ref, dk_ref, dv_ref,
           qd, kv, ld, ex, thr, kt, vt, qt, dot, p_a, p_b, p_c, ds_a, ds_b, ds_c, dqt, dkt, dvt,
           pq, rb, sa, ra, pk, rd, sz, rz, o_in, lse_in,
           in_s, lda_s, lda_r, ldb_s, ldb_r, qa_s, qa_r, qb_s, qb_r, kz_s, kz_r, kd_s, kd_r,
           rb_s, rb_r, ra_s, ra_r, rd_s, rd_r, rz_s, rz_r):
    me = lax.axis_index('cp')
    core = lax.rem(me, 2)
    x = lax.rem(lax.div(me, 2), 4)
    y = lax.rem(lax.div(me, 8), 4)
    z = lax.div(me, 32)
    a = x + core * (y - x)
    b = y + core * (x - y)
    step_a, step_b = 2 + 6 * core, 8 - 6 * core

    def dev_q(b_, a_):
        return z * 32 + b_ * step_b + a_ * step_a + core

    def dev_k(z_, c_):
        return z_ * 32 + y * 8 + x * 2 + c_

    def turn(i, d):
        return lax.rem(i + d, 4)

    def remote(src, dst, ss, rs, dev):
        return pltpu.make_async_remote_copy(src_ref=src, dst_ref=dst, send_sem=ss, recv_sem=rs,
                                            device_id={'cp': dev}, device_id_type=MESH)

    D3 = (1, 2, 3)
    slot = b * 4 + a

    def rows_g(g):
        return pl.ds(pl.multiple_of(g * GR, GR), GR)

    def ld_a(d):
        return remote(ld.at[slot], ld.at[slot], lda_s.at[d - 1], lda_r.at[d - 1], dev_q(b, turn(a, d)))

    def ld_b(d):
        r = ld.at[pl.ds(b * 4, 4)]
        return remote(r, r, ldb_s.at[d - 1], ldb_r.at[d - 1], dev_q(turn(b, d), a))

    def q_a(g, d):
        r = qd.at[slot, :, rows_g(g), :]
        return remote(r, r, qa_s.at[g, d - 1], qa_r.at[g, d - 1], dev_q(b, turn(a, d)))

    def q_b(g, d):
        r = qd.at[pl.ds(b * 4, 4), :, rows_g(g), :]
        return remote(r, r, qb_s.at[g, d - 1], qb_r.at[g, d - 1], dev_q(turn(b, d), a))

    def q_n(g, n):
        r = qd.at[pl.ds(b * 4, 4), :, rows_g(g), :]
        return remote(r, r, qb_s.at[g, n], qb_r.at[g, n], dev_q(turn(b, 1 + 2 * n), a))

    def q_f(g, n):
        r = qd.at[pl.ds(turn(b, 3 - 2 * n) * 4 + 2 * n, 2), :, rows_g(g), :]
        return remote(r, r, qb_s.at[g, 2 + n], qb_r.at[g, 2 + n], dev_q(turn(b, 1 + 2 * n), a))

    def k_z(j, d):
        r = kv.at[core, z, :, pl.ds(pl.multiple_of(j * KR, KR), KR), :]
        return remote(r, r, kz_s.at[j, d - 1], kz_r.at[j, d - 1], dev_k(turn(z, d), core))

    def k_d(j, d):
        r = kv.at[core, turn(z, 4 - d), :, pl.ds(pl.multiple_of(j * KR, KR), KR), :]
        return remote(r, r, kd_s.at[j, d], kd_r.at[j, d], dev_k(z, 1 - core))

    def r_b(g, d):
        return remote(pq.at[g, pl.ds(turn(b, d) * 4, 4)], rb.at[g, d - 1], rb_s.at[g, d - 1], rb_r.at[g, d - 1],
                      dev_q(turn(b, d), a))

    def r_a(g, d):
        return remote(sa.at[g, turn(a, d)], ra.at[g, d - 1], ra_s.at[g, d - 1], ra_r.at[g, d - 1],
                      dev_q(b, turn(a, d)))

    def r_d(g):
        return remote(pk.at[g, 1 - core], rd.at[g], rd_s.at[g], rd_r.at[g], dev_k(z, 1 - core))

    def r_z(g, d):
        return remote(sz.at[g, turn(z, d)], rz.at[g, d - 1], rz_s.at[g, d - 1], rz_r.at[g, d - 1],
                      dev_k(turn(z, d), core))

    barrier = pltpu.get_barrier_semaphore()
    peers = [dev_q(b, turn(a, d)) for d in D3] + [dev_q(turn(b, d), a) for d in D3]
    peers += [dev_k(turn(z, d), core) for d in D3] + [dev_k(z, 1 - core)]
    for p in peers:
        pl.semaphore_signal(barrier, inc=1, device_id={'cp': p}, device_id_type=MESH)
    ins = [(do_hbm, qd.at[slot, 1]), (o_hbm, o_in), (lse_hbm, lse_in), (q_hbm, qd.at[slot, 0]),
           (k_hbm, kv.at[core, z, 0]), (v_hbm, kv.at[core, z, 1])]
    ins = [pltpu.make_async_copy(src, dst, in_s.at[n]) for n, (src, dst) in enumerate(ins)]
    for c in ins:
        c.start()
    qi = lax.broadcasted_iota(jnp.int32, (BQ, 1), 0)
    ki = lax.broadcasted_iota(jnp.int32, (1, BK), 1)
    qpos = (qi & (L - 1)) * 128 + dev_q(qi >> 7, (qi >> 5) & 3)
    kpos = (ki & (L - 1)) * 128 + dev_k((ki >> 5) & 3, ki >> 7)
    thr[0] = jnp.full((BQ, BK), jnp.inf, F32)
    thr[1] = jnp.where(kpos <= qpos, jnp.inf, -jnp.inf).astype(F32)
    for c in ins:
        c.wait()
    def split(t):
        hi = t.astype(BF16).astype(F32)
        mid = (t - hi).astype(BF16).astype(F32)
        return hi, mid, t - hi - mid

    with jax.named_scope('own_ld'):
        ld[slot] = jnp.zeros((4, 8, 128), F32)
        for j in range(4):
            rows_j = pl.ds(j * 128, 128)
            d_j = jnp.sum(qd[slot, 1, rows_j, :].astype(F32) * o_in[rows_j, :].astype(F32), axis=1, keepdims=True)
            d_j = jnp.broadcast_to(d_j, (128, 128)).T[:1]
            for n, t in enumerate(split(lse_in[:, rows_j] * (-1.0 / SCALE)) + split(-d_j)):
                ld[slot, j, pl.ds(n, 1), :] = t
    with jax.named_scope('barrier'):
        pl.semaphore_wait(barrier, len(peers))

    def start_a(g):
        for d in D3:
            q_a(g, d).start()

    for d in D3:
        ld_a(d).start()
    for d in D3:
        k_z(0, d).start()
    k_d(0, 0).start()
    start_a(7)

    def start_k(j, _):
        for d in D3:
            k_z(j, d).start()
        k_d(j, 0).start()
        return 0
    lax.fori_loop(1, KQ, start_k, 0)
    ex[...] = jnp.zeros_like(ex)
    ri = lax.broadcasted_iota(jnp.int32, (HD, BK), 0)
    for c in range(NC):
        kt[c, HD:] = jnp.where(ri < 3, 1.0, 0.0).astype(BF16)
        vt[c, HD:] = jnp.where((ri >= 3) & (ri < 6), 1.0, 0.0).astype(BF16)
    dkt[...] = jnp.zeros_like(dkt)
    dvt[...] = jnp.zeros_like(dvt)
    dqt[...] = jnp.zeros_like(dqt)

    def got_a(g):
        for d in D3:
            q_a(g, d).wait_recv()

    def prep_e(i, _):
        for n in range(2):
            for j in range(4):
                ex[2 * i + n, pl.ds(j * 128, 128), pl.ds(0, 8)] = ld[2 * i + n, j].T.astype(BF16)
        return 0

    def pass_k(j):
        with jax.named_scope('pass_k'):
            for d in D3:
                k_z(j, d).wait_recv()
        for d in D3:
            k_d(j, d).start()

    with jax.named_scope('w_lda'):
        for d in D3:
            ld_a(d).wait_recv()
    for d in D3:
        ld_b(d).start()
    with jax.named_scope('got_a7'):
        got_a(7)
    for d in D3:
        q_b(7, d).start()
    start_a(6)
    start_a(5)
    pass_k(0)
    with jax.named_scope('w_ldb'):
        for d in D3:
            ld_b(d).wait_recv()
    with jax.named_scope('prep_e'):
        lax.fori_loop(0, NQ // 2, prep_e, 0)
    start_a(0)
    start_a(4)

    def rows_q(which, r):
        return qd[:, which, pl.ds(pl.multiple_of(r * L, L), L), :].reshape(BQ, HD)

    def rows_k(which, c):
        return kv[:, :, which, pl.ds(pl.multiple_of(c * L, L), L), :].reshape(BK, HD)

    def rows_e(r):
        return ex[:, pl.ds(pl.multiple_of(r * L, L), L), :].reshape(BQ, HD)

    def prep_k(c, _):
        kt[c, :HD] = rows_k(0, c).T
        vt[c, :HD] = rows_k(1, c).T
        return 0

    def take_k(j):
        with jax.named_scope('take_k'):
            for d in (0, 1, 2, 3):
                k_d(j, d).wait_recv()
        lax.fori_loop(j * (KR // L), (j + 1) * (KR // L), prep_k, 0)

    def a_mm(r, c):
        e = rows_e(r)
        return (dg(jnp.concatenate([rows_q(0, r), e], axis=1), kt[c], 1, 0),
                dg(jnp.concatenate([rows_q(1, r), e], axis=1), vt[c], 1, 0))

    def a_vpu(sdp, diag, p_s, ds_s):
        s, dp = sdp
        t = s * (SCALE * LOG2E)
        if diag is not None:
            t = jnp.minimum(t, thr[diag])
        p = jnp.exp2(t)
        p_s[...] = p.astype(BF16)
        ds_s[...] = (p * dp).astype(BF16)

    def b_mm(c, h, p_s, ds_s):
        p, ds = p_s[...], ds_s[...]
        dqt[h] += dg(kt[c, :HD], ds, 1, 1)
        return dg(dot[h], p, 1, 0), dg(qt[h], ds, 1, 0)

    def q_prep(r, h):
        qt[h] = rows_q(0, r).T
        dot[h] = rows_q(1, r).T

    def finish_q(g, h):
        pq[g, :, pl.ds(h * L, L), :] = dqt[h].T.reshape(NQ, L, HD)
        dqt[h] = jnp.zeros((HD, BQ), F32)

    def finish_k(g, h):
        r = 2 * g + h
        pk[g, :, :, 0, pl.ds(h * L, L), :] = dkt[r].T.reshape(2, 4, L, HD)
        pk[g, :, :, 1, pl.ds(h * L, L), :] = dvt[r].T.reshape(2, 4, L, HD)

    def one(c, r0, d0):
        sdp = a_mm(r0, c + 1)
        dv, dk = b_mm(c, 0, p_a, ds_a)
        a_vpu(sdp, d0, p_a, ds_a)
        sdp = a_mm(r0 + 1, c + 1)
        dv1, dk1 = b_mm(c, 1, p_b, ds_b)
        a_vpu(sdp, None, p_b, ds_b)
        dvt[c] += dv + dv1
        dkt[c] += dk + dk1

    def two(c, r0):
        one(c, r0, None)
        one(c + 1, r0, lax.div(c + 2, r0))

    def tail(g, nxt=None):
        r0, r1 = 2 * g, 2 * g + 1
        sdp = a_mm(r1, r1)
        dv, dk = b_mm(r0, 0, p_a, ds_a)
        a_vpu(sdp, 1, p_c, ds_c)
        if nxt is not None:
            sdp = a_mm(2 * nxt, 0)
        dv1, dk1 = b_mm(r0, 1, p_b, ds_b)
        if nxt is not None:
            a_vpu(sdp, lax.div(7 - nxt, 7), p_a, ds_a)
        dvt[r0] += dv + dv1
        dkt[r0] += dk + dk1
        if nxt is not None:
            sdp = a_mm(2 * nxt + 1, 0)
        dv, dk = b_mm(r1, 1, p_c, ds_c)
        if nxt is not None:
            a_vpu(sdp, None, p_b, ds_b)
        dvt[r1] += dv
        dkt[r1] += dk
        finish_q(g, 0)
        finish_k(g, 0)
        finish_q(g, 1)
        finish_k(g, 1)
        if nxt is not None:
            q_prep(2 * nxt, 0)
            q_prep(2 * nxt + 1, 1)

    def send_q(g):
        for d in D3:
            r_b(g, d).start()

    def send_k(g):
        r_d(g).start()

    def mid_q(g):
        with jax.named_scope('mid_q'):
            for d in D3:
                r_b(g, d).wait_recv()
            sa[g] = pq[g, pl.ds(b * 4, 4)] + rb[g, 0] + rb[g, 1] + rb[g, 2]
        for d in D3:
            r_a(g, d).start()

    def mid_k(g):
        with jax.named_scope('mid_k'):
            r_d(g).wait_recv()
            sz[g] = pk[g, core] + rd[g]
        for d in D3:
            r_z(g, d).start()

    def end_q(g):
        with jax.named_scope('end_q'):
            for d in D3:
                r_a(g, d).wait_recv()
            dq = sa[g, a] + ra[g, 0] + ra[g, 1] + ra[g, 2]
            dq_ref[rows_g(g), :] = (dq * SCALE).astype(BF16)

    def end_k(g):
        with jax.named_scope('end_k'):
            for d in D3:
                r_z(g, d).wait_recv()
            dkv = sz[g, z] + rz[g, 0] + rz[g, 1] + rz[g, 2]
            dk_ref[rows_g(g), :] = (dkv[0] * SCALE).astype(BF16)
            dv_ref[rows_g(g), :] = dkv[1].astype(BF16)

    def pass_q(g):
        with jax.named_scope('pass_q'):
            for n in (0, 1):
                q_n(g, n).wait_recv()
        for n in (0, 1):
            q_f(g, n).start()

    def next_q(g):
        with jax.named_scope('next_q'):
            got_a(g)
        for n in (0, 1):
            q_n(g, n).start()

    take_k(0)
    with jax.named_scope('first_q'):
        for d in D3:
            q_b(7, d).wait_recv()
    q_prep(14, 0)
    q_prep(15, 1)
    with jax.named_scope('first'):
        a_vpu(a_mm(14, 0), None, p_a, ds_a)
        a_vpu(a_mm(15, 0), None, p_b, ds_b)
    next_q(6)
    for g in (3, 2, 1):
        start_a(g)
    pass_k(1)

    def group(i):
        late = lax.div(i + 4, 8)
        return 7 - i + late - 4 * (lax.div(i + 5, 8) - late)

    def at(events, j):
        for when, act in events.items():
            pl.when(j == when)(act)

    def runs(*acts):
        def run():
            for f, arg in acts:
                f(arg)
        return run

    ahead = {
        0: {1: runs((take_k, 1), (next_q, 5)), 2: runs((pass_k, 2), (next_q, 0)), 3: runs((take_k, 2), (next_q, 4)),
            4: runs((pass_k, 3), (pass_q, 6), (next_q, 3)), 5: runs((take_k, 3), (pass_q, 5), (next_q, 2)),
            6: runs((pass_q, 0), (next_q, 1))},
        1: {1: runs((pass_q, 3)), 2: runs((mid_k, 7), (pass_q, 2)), 3: runs((pass_q, 1))},
        2: {2: runs((mid_k, 6)), 3: runs((end_k, 7))},
        4: {1: runs((mid_k, 5), (end_k, 6)), 2: runs((end_q, 6))},
        5: {2: runs((mid_k, 4), (end_k, 5))},
        6: {1: runs((mid_k, 3), (mid_q, 4), (end_k, 4))},
    }
    behind = {
        0: runs((pass_q, 4)),
        1: runs((mid_q, 7)),
        2: runs((mid_q, 6), (end_q, 7)),
        4: runs((mid_q, 5), (mid_q, 0)),
        5: runs((end_q, 5), (end_q, 0)),
    }

    def superstep(i, _):
        g = group(i)
        g1 = group(i + 1)

        def pair(j, _):
            for when, events in ahead.items():
                pl.when(i == when)(functools.partial(at, events, j))
            with jax.named_scope('two'):
                two(2 * j, 2 * g)
            return 0
        lax.fori_loop(0, g, pair, 0)
        with jax.named_scope('take_q'):
            for n in (0, 1):
                q_f(g1, n).wait_recv()
        with jax.named_scope('tail'):
            tail(g, g1)
        send_q(g)
        pl.when(i != 3)(functools.partial(send_k, g))
        for when, act in behind.items():
            pl.when(i == when)(act)
        return 0
    lax.fori_loop(0, NG - 1, superstep, 0)

    with jax.named_scope('two'):
        two(0, 2)
    finish_k(0, 0)
    finish_k(0, 1)
    send_k(0)
    mid_k(2)
    with jax.named_scope('tail'):
        tail(1)
    send_q(1)
    send_k(1)
    mid_k(0)
    mid_q(3)
    mid_k(1)
    end_k(3)
    end_q(4)
    mid_q(2)
    mid_q(1)
    end_k(2)
    end_k(0)
    end_q(3)
    end_k(1)
    end_q(2)
    end_q(1)

    for d in D3:
        ld_a(d).wait_send()
        ld_b(d).wait_send()
        q_b(7, d).wait_send()

    def sent_f(g, _):
        for n in (0, 1):
            q_n(g, n).wait_send()
            q_f(g, n).wait_send()
        return 0
    lax.fori_loop(0, 7, sent_f, 0)

    def sent_k(j, _):
        for d in D3:
            k_z(j, d).wait_send()
        for d in (0, 1, 2, 3):
            k_d(j, d).wait_send()
        return 0
    lax.fori_loop(0, KQ, sent_k, 0)

    def sent(g, _):
        r_d(g).wait_send()
        for d in D3:
            for f in (q_a, r_b, r_a, r_z):
                f(g, d).wait_send()
        return 0
    lax.fori_loop(0, NG, sent, 0)


def local(q, k, v, o, dout, lse):
    flat = (ROWS, HD)
    vm = pl.BlockSpec(memory_space=pltpu.VMEM)
    V, DMA = pltpu.VMEM, pltpu.SemaphoreType.DMA
    scratch = [
        V((NQ, 2, ROWS, HD), BF16), V((2, 4, 2, ROWS, HD), BF16), V((NQ, 4, 8, 128), F32),
        V((NQ, ROWS, HD), BF16), V((2, BQ, BK), F32),
        V((NC, 2 * HD, BK), BF16), V((NC, 2 * HD, BK), BF16), V((2, HD, BQ), BF16), V((2, HD, BQ), BF16),
        *[V((BQ, BK), BF16)] * 6,
        V((2, HD, BQ), F32), V((NC, HD, BK), F32), V((NC, HD, BK), F32),
        V((NG, NQ, GR, HD), F32), V((NG, 3, 4, GR, HD), F32), V((NG, 4, GR, HD), F32), V((NG, 3, GR, HD), F32),
        V((NG, 2, 4, 2, GR, HD), F32), V((NG, 4, 2, GR, HD), F32), V((NG, 4, 2, GR, HD), F32),
        V((NG, 3, 2, GR, HD), F32), V((ROWS, HD), BF16), V((1, ROWS), F32),
        DMA((6,)),
        *[DMA((3,))] * 4, *[DMA((NG, 3))] * 2, *[DMA((NG, 4))] * 2, *[DMA((KQ, 3))] * 2, *[DMA((KQ, 4))] * 2,
        *[DMA((NG, 3))] * 4, *[DMA((NG,))] * 2, *[DMA((NG, 3))] * 2,
    ]
    outs = pl.pallas_call(
        kernel,
        out_shape=[jax.ShapeDtypeStruct(flat, BF16)] * 3,
        in_specs=[pl.BlockSpec(memory_space=pl.ANY)] * 6, out_specs=[vm] * 3,
        scratch_shapes=scratch,
        compiler_params=pltpu.CompilerParams(collective_id=0, has_side_effects=True, vmem_limit_bytes=62 << 20),
    )(*[t.reshape(flat) for t in (q, k, v, o, dout)], lse)
    return tuple(t.reshape(ROWS, 1, HD) for t in outs)


def solution(mesh):
    rows = P(('data', 'cp'))
    cols = P(None, ('data', 'cp'))
    return jax.shard_map(local, mesh=mesh, in_specs=(rows, rows, rows, rows, rows, cols),
                         out_specs=(rows, rows, rows), check_vma=False)
```

```python
import functools
import math

import jax
import jax.numpy as jnp
from jax import lax
from jax.experimental import pallas as pl
from jax.experimental.pallas import tpu as pltpu
from jax.sharding import PartitionSpec as P

F32, BF16 = jnp.float32, jnp.bfloat16
MESH = pl.DeviceIdType.MESH
ROWS, HD = 512, 128
L = 32
NC = ROWS // L
NG, GR = 8, 64
NQ, NK = 16, 8
BQ, BK = NQ * L, NK * L
KQ, KR = 4, 128
SCALE = HD ** -0.5
LOG2E = math.log2(math.e)


def dg(a, b, ca, cb):
    return lax.dot_general(a, b, (((ca,), (cb,)), ((), ())), preferred_element_type=F32)


def kernel(q_hbm, k_hbm, v_hbm, o_hbm, do_hbm, lse_hbm, dq_ref, dk_ref, dv_ref,
           qd, kv, ld, ex, thr, kt, vt, qt, dot, p_a, p_b, p_c, ds_a, ds_b, ds_c, dqt, dkt, dvt,
           pq, rb, sa, ra, pk, rd, sz, rz, o_in, lse_in,
           in_s, ld_s, qa_s, qb_s, kz_s, kd_s, rb_s, ra_s, rd_s, rz_s,
           lda_r, ldb_r, qa_r, q7_r, qn_r, qf_r, kz_r, kd_r, rb_r, ra_r, rd_r, rz_r):
    me = lax.axis_index('cp')
    core = lax.rem(me, 2)
    x = lax.rem(lax.div(me, 2), 4)
    y = lax.rem(lax.div(me, 8), 4)
    z = lax.div(me, 32)
    a = x + core * (y - x)
    b = y + core * (x - y)
    step_a, step_b = 2 + 6 * core, 8 - 6 * core

    def dev_q(b_, a_):
        return z * 32 + b_ * step_b + a_ * step_a + core

    def dev_k(z_, c_):
        return z_ * 32 + y * 8 + x * 2 + c_

    def turn(i, d):
        return lax.rem(i + d, 4)

    def remote(src, dst, ss, rs, dev):
        return pltpu.make_async_remote_copy(src_ref=src, dst_ref=dst, send_sem=ss, recv_sem=rs,
                                            device_id={'cp': dev}, device_id_type=MESH)

    D3 = (1, 2, 3)
    slot = b * 4 + a

    def rows_g(g):
        return pl.ds(pl.multiple_of(g * GR, GR), GR)

    def got(ref, sem):
        pltpu.make_async_copy(ref, ref, sem).wait()

    def own_a(src, ss, rs, d):
        return remote(src, src, ss, rs, dev_q(b, turn(a, d)))

    def to_b(src, ss, rs, d):
        return remote(src, src, ss, rs, dev_q(turn(b, d), a))

    def q_blk(n, g):
        return qd.at[b * 4 + turn(a, n), :, rows_g(g), :]

    def q_row(b_, g, n=0, size=4):
        return qd.at[pl.ds(b_ * 4 + n, size), :, rows_g(g), :]

    def q_n(g, n):
        return to_b(q_row(b, g), qb_s.at[0], qn_r.at[g], 1 + 2 * n)

    def q_f(g, n):
        return to_b(q_row(turn(b, 3 - 2 * n), g, 2 * n, 2), qb_s.at[0], qf_r.at[g], 1 + 2 * n)

    def k_z(j, d):
        r = kv.at[core, z, :, pl.ds(pl.multiple_of(j * KR, KR), KR), :]
        return remote(r, r, kz_s.at[0], kz_r.at[j], dev_k(turn(z, d), core))

    def k_d(j, d):
        r = kv.at[core, turn(z, 4 - d), :, pl.ds(pl.multiple_of(j * KR, KR), KR), :]
        return remote(r, r, kd_s.at[0], kd_r.at[j], dev_k(z, 1 - core))

    def r_b(g, d):
        return remote(pq.at[g, pl.ds(turn(b, d) * 4, 4)], rb.at[g, d - 1], rb_s.at[0], rb_r.at[g], dev_q(turn(b, d), a))

    def r_a(g, d):
        return remote(sa.at[g, turn(a, d)], ra.at[g, d - 1], ra_s.at[0], ra_r.at[g], dev_q(b, turn(a, d)))

    def r_d(g):
        return remote(pk.at[g, 1 - core], rd.at[g], rd_s.at[0], rd_r.at[g], dev_k(z, 1 - core))

    def r_z(g, d):
        return remote(sz.at[g, turn(z, d)], rz.at[g, d - 1], rz_s.at[0], rz_r.at[g], dev_k(turn(z, d), core))

    barrier = pltpu.get_barrier_semaphore()
    peers = [dev_q(b, turn(a, d)) for d in D3] + [dev_q(turn(b, d), a) for d in D3]
    peers += [dev_k(turn(z, d), core) for d in D3] + [dev_k(z, 1 - core)]
    for p in peers:
        pl.semaphore_signal(barrier, inc=1, device_id={'cp': p}, device_id_type=MESH)
    ins = [(do_hbm, qd.at[slot, 1], 0), (q_hbm, qd.at[slot, 0], 0), (k_hbm, kv.at[core, z, 0], 1),
           (v_hbm, kv.at[core, z, 1], 1), (o_hbm, o_in, 2), (lse_hbm, lse_in, 3)]
    for src, dst, n in ins:
        pltpu.make_async_copy(src, dst, in_s.at[n]).start()
    ld[slot] = jnp.zeros((4, 8, 128), F32)
    for ref, n in ((qd.at[slot], 0), (kv.at[core, z], 1), (o_in, 2), (lse_in, 3)):
        got(ref, in_s.at[n])

    def split(t):
        hi = t.astype(BF16).astype(F32)
        mid = (t - hi).astype(BF16).astype(F32)
        return hi, mid, t - hi - mid

    with jax.named_scope('own_ld'):
        for j in range(4):
            rows_j = pl.ds(j * 128, 128)
            d_j = jnp.sum(qd[slot, 1, rows_j, :].astype(F32) * o_in[rows_j, :].astype(F32), axis=1, keepdims=True)
            d_j = jnp.broadcast_to(d_j, (128, 128)).T[:1]
            for n, t in enumerate(split(lse_in[:, rows_j] * (-1.0 / SCALE)) + split(-d_j)):
                ld[slot, j, pl.ds(n, 1), :] = t
    with jax.named_scope('barrier'):
        pl.semaphore_wait(barrier, len(peers))

    def start_a(g):
        for d in D3:
            own_a(q_blk(0, g), qa_s.at[0], qa_r.at[g], d).start()

    for d in D3:
        own_a(ld.at[slot], ld_s.at[0], lda_r.at[0], d).start()
    for d in D3:
        k_z(0, d).start()
    k_d(0, 0).start()
    start_a(7)
    for d in D3:
        to_b(ld.at[slot], ld_s.at[0], ldb_r.at[0], d).start()
    for d in D3:
        to_b(q_blk(0, 7), qb_s.at[0], q7_r.at[0], d).start()

    def start_k(j, _):
        for d in D3:
            k_z(j, d).start()
        k_d(j, 0).start()
        return 0
    lax.fori_loop(1, KQ, start_k, 0)
    qi = lax.broadcasted_iota(jnp.int32, (BQ, 1), 0)
    ki = lax.broadcasted_iota(jnp.int32, (1, BK), 1)
    qpos = (qi & (L - 1)) * 128 + dev_q(qi >> 7, (qi >> 5) & 3)
    kpos = (ki & (L - 1)) * 128 + dev_k((ki >> 5) & 3, ki >> 7)
    thr[0] = jnp.full((BQ, BK), jnp.inf, F32)
    thr[1] = jnp.where(kpos <= qpos, jnp.inf, -jnp.inf).astype(F32)
    ex[...] = jnp.zeros_like(ex)
    ri = lax.broadcasted_iota(jnp.int32, (HD, BK), 0)
    for c in range(NC):
        kt[c, HD:] = jnp.where(ri < 3, 1.0, 0.0).astype(BF16)
        vt[c, HD:] = jnp.where((ri >= 3) & (ri < 6), 1.0, 0.0).astype(BF16)
    def got_a(g):
        got(qd.at[pl.ds(0, 3), :, rows_g(g), :], qa_r.at[g])

    def prep_e(i, _):
        for n in range(4):
            for j in range(4):
                ex[4 * i + n, pl.ds(j * 128, 128), pl.ds(0, 8)] = ld[4 * i + n, j].T.astype(BF16)
        return 0

    def pass_k(j):
        with jax.named_scope('pass_k'):
            got(kv.at[0, pl.ds(0, 3), :, pl.ds(0, KR), :], kz_r.at[j])
        for d in D3:
            k_d(j, d).start()

    with jax.named_scope('w_lda'):
        got(ld.at[pl.ds(0, 3)], lda_r.at[0])
    for n in D3:
        for d in D3:
            to_b(ld.at[b * 4 + turn(a, n)], ld_s.at[0], ldb_r.at[0], d).start()
    with jax.named_scope('got_a7'):
        got_a(7)
    for n in D3:
        for d in D3:
            to_b(q_blk(n, 7), qb_s.at[0], q7_r.at[0], d).start()
    dkt[...] = jnp.zeros_like(dkt)
    dvt[...] = jnp.zeros_like(dvt)
    dqt[...] = jnp.zeros_like(dqt)
    pass_k(0)
    with jax.named_scope('w_ldb'):
        got(ld.at[pl.ds(0, 12)], ldb_r.at[0])
    start_a(6)
    with jax.named_scope('prep_e'):
        lax.fori_loop(0, NQ // 4, prep_e, 0)
    start_a(5)

    def rows_q(which, r):
        return qd[:, which, pl.ds(pl.multiple_of(r * L, L), L), :].reshape(BQ, HD)

    def rows_k(which, c):
        return kv[:, :, which, pl.ds(pl.multiple_of(c * L, L), L), :].reshape(BK, HD)

    def rows_e(r):
        return ex[:, pl.ds(pl.multiple_of(r * L, L), L), :].reshape(BQ, HD)

    def take_k(j):
        with jax.named_scope('take_k'):
            got(kv.at[0, :, :, pl.ds(0, KR), :], kd_r.at[j])
        with jax.named_scope('prep_k'):
            for n in range(KR // L):
                c = j * (KR // L) + n
                kt[c, :HD] = rows_k(0, c).T
                vt[c, :HD] = rows_k(1, c).T

    def a_mm(r, c):
        e = rows_e(r)
        return (dg(jnp.concatenate([rows_q(0, r), e], axis=1), kt[c], 1, 0),
                dg(jnp.concatenate([rows_q(1, r), e], axis=1), vt[c], 1, 0))

    def a_vpu(sdp, diag, p_s, ds_s):
        s, dp = sdp
        t = s * (SCALE * LOG2E)
        if diag is not None:
            t = jnp.minimum(t, thr[diag])
        p = jnp.exp2(t)
        p_s[...] = p.astype(BF16)
        ds_s[...] = (p * dp).astype(BF16)

    def b_mm(c, h, p_s, ds_s):
        p, ds = p_s[...], ds_s[...]
        dqt[h] += dg(kt[c, :HD], ds, 1, 1)
        return dg(dot[h], p, 1, 0), dg(qt[h], ds, 1, 0)

    def q_prep(r, h):
        qt[h] = rows_q(0, r).T
        dot[h] = rows_q(1, r).T

    def finish_q(g, h):
        pq[g, :, pl.ds(h * L, L), :] = dqt[h].T.reshape(NQ, L, HD)
        dqt[h] = jnp.zeros((HD, BQ), F32)

    def finish_k(g, h):
        r = 2 * g + h
        pk[g, :, :, 0, pl.ds(h * L, L), :] = dkt[r].T.reshape(2, 4, L, HD)
        pk[g, :, :, 1, pl.ds(h * L, L), :] = dvt[r].T.reshape(2, 4, L, HD)

    def one(c, r0, d0):
        sdp = a_mm(r0, c + 1)
        dv, dk = b_mm(c, 0, p_a, ds_a)
        a_vpu(sdp, d0, p_a, ds_a)
        sdp = a_mm(r0 + 1, c + 1)
        dv1, dk1 = b_mm(c, 1, p_b, ds_b)
        a_vpu(sdp, None, p_b, ds_b)
        dvt[c] += dv + dv1
        dkt[c] += dk + dk1

    def two(c, r0):
        one(c, r0, None)
        one(c + 1, r0, lax.div(c + 2, r0))

    def tail(g, nxt=None):
        r0, r1 = 2 * g, 2 * g + 1
        sdp = a_mm(r1, r1)
        dv, dk = b_mm(r0, 0, p_a, ds_a)
        a_vpu(sdp, 1, p_c, ds_c)
        if nxt is not None:
            sdp = a_mm(2 * nxt, 0)
        dv1, dk1 = b_mm(r0, 1, p_b, ds_b)
        if nxt is not None:
            a_vpu(sdp, lax.div(7 - nxt, 7), p_a, ds_a)
        dvt[r0] += dv + dv1
        dkt[r0] += dk + dk1
        if nxt is not None:
            sdp = a_mm(2 * nxt + 1, 0)
        dv, dk = b_mm(r1, 1, p_c, ds_c)
        if nxt is not None:
            a_vpu(sdp, None, p_b, ds_b)
        dvt[r1] += dv
        dkt[r1] += dk
        finish_q(g, 0)
        finish_k(g, 0)
        finish_q(g, 1)
        finish_k(g, 1)
        if nxt is not None:
            q_prep(2 * nxt, 0)
            q_prep(2 * nxt + 1, 1)

    def send_q(g):
        for d in D3:
            r_b(g, d).start()

    def send_k(g):
        r_d(g).start()

    def mid_q(g):
        with jax.named_scope('mid_q'):
            got(rb.at[g], rb_r.at[g])
            sa[g] = pq[g, pl.ds(b * 4, 4)] + rb[g, 0] + rb[g, 1] + rb[g, 2]
        for d in D3:
            r_a(g, d).start()

    def mid_k(g):
        with jax.named_scope('mid_k'):
            got(rd.at[g], rd_r.at[g])
            sz[g] = pk[g, core] + rd[g]
        for d in D3:
            r_z(g, d).start()

    def end_q(g):
        with jax.named_scope('end_q'):
            got(ra.at[g], ra_r.at[g])
            dq = sa[g, a] + ra[g, 0] + ra[g, 1] + ra[g, 2]
            dq_ref[rows_g(g), :] = (dq * SCALE).astype(BF16)

    def end_k(g):
        with jax.named_scope('end_k'):
            got(rz.at[g], rz_r.at[g])
            dkv = sz[g, z] + rz[g, 0] + rz[g, 1] + rz[g, 2]
            dk_ref[rows_g(g), :] = (dkv[0] * SCALE).astype(BF16)
            dv_ref[rows_g(g), :] = dkv[1].astype(BF16)

    def pass_q(g):
        with jax.named_scope('pass_q'):
            got(q_row(0, g, 0, 8), qn_r.at[g])
        for n in (0, 1):
            q_f(g, n).start()

    def next_q(g):
        with jax.named_scope('next_q'):
            got_a(g)
        for n in (0, 1):
            q_n(g, n).start()

    take_k(0)
    with jax.named_scope('first_q'):
        got(q_row(0, 7, 0, 12), q7_r.at[0])
    q_prep(14, 0)
    q_prep(15, 1)
    with jax.named_scope('first'):
        a_vpu(a_mm(14, 0), None, p_a, ds_a)
        a_vpu(a_mm(15, 0), None, p_b, ds_b)
    next_q(6)
    for g in (0, 4, 3, 2, 1):
        start_a(g)
    pass_k(1)

    def group(i):
        late = lax.div(i + 4, 8)
        return 7 - i + late - 4 * (lax.div(i + 5, 8) - late)

    def at(events, j):
        for when, act in events.items():
            pl.when(j == when)(act)

    def runs(*acts):
        def run():
            for f, arg in acts:
                f(arg)
        return run

    ahead = {
        0: {1: runs((take_k, 1), (next_q, 5)), 2: runs((pass_k, 2), (next_q, 0)), 3: runs((take_k, 2), (next_q, 4)),
            4: runs((pass_k, 3), (pass_q, 6), (next_q, 3)), 5: runs((take_k, 3), (pass_q, 5), (next_q, 2)),
            6: runs((pass_q, 0), (next_q, 1))},
        1: {1: runs((pass_q, 3)), 2: runs((mid_k, 7), (pass_q, 2)), 3: runs((pass_q, 1))},
        2: {2: runs((mid_k, 6))},
        4: {1: runs((mid_k, 5))},
        5: {1: runs((mid_k, 4), (mid_q, 0))},
        6: {1: runs((mid_k, 3))},
    }
    behind = {
        0: runs((pass_q, 4)),
        1: runs((mid_q, 7)),
        2: runs((mid_q, 6)),
        4: runs((mid_q, 5)),
        6: runs((mid_q, 4)),
    }

    def superstep(i, _):
        g = group(i)
        g1 = group(i + 1)

        def pair(j, _):
            def at_some(whens):
                for when in whens:
                    pl.when(i == when)(functools.partial(at, ahead[when], j))
            pl.when(i < 2)(functools.partial(at_some, (0, 1)))
            pl.when(i >= 2)(functools.partial(at_some, (2, 4, 5, 6)))
            with jax.named_scope('two'):
                two(2 * j, 2 * g)
            return 0
        lax.fori_loop(0, g, pair, 0)
        with jax.named_scope('take_q'):
            got(q_row(0, g1), qf_r.at[g1])
        with jax.named_scope('tail'):
            tail(g, g1)
        send_q(g)
        pl.when(i != 3)(functools.partial(send_k, g))
        for when, act in behind.items():
            pl.when(i == when)(act)
        return 0
    lax.fori_loop(0, NG - 1, superstep, 0)

    with jax.named_scope('two'):
        two(0, 2)
    finish_k(0, 0)
    finish_k(0, 1)
    send_k(0)
    mid_k(2)
    with jax.named_scope('tail'):
        tail(1)
    send_q(1)
    send_k(1)
    mid_k(0)
    mid_q(3)
    mid_k(1)
    for g in (7, 6, 5):
        end_k(g)
        end_q(g)
    end_q(0)
    mid_q(2)
    end_k(4)
    end_q(4)
    mid_q(1)
    end_k(3)
    end_k(2)
    end_q(3)
    end_k(0)
    end_k(1)
    end_q(2)
    end_q(1)

    got(ld.at[pl.ds(0, 15)], ld_s.at[0])
    got(qd.at[pl.ds(0, 3)], qa_s.at[0])
    got(qd.at[pl.ds(0, 12)], qb_s.at[0])
    got(kv.at[0, pl.ds(0, 3)], kz_s.at[0])
    got(kv.at[0], kd_s.at[0])
    got(pq.at[pl.ds(0, 6)], rb_s.at[0])
    got(sa.at[pl.ds(0, 6)], ra_s.at[0])
    got(rd, rd_s.at[0])
    got(rz, rz_s.at[0])


def put(*refs):
    sem = refs[6]
    copies = [pltpu.make_async_copy(refs[n], refs[3 + n], sem.at[n]) for n in range(3)]
    for c in copies:
        c.start()
    for c in copies:
        c.wait()


def local(q, k, v, o, dout, lse):
    flat = (ROWS, HD)
    vm = pl.BlockSpec(memory_space=pltpu.VMEM)
    V, DMA = pltpu.VMEM, pltpu.SemaphoreType.DMA
    scratch = [
        V((NQ, 2, ROWS, HD), BF16), V((2, 4, 2, ROWS, HD), BF16), V((NQ, 4, 8, 128), F32),
        V((NQ, ROWS, HD), BF16), V((2, BQ, BK), F32),
        V((NC, 2 * HD, BK), BF16), V((NC, 2 * HD, BK), BF16), V((2, HD, BQ), BF16), V((2, HD, BQ), BF16),
        *[V((BQ, BK), BF16)] * 6,
        V((2, HD, BQ), F32), V((NC, HD, BK), F32), V((NC, HD, BK), F32),
        V((NG, NQ, GR, HD), F32), V((NG, 3, 4, GR, HD), F32), V((NG, 4, GR, HD), F32), V((NG, 3, GR, HD), F32),
        V((NG, 2, 4, 2, GR, HD), F32), V((NG, 4, 2, GR, HD), F32), V((NG, 4, 2, GR, HD), F32),
        V((NG, 3, 2, GR, HD), F32), V((ROWS, HD), BF16), V((1, ROWS), F32),
        DMA((4,)), *[DMA((1,))] * 9,
        DMA((1,)), DMA((1,)), DMA((NG,)), DMA((1,)), DMA((NG,)), DMA((NG,)), DMA((KQ,)), DMA((KQ,)), *[DMA((NG,))] * 4,
    ]
    outs = pl.pallas_call(
        kernel,
        out_shape=[pltpu.VMEM(flat, BF16)] * 3,
        in_specs=[pl.BlockSpec(memory_space=pl.ANY)] * 6, out_specs=[vm] * 3,
        scratch_shapes=scratch,
        compiler_params=pltpu.CompilerParams(collective_id=0, has_side_effects=True, vmem_limit_bytes=62 << 20),
    )(*[t.reshape(flat) for t in (q, k, v, o, dout)], lse)
    outs = pl.pallas_call(
        put,
        out_shape=[jax.ShapeDtypeStruct(flat, BF16)] * 3,
        in_specs=[vm] * 3, out_specs=[pl.BlockSpec(memory_space=pl.ANY)] * 3,
        scratch_shapes=[DMA((3,))],
    )(*[pltpu.with_memory_space_constraint(t, pltpu.VMEM) for t in outs])
    return tuple(t.reshape(ROWS, 1, HD) for t in outs)


def solution(mesh):
    rows = P(('data', 'cp'))
    cols = P(None, ('data', 'cp'))
    return jax.shard_map(local, mesh=mesh, in_specs=(rows, rows, rows, rows, rows, cols),
                         out_specs=(rows, rows, rows), check_vma=False)
```

```python
import functools
import math

import jax
import jax.numpy as jnp
from jax import lax
from jax.experimental import pallas as pl
from jax.experimental.pallas import tpu as pltpu
from jax.sharding import PartitionSpec as P

F32, BF16 = jnp.float32, jnp.bfloat16
MESH = pl.DeviceIdType.MESH
ROWS, HD = 512, 128
L = 32
NC = ROWS // L
NG, GR = 8, 64
NQ, NK = 16, 8
BQ, BK = NQ * L, NK * L
KQ, KR = 4, 128
SCALE = HD ** -0.5
LOG2E = math.log2(math.e)


def dg(a, b, ca, cb):
    return lax.dot_general(a, b, (((ca,), (cb,)), ((), ())), preferred_element_type=F32)


def kernel(q_hbm, k_hbm, v_hbm, o_hbm, do_hbm, lse_hbm, dq_ref, dk_ref, dv_ref,
           qd, kv, ld, ex, thr, kt, vt, qt, dot, p_a, p_b, p_c, ds_a, ds_b, ds_c, dqt, dkt, dvt,
           pq, rb, sa, ra, pk, rd, sz, rz, o_in, lse_in,
           in_s, ld_s, qa_s, qb_s, kz_s, kd_s, rb_s, ra_s, rd_s, rz_s,
           lda_r, ldb_r, qa_r, q7_r, qn_r, qf_r, kz_r, kd_r, rb_r, ra_r, rd_r, rz_r):
    me = lax.axis_index('cp')
    core = lax.rem(me, 2)
    x = lax.rem(lax.div(me, 2), 4)
    y = lax.rem(lax.div(me, 8), 4)
    z = lax.div(me, 32)
    a = x + core * (y - x)
    b = y + core * (x - y)
    step_a, step_b = 2 + 6 * core, 8 - 6 * core

    def dev_q(b_, a_):
        return z * 32 + b_ * step_b + a_ * step_a + core

    def dev_k(z_, c_):
        return z_ * 32 + y * 8 + x * 2 + c_

    def turn(i, d):
        return lax.rem(i + d, 4)

    def remote(src, dst, ss, rs, dev):
        return pltpu.make_async_remote_copy(src_ref=src, dst_ref=dst, send_sem=ss, recv_sem=rs,
                                            device_id={'cp': dev}, device_id_type=MESH)

    D3 = (1, 2, 3)
    slot = b * 4 + a

    def rows_g(g):
        return pl.ds(pl.multiple_of(g * GR, GR), GR)

    def got(ref, sem):
        pltpu.make_async_copy(ref, ref, sem).wait()

    def own_a(src, ss, rs, d):
        return remote(src, src, ss, rs, dev_q(b, turn(a, d)))

    def to_b(src, ss, rs, d):
        return remote(src, src, ss, rs, dev_q(turn(b, d), a))

    def q_blk(n, g):
        return qd.at[b * 4 + turn(a, n), :, rows_g(g), :]

    def q_row(b_, g, n=0, size=4):
        return qd.at[pl.ds(b_ * 4 + n, size), :, rows_g(g), :]

    def q_n(g, n):
        return to_b(q_row(b, g), qb_s.at[0], qn_r.at[g], 1 + 2 * n)

    def q_f(g, n):
        return to_b(q_row(turn(b, 3 - 2 * n), g, 2 * n, 2), qb_s.at[0], qf_r.at[g], 1 + 2 * n)

    def k_z(j, d):
        r = kv.at[core, z, :, pl.ds(pl.multiple_of(j * KR, KR), KR), :]
        return remote(r, r, kz_s.at[0], kz_r.at[j], dev_k(turn(z, d), core))

    def k_d(j, d):
        r = kv.at[core, turn(z, 4 - d), :, pl.ds(pl.multiple_of(j * KR, KR), KR), :]
        return remote(r, r, kd_s.at[0], kd_r.at[j], dev_k(z, 1 - core))

    def r_b(g, d):
        return remote(pq.at[g, pl.ds(turn(b, d) * 4, 4)], rb.at[g, d - 1], rb_s.at[0], rb_r.at[g], dev_q(turn(b, d), a))

    def r_a(g, d):
        return remote(sa.at[g, turn(a, d)], ra.at[g, d - 1], ra_s.at[0], ra_r.at[g], dev_q(b, turn(a, d)))

    def r_d(g):
        return remote(pk.at[g, 1 - core], rd.at[g], rd_s.at[0], rd_r.at[g], dev_k(z, 1 - core))

    def r_z(g, d):
        return remote(sz.at[g, turn(z, d)], rz.at[g, d - 1], rz_s.at[0], rz_r.at[g], dev_k(turn(z, d), core))

    barrier = pltpu.get_barrier_semaphore()
    peers = [dev_q(b, turn(a, d)) for d in D3] + [dev_q(turn(b, d), a) for d in D3]
    peers += [dev_k(turn(z, d), core) for d in D3] + [dev_k(z, 1 - core)]
    for p in peers:
        pl.semaphore_signal(barrier, inc=1, device_id={'cp': p}, device_id_type=MESH)
    ins = [(do_hbm, qd.at[slot, 1], 0), (q_hbm, qd.at[slot, 0], 0), (k_hbm, kv.at[core, z, 0], 1),
           (v_hbm, kv.at[core, z, 1], 1), (o_hbm, o_in, 2), (lse_hbm, lse_in, 3)]
    for src, dst, n in ins:
        pltpu.make_async_copy(src, dst, in_s.at[n]).start()
    ld[slot] = jnp.zeros((4, 8, 128), F32)
    for ref, n in ((qd.at[slot], 0), (kv.at[core, z], 1), (o_in, 2), (lse_in, 3)):
        got(ref, in_s.at[n])

    def split(t):
        hi = t.astype(BF16).astype(F32)
        mid = (t - hi).astype(BF16).astype(F32)
        return hi, mid, t - hi - mid

    with jax.named_scope('own_ld'):
        for j in range(4):
            rows_j = pl.ds(j * 128, 128)
            d_j = jnp.sum(qd[slot, 1, rows_j, :].astype(F32) * o_in[rows_j, :].astype(F32), axis=1, keepdims=True)
            d_j = jnp.broadcast_to(d_j, (128, 128)).T[:1]
            for n, t in enumerate(split(lse_in[:, rows_j] * (-1.0 / SCALE)) + split(-d_j)):
                ld[slot, j, pl.ds(n, 1), :] = t
    with jax.named_scope('barrier'):
        pl.semaphore_wait(barrier, len(peers))

    def start_a(g):
        for d in D3:
            own_a(q_blk(0, g), qa_s.at[0], qa_r.at[g], d).start()

    for d in D3:
        own_a(ld.at[slot], ld_s.at[0], lda_r.at[0], d).start()
    for d in D3:
        k_z(0, d).start()
    k_d(0, 0).start()
    start_a(7)
    for d in D3:
        to_b(ld.at[slot], ld_s.at[0], ldb_r.at[0], d).start()
    for d in D3:
        to_b(q_blk(0, 7), qb_s.at[0], q7_r.at[0], d).start()

    def start_k(j, _):
        for d in D3:
            k_z(j, d).start()
        k_d(j, 0).start()
        return 0
    lax.fori_loop(1, KQ, start_k, 0)
    qi = lax.broadcasted_iota(jnp.int32, (BQ, 1), 0)
    ki = lax.broadcasted_iota(jnp.int32, (1, BK), 1)
    qpos = (qi & (L - 1)) * 128 + dev_q(qi >> 7, (qi >> 5) & 3)
    kpos = (ki & (L - 1)) * 128 + dev_k((ki >> 5) & 3, ki >> 7)
    thr[0] = jnp.full((BQ, BK), jnp.inf, F32)
    thr[1] = jnp.where(kpos <= qpos, jnp.inf, -jnp.inf).astype(F32)
    ex[...] = jnp.zeros_like(ex)
    ri = lax.broadcasted_iota(jnp.int32, (HD, BK), 0)
    for c in range(NC):
        kt[c, HD:] = jnp.where(ri < 3, 1.0, 0.0).astype(BF16)
        vt[c, HD:] = jnp.where((ri >= 3) & (ri < 6), 1.0, 0.0).astype(BF16)
    def got_a(g):
        got(qd.at[pl.ds(0, 3), :, rows_g(g), :], qa_r.at[g])

    def prep_e(i, _):
        for n in range(4):
            for j in range(4):
                ex[4 * i + n, pl.ds(j * 128, 128), pl.ds(0, 8)] = ld[4 * i + n, j].T.astype(BF16)
        return 0

    def pass_k(j):
        with jax.named_scope('pass_k'):
            got(kv.at[0, pl.ds(0, 3), :, pl.ds(0, KR), :], kz_r.at[j])
        for d in D3:
            k_d(j, d).start()

    with jax.named_scope('w_lda'):
        got(ld.at[pl.ds(0, 3)], lda_r.at[0])
    for n in D3:
        for d in D3:
            to_b(ld.at[b * 4 + turn(a, n)], ld_s.at[0], ldb_r.at[0], d).start()
    with jax.named_scope('got_a7'):
        got_a(7)
    for n in D3:
        for d in D3:
            to_b(q_blk(n, 7), qb_s.at[0], q7_r.at[0], d).start()
    start_a(6)
    dkt[...] = jnp.zeros_like(dkt)
    dvt[...] = jnp.zeros_like(dvt)
    dqt[...] = jnp.zeros_like(dqt)
    pass_k(0)
    with jax.named_scope('w_ldb'):
        got(ld.at[pl.ds(0, 12)], ldb_r.at[0])
    with jax.named_scope('prep_e'):
        lax.fori_loop(0, NQ // 4, prep_e, 0)

    def rows_q(which, r):
        return qd[:, which, pl.ds(pl.multiple_of(r * L, L), L), :].reshape(BQ, HD)

    def rows_k(which, c):
        return kv[:, :, which, pl.ds(pl.multiple_of(c * L, L), L), :].reshape(BK, HD)

    def rows_e(r):
        return ex[:, pl.ds(pl.multiple_of(r * L, L), L), :].reshape(BQ, HD)

    def take_k(j):
        with jax.named_scope('take_k'):
            got(kv.at[0, :, :, pl.ds(0, KR), :], kd_r.at[j])
        with jax.named_scope('prep_k'):
            for n in range(KR // L):
                c = j * (KR // L) + n
                kt[c, :HD] = rows_k(0, c).T
                vt[c, :HD] = rows_k(1, c).T

    def a_mm(r, c):
        e = rows_e(r)
        return (dg(jnp.concatenate([rows_q(0, r), e], axis=1), kt[c], 1, 0),
                dg(jnp.concatenate([rows_q(1, r), e], axis=1), vt[c], 1, 0))

    def a_vpu(sdp, diag, p_s, ds_s):
        s, dp = sdp
        t = s * (SCALE * LOG2E)
        if diag is not None:
            t = jnp.minimum(t, thr[diag])
        p = jnp.exp2(t)
        p_s[...] = p.astype(BF16)
        ds_s[...] = (p * dp).astype(BF16)

    def b_mm(c, h, p_s, ds_s):
        p, ds = p_s[...], ds_s[...]
        dqt[h] += dg(kt[c, :HD], ds, 1, 1)
        return dg(dot[h], p, 1, 0), dg(qt[h], ds, 1, 0)

    def q_prep(r, h):
        qt[h] = rows_q(0, r).T
        dot[h] = rows_q(1, r).T

    def finish_q(g, h):
        pq[g, :, pl.ds(h * L, L), :] = dqt[h].T.reshape(NQ, L, HD)
        dqt[h] = jnp.zeros((HD, BQ), F32)

    def finish_k(g, h):
        r = 2 * g + h
        pk[g, :, :, 0, pl.ds(h * L, L), :] = dkt[r].T.reshape(2, 4, L, HD)
        pk[g, :, :, 1, pl.ds(h * L, L), :] = dvt[r].T.reshape(2, 4, L, HD)

    def one(c, r0, d0):
        sdp = a_mm(r0, c + 1)
        dv, dk = b_mm(c, 0, p_a, ds_a)
        a_vpu(sdp, d0, p_a, ds_a)
        sdp = a_mm(r0 + 1, c + 1)
        dv1, dk1 = b_mm(c, 1, p_b, ds_b)
        a_vpu(sdp, None, p_b, ds_b)
        dvt[c] += dv + dv1
        dkt[c] += dk + dk1

    def two(c, r0):
        one(c, r0, None)
        one(c + 1, r0, lax.div(c + 2, r0))

    def tail(g, nxt=None):
        r0, r1 = 2 * g, 2 * g + 1
        sdp = a_mm(r1, r1)
        dv, dk = b_mm(r0, 0, p_a, ds_a)
        a_vpu(sdp, 1, p_c, ds_c)
        if nxt is not None:
            sdp = a_mm(2 * nxt, 0)
        dv1, dk1 = b_mm(r0, 1, p_b, ds_b)
        if nxt is not None:
            a_vpu(sdp, lax.div(7 - nxt, 7), p_a, ds_a)
        dvt[r0] += dv + dv1
        dkt[r0] += dk + dk1
        if nxt is not None:
            sdp = a_mm(2 * nxt + 1, 0)
        dv, dk = b_mm(r1, 1, p_c, ds_c)
        if nxt is not None:
            a_vpu(sdp, None, p_b, ds_b)
        dvt[r1] += dv
        dkt[r1] += dk
        finish_q(g, 0)
        finish_k(g, 0)
        finish_q(g, 1)
        finish_k(g, 1)
        if nxt is not None:
            q_prep(2 * nxt, 0)
            q_prep(2 * nxt + 1, 1)

    def send_q(g):
        for d in D3:
            r_b(g, d).start()

    def send_k(g):
        r_d(g).start()

    def mid_q(g):
        with jax.named_scope('mid_q'):
            got(rb.at[g], rb_r.at[g])
            sa[g] = pq[g, pl.ds(b * 4, 4)] + rb[g, 0] + rb[g, 1] + rb[g, 2]
        for d in D3:
            r_a(g, d).start()

    def mid_k(g):
        with jax.named_scope('mid_k'):
            got(rd.at[g], rd_r.at[g])
            sz[g] = pk[g, core] + rd[g]
        for d in D3:
            r_z(g, d).start()

    def end_q(g):
        with jax.named_scope('end_q'):
            got(ra.at[g], ra_r.at[g])
            dq = sa[g, a] + ra[g, 0] + ra[g, 1] + ra[g, 2]
            dq_ref[rows_g(g), :] = (dq * SCALE).astype(BF16)

    def end_k(g):
        with jax.named_scope('end_k'):
            got(rz.at[g], rz_r.at[g])
            dkv = sz[g, z] + rz[g, 0] + rz[g, 1] + rz[g, 2]
            dk_ref[rows_g(g), :] = (dkv[0] * SCALE).astype(BF16)
            dv_ref[rows_g(g), :] = dkv[1].astype(BF16)

    def pass_q(g):
        with jax.named_scope('pass_q'):
            got(q_row(0, g, 0, 8), qn_r.at[g])
        for n in (0, 1):
            q_f(g, n).start()

    def next_q(g):
        with jax.named_scope('next_q'):
            got_a(g)
        for n in (0, 1):
            q_n(g, n).start()

    take_k(0)
    pass_k(1)
    with jax.named_scope('first_q'):
        got(q_row(0, 7, 0, 12), q7_r.at[0])
    q_prep(14, 0)
    q_prep(15, 1)
    next_q(6)
    for g in (5, 0, 4, 3, 2, 1):
        start_a(g)
    with jax.named_scope('first'):
        a_vpu(a_mm(14, 0), None, p_a, ds_a)
        a_vpu(a_mm(15, 0), None, p_b, ds_b)

    def group(i):
        late = lax.div(i + 4, 8)
        return 7 - i + late - 4 * (lax.div(i + 5, 8) - late)

    def at(events, j):
        for when, act in events.items():
            pl.when(j == when)(act)

    def runs(*acts):
        def run():
            for f, arg in acts:
                f(arg)
        return run

    ahead = {
        0: {1: runs((take_k, 1)), 2: runs((pass_k, 2)), 3: runs((take_k, 2), (next_q, 5)),
            4: runs((pass_k, 3), (pass_q, 6), (next_q, 0)), 5: runs((take_k, 3), (next_q, 4)),
            6: runs((next_q, 3))},
        1: {1: runs((pass_q, 5), (next_q, 1)), 2: runs((mid_k, 7), (pass_q, 0)), 3: runs((pass_q, 4)), 4: runs((pass_q, 3))},
        2: {1: runs((pass_q, 2)), 2: runs((mid_k, 6)), 3: runs((pass_q, 1))},
        4: {1: runs((mid_k, 5))},
        5: {1: runs((mid_k, 4)), 2: runs((mid_q, 0))},
        6: {1: runs((mid_k, 3))},
    }
    behind = {
        0: runs((next_q, 2)),
        1: runs((mid_q, 7)),
        2: runs((mid_q, 6)),
        4: runs((mid_q, 5)),
        6: runs((mid_q, 4)),
    }

    def superstep(i, _):
        g = group(i)
        g1 = group(i + 1)

        def pair(j, _):
            def at_some(whens):
                for when in whens:
                    pl.when(i == when)(functools.partial(at, ahead[when], j))
            pl.when(i < 2)(functools.partial(at_some, (0, 1)))
            pl.when(i >= 2)(functools.partial(at_some, (2, 4, 5, 6)))
            with jax.named_scope('two'):
                two(2 * j, 2 * g)
            return 0
        lax.fori_loop(0, g, pair, 0)
        with jax.named_scope('take_q'):
            got(q_row(0, g1), qf_r.at[g1])
        with jax.named_scope('tail'):
            tail(g, g1)
        send_q(g)
        pl.when(i != 3)(functools.partial(send_k, g))
        for when, act in behind.items():
            pl.when(i == when)(act)
        return 0
    lax.fori_loop(0, NG - 1, superstep, 0)

    with jax.named_scope('two'):
        two(0, 2)
    finish_k(0, 0)
    finish_k(0, 1)
    send_k(0)
    mid_k(2)
    with jax.named_scope('tail'):
        tail(1)
    send_q(1)
    send_k(1)
    mid_k(0)
    mid_q(3)
    mid_k(1)
    for g in (7, 6, 5):
        end_k(g)
        end_q(g)
    end_q(0)
    mid_q(2)
    end_k(4)
    end_q(4)
    mid_q(1)
    end_k(3)
    end_k(2)
    end_q(3)
    end_k(0)
    end_k(1)
    end_q(2)
    end_q(1)

    got(ld.at[pl.ds(0, 15)], ld_s.at[0])
    got(qd.at[pl.ds(0, 3)], qa_s.at[0])
    got(qd.at[pl.ds(0, 12)], qb_s.at[0])
    got(kv.at[0, pl.ds(0, 3)], kz_s.at[0])
    got(kv.at[0], kd_s.at[0])
    got(pq.at[pl.ds(0, 6)], rb_s.at[0])
    got(sa.at[pl.ds(0, 6)], ra_s.at[0])
    got(rd, rd_s.at[0])
    got(rz, rz_s.at[0])


def put(*refs):
    sem = refs[6]
    copies = [pltpu.make_async_copy(refs[n], refs[3 + n], sem.at[n]) for n in range(3)]
    for c in copies:
        c.start()
    for c in copies:
        c.wait()


def local(q, k, v, o, dout, lse):
    flat = (ROWS, HD)
    vm = pl.BlockSpec(memory_space=pltpu.VMEM)
    V, DMA = pltpu.VMEM, pltpu.SemaphoreType.DMA
    scratch = [
        V((NQ, 2, ROWS, HD), BF16), V((2, 4, 2, ROWS, HD), BF16), V((NQ, 4, 8, 128), F32),
        V((NQ, ROWS, HD), BF16), V((2, BQ, BK), F32),
        V((NC, 2 * HD, BK), BF16), V((NC, 2 * HD, BK), BF16), V((2, HD, BQ), BF16), V((2, HD, BQ), BF16),
        *[V((BQ, BK), BF16)] * 6,
        V((2, HD, BQ), F32), V((NC, HD, BK), F32), V((NC, HD, BK), F32),
        V((NG, NQ, GR, HD), F32), V((NG, 3, 4, GR, HD), F32), V((NG, 4, GR, HD), F32), V((NG, 3, GR, HD), F32),
        V((NG, 2, 4, 2, GR, HD), F32), V((NG, 4, 2, GR, HD), F32), V((NG, 4, 2, GR, HD), F32),
        V((NG, 3, 2, GR, HD), F32), V((ROWS, HD), BF16), V((1, ROWS), F32),
        DMA((4,)), *[DMA((1,))] * 9,
        DMA((1,)), DMA((1,)), DMA((NG,)), DMA((1,)), DMA((NG,)), DMA((NG,)), DMA((KQ,)), DMA((KQ,)), *[DMA((NG,))] * 4,
    ]
    outs = pl.pallas_call(
        kernel,
        out_shape=[pltpu.VMEM(flat, BF16)] * 3,
        in_specs=[pl.BlockSpec(memory_space=pl.ANY)] * 6, out_specs=[vm] * 3,
        scratch_shapes=scratch,
        compiler_params=pltpu.CompilerParams(collective_id=0, has_side_effects=True, vmem_limit_bytes=62 << 20),
    )(*[t.reshape(flat) for t in (q, k, v, o, dout)], lse)
    outs = pl.pallas_call(
        put,
        out_shape=[jax.ShapeDtypeStruct(flat, BF16)] * 3,
        in_specs=[vm] * 3, out_specs=[pl.BlockSpec(memory_space=pl.ANY)] * 3,
        scratch_shapes=[DMA((3,))],
    )(*[pltpu.with_memory_space_constraint(t, pltpu.VMEM) for t in outs])
    return tuple(t.reshape(ROWS, 1, HD) for t in outs)


def solution(mesh):
    rows = P(('data', 'cp'))
    cols = P(None, ('data', 'cp'))
    return jax.shard_map(local, mesh=mesh, in_specs=(rows, rows, rows, rows, rows, cols),
                         out_specs=(rows, rows, rows), check_vma=False)
```

```python
import functools
import math

import jax
import jax.numpy as jnp
from jax import lax
from jax.experimental import pallas as pl
from jax.experimental.pallas import tpu as pltpu
from jax.sharding import PartitionSpec as P

F32, BF16 = jnp.float32, jnp.bfloat16
MESH = pl.DeviceIdType.MESH
ROWS, HD = 512, 128
L = 32
NC = ROWS // L
NG, GR = 8, 64
NQ, NK = 16, 8
BQ, BK = NQ * L, NK * L
KQ, KR = 4, 128
SCALE = HD ** -0.5
LOG2E = math.log2(math.e)


def dg(a, b, ca, cb):
    return lax.dot_general(a, b, (((ca,), (cb,)), ((), ())), preferred_element_type=F32)


def kernel(q_hbm, k_hbm, v_hbm, o_hbm, do_hbm, lse_hbm, dq_ref, dk_ref, dv_ref,
           qd, kv, ld, ex, thr, kt, vt, qt, dot, p_a, p_b, p_c, ds_a, ds_b, ds_c, dqt, dkt, dvt,
           pq, rb, sa, ra, pk, rd, sz, rz, o_in, lse_in,
           in_s, ld_s, qa_s, qb_s, kz_s, kd_s, rb_s, ra_s, rd_s, rz_s,
           lda_r, ldb_r, qa_r, q7a_r, q7_r, qn_r, qf_r, kz_r, kd_r, rb_r, rf_r, ra_r, rd_r, rz_r, rzf_r):
    me = lax.axis_index('cp')
    core = lax.rem(me, 2)
    x = lax.rem(lax.div(me, 2), 4)
    y = lax.rem(lax.div(me, 8), 4)
    z = lax.div(me, 32)
    a = x + core * (y - x)
    b = y + core * (x - y)
    step_a, step_b = 2 + 6 * core, 8 - 6 * core

    def dev_q(b_, a_):
        return z * 32 + b_ * step_b + a_ * step_a + core

    def dev_k(z_, c_):
        return z_ * 32 + y * 8 + x * 2 + c_

    def turn(i, d):
        return lax.rem(i + d, 4)

    def remote(src, dst, ss, rs, dev):
        return pltpu.make_async_remote_copy(src_ref=src, dst_ref=dst, send_sem=ss, recv_sem=rs,
                                            device_id={'cp': dev}, device_id_type=MESH)

    D3 = (1, 2, 3)
    slot = b * 4 + a

    def rows_g(g):
        return pl.ds(pl.multiple_of(g * GR, GR), GR)

    def got(ref, sem):
        pltpu.make_async_copy(ref, ref, sem).wait()

    def own_a(src, ss, rs, d):
        return remote(src, src, ss, rs, dev_q(b, turn(a, d)))

    def to_b(src, ss, rs, d):
        return remote(src, src, ss, rs, dev_q(turn(b, d), a))

    def q_blk(n, g):
        return qd.at[b * 4 + turn(a, n), :, rows_g(g), :]

    def q_row(b_, g, n=0, size=4):
        return qd.at[pl.ds(b_ * 4 + n, size), :, rows_g(g), :]

    def q_n(g, n):
        return to_b(q_row(b, g), qb_s.at[0], qn_r.at[g], 1 + 2 * n)

    def q_f(g, n):
        return to_b(q_row(turn(b, 3 - 2 * n), g, 2 * n, 2), qb_s.at[0], qf_r.at[g], 1 + 2 * n)

    def k_z(j, d):
        r = kv.at[core, z, :, pl.ds(pl.multiple_of(j * KR, KR), KR), :]
        return remote(r, r, kz_s.at[0], kz_r.at[j], dev_k(turn(z, d), core))

    def k_d(j, d):
        r = kv.at[core, turn(z, 4 - d), :, pl.ds(pl.multiple_of(j * KR, KR), KR), :]
        return remote(r, r, kd_s.at[0], kd_r.at[j], dev_k(z, 1 - core))

    def r_b(g, d):
        return remote(pq.at[g, pl.ds(turn(b, d) * 4, 4)], rb.at[g, d - 1], rb_s.at[0], rb_r.at[g], dev_q(turn(b, d), a))

    def r_opp(g, n):
        return remote(pq.at[g, pl.ds(turn(b, 2) * 4 + 2 * n, 2)], rb.at[g, 2, pl.ds(2 * n, 2)], rb_s.at[0], rb_r.at[g],
                      dev_q(turn(b, 1 + 2 * n), a))

    def r_near(g, n):
        return remote(pq.at[g, pl.ds(turn(b, 1 + 2 * n) * 4 + 2 - 2 * n, 2)], rb.at[g, n, pl.ds(2 - 2 * n, 2)],
                      rb_s.at[0], rf_r.at[g], dev_q(turn(b, 1 + 2 * n), a))

    def r_on(g, n):
        return remote(rb.at[g, 2, pl.ds(2 * n, 2)], rb.at[g, n, pl.ds(2 * n, 2)],
                      rb_s.at[0], rf_r.at[g], dev_q(turn(b, 1 + 2 * n), a))

    def r_a(g, d):
        return remote(sa.at[g, turn(a, d)], ra.at[g, d - 1], ra_s.at[0], ra_r.at[g], dev_q(b, turn(a, d)))

    def r_d(g):
        return remote(pk.at[g, 1 - core], rd.at[g], rd_s.at[0], rd_r.at[g], dev_k(z, 1 - core))

    def r_z(g, d):
        return remote(sz.at[g, turn(z, d)], rz.at[g, d - 1], rz_s.at[0], rz_r.at[g], dev_k(turn(z, d), core))

    def k_opp(g, n):
        return remote(sz.at[g, turn(z, 2), n], rz.at[g, 2, n], rz_s.at[0], rz_r.at[g], dev_k(turn(z, 1 + 2 * n), core))

    def k_near(g, n):
        return remote(sz.at[g, turn(z, 1 + 2 * n), 1 - n], rz.at[g, n, 1 - n], rz_s.at[0], rzf_r.at[g],
                      dev_k(turn(z, 1 + 2 * n), core))

    def k_on(g, n):
        return remote(rz.at[g, 2, n], rz.at[g, n, n], rz_s.at[0], rzf_r.at[g], dev_k(turn(z, 1 + 2 * n), core))

    barrier = pltpu.get_barrier_semaphore()
    peers = [dev_q(b, turn(a, d)) for d in D3] + [dev_q(turn(b, d), a) for d in D3]
    peers += [dev_k(turn(z, d), core) for d in D3] + [dev_k(z, 1 - core)]
    for p in peers:
        pl.semaphore_signal(barrier, inc=1, device_id={'cp': p}, device_id_type=MESH)
    ins = [(do_hbm, qd.at[slot, 1], 0), (q_hbm, qd.at[slot, 0], 0), (k_hbm, kv.at[core, z, 0], 1),
           (v_hbm, kv.at[core, z, 1], 1), (o_hbm, o_in, 2), (lse_hbm, lse_in, 3)]
    for src, dst, n in ins:
        pltpu.make_async_copy(src, dst, in_s.at[n]).start()
    ld[slot] = jnp.zeros((4, 8, 128), F32)
    for ref, n in ((qd.at[slot], 0), (kv.at[core, z], 1), (o_in, 2), (lse_in, 3)):
        got(ref, in_s.at[n])

    def split(t):
        hi = t.astype(BF16).astype(F32)
        mid = (t - hi).astype(BF16).astype(F32)
        return hi, mid, t - hi - mid

    with jax.named_scope('own_ld'):
        for j in range(4):
            rows_j = pl.ds(j * 128, 128)
            d_j = jnp.sum(qd[slot, 1, rows_j, :].astype(F32) * o_in[rows_j, :].astype(F32), axis=1, keepdims=True)
            d_j = jnp.broadcast_to(d_j, (128, 128)).T[:1]
            for n, t in enumerate(split(lse_in[:, rows_j] * (-1.0 / SCALE)) + split(-d_j)):
                ld[slot, j, pl.ds(n, 1), :] = t
    with jax.named_scope('barrier'):
        pl.semaphore_wait(barrier, len(peers))

    def start_a(g):
        for d in D3:
            own_a(q_blk(0, g), qa_s.at[0], qa_r.at[g], d).start()

    for d in D3:
        own_a(ld.at[slot], ld_s.at[0], lda_r.at[0], d).start()
    for d in D3:
        k_z(0, d).start()
    k_d(0, 0).start()
    for d in D3:
        own_a(q_blk(0, 7), qa_s.at[0], q7a_r.at[a], d).start()
    for d in D3:
        to_b(ld.at[slot], ld_s.at[0], ldb_r.at[0], d).start()
    for d in D3:
        to_b(q_blk(0, 7), qb_s.at[0], q7_r.at[0], d).start()

    def start_k(j, _):
        for d in D3:
            k_z(j, d).start()
        k_d(j, 0).start()
        return 0
    lax.fori_loop(1, KQ, start_k, 0)
    qi = lax.broadcasted_iota(jnp.int32, (BQ, 1), 0)
    ki = lax.broadcasted_iota(jnp.int32, (1, BK), 1)
    qpos = (qi & (L - 1)) * 128 + dev_q(qi >> 7, (qi >> 5) & 3)
    kpos = (ki & (L - 1)) * 128 + dev_k((ki >> 5) & 3, ki >> 7)
    thr[0] = jnp.full((BQ, BK), jnp.inf, F32)
    thr[1] = jnp.where(kpos <= qpos, jnp.inf, -jnp.inf).astype(F32)
    ex[...] = jnp.zeros_like(ex)
    ri = lax.broadcasted_iota(jnp.int32, (HD, BK), 0)
    for c in range(NC):
        kt[c, HD:] = jnp.where(ri < 3, 1.0, 0.0).astype(BF16)
        vt[c, HD:] = jnp.where((ri >= 3) & (ri < 6), 1.0, 0.0).astype(BF16)
    def got_a(g):
        got(qd.at[pl.ds(0, 3), :, rows_g(g), :], qa_r.at[g])

    def prep_e(i, _):
        for n in range(4):
            for j in range(4):
                ex[4 * i + n, pl.ds(j * 128, 128), pl.ds(0, 8)] = ld[4 * i + n, j].T.astype(BF16)
        return 0

    def pass_k(j):
        with jax.named_scope('pass_k'):
            got(kv.at[0, pl.ds(0, 3), :, pl.ds(0, KR), :], kz_r.at[j])
        for d in D3:
            k_d(j, d).start()

    with jax.named_scope('w_lda'):
        got(ld.at[pl.ds(0, 3)], lda_r.at[0])
    for n in D3:
        for d in D3:
            to_b(ld.at[b * 4 + turn(a, n)], ld_s.at[0], ldb_r.at[0], d).start()
    for p in (0, 1, 3, 2):
        @pl.when(a != p)
        def _():
            r = qd.at[b * 4 + p, :, rows_g(7), :]
            with jax.named_scope('got_a7'):
                got(r, q7a_r.at[p])
            for d in D3:
                to_b(r, qb_s.at[0], q7_r.at[0], d).start()
    start_a(6)
    dkt[...] = jnp.zeros_like(dkt)
    dvt[...] = jnp.zeros_like(dvt)
    dqt[...] = jnp.zeros_like(dqt)
    pass_k(0)
    with jax.named_scope('w_ldb'):
        got(ld.at[pl.ds(0, 12)], ldb_r.at[0])
    with jax.named_scope('prep_e'):
        lax.fori_loop(0, NQ // 4, prep_e, 0)

    def rows_q(which, r):
        return qd[:, which, pl.ds(pl.multiple_of(r * L, L), L), :].reshape(BQ, HD)

    def rows_k(which, c):
        return kv[:, :, which, pl.ds(pl.multiple_of(c * L, L), L), :].reshape(BK, HD)

    def rows_e(r):
        return ex[:, pl.ds(pl.multiple_of(r * L, L), L), :].reshape(BQ, HD)

    def take_k(j):
        with jax.named_scope('take_k'):
            got(kv.at[0, :, :, pl.ds(0, KR), :], kd_r.at[j])
        with jax.named_scope('prep_k'):
            for n in range(KR // L):
                c = j * (KR // L) + n
                kt[c, :HD] = rows_k(0, c).T
                vt[c, :HD] = rows_k(1, c).T

    def a_mm(r, c):
        e = rows_e(r)
        return (dg(jnp.concatenate([rows_q(0, r), e], axis=1), kt[c], 1, 0),
                dg(jnp.concatenate([rows_q(1, r), e], axis=1), vt[c], 1, 0))

    def a_vpu(sdp, diag, p_s, ds_s):
        s, dp = sdp
        t = s * (SCALE * LOG2E)
        if diag is not None:
            t = jnp.minimum(t, thr[diag])
        p = jnp.exp2(t)
        p_s[...] = p.astype(BF16)
        ds_s[...] = (p * dp).astype(BF16)

    def b_mm(c, h, p_s, ds_s):
        p, ds = p_s[...], ds_s[...]
        dqt[h] += dg(kt[c, :HD], ds, 1, 1)
        return dg(dot[h], p, 1, 0), dg(qt[h], ds, 1, 0)

    def q_prep(r, h):
        qt[h] = rows_q(0, r).T
        dot[h] = rows_q(1, r).T

    def finish_q(g, h):
        pq[g, :, pl.ds(h * L, L), :] = dqt[h].T.reshape(NQ, L, HD)
        dqt[h] = jnp.zeros((HD, BQ), F32)

    def finish_k(g, h):
        r = 2 * g + h
        pk[g, :, :, 0, pl.ds(h * L, L), :] = dkt[r].T.reshape(2, 4, L, HD)
        pk[g, :, :, 1, pl.ds(h * L, L), :] = dvt[r].T.reshape(2, 4, L, HD)

    def one(c, r0, d0):
        sdp = a_mm(r0, c + 1)
        dv, dk = b_mm(c, 0, p_a, ds_a)
        a_vpu(sdp, d0, p_a, ds_a)
        sdp = a_mm(r0 + 1, c + 1)
        dv1, dk1 = b_mm(c, 1, p_b, ds_b)
        a_vpu(sdp, None, p_b, ds_b)
        dvt[c] += dv + dv1
        dkt[c] += dk + dk1

    def two(c, r0):
        one(c, r0, None)
        one(c + 1, r0, lax.div(c + 2, r0))

    def tail(g, nxt=None):
        r0, r1 = 2 * g, 2 * g + 1
        sdp = a_mm(r1, r1)
        dv, dk = b_mm(r0, 0, p_a, ds_a)
        a_vpu(sdp, 1, p_c, ds_c)
        dv1, dk1 = b_mm(r0, 1, p_b, ds_b)
        dvt[r0] += dv + dv1
        dkt[r0] += dk + dk1
        finish_q(g, 0)
        finish_k(g, 0)
        if nxt is not None:
            sdp = a_mm(2 * nxt, 0)
        dv, dk = b_mm(r1, 1, p_c, ds_c)
        if nxt is not None:
            a_vpu(sdp, lax.div(7 - nxt, 7), p_a, ds_a)
        dvt[r1] += dv
        dkt[r1] += dk
        if nxt is not None:
            sdp = a_mm(2 * nxt + 1, 0)
        finish_q(g, 1)
        finish_k(g, 1)
        if nxt is not None:
            a_vpu(sdp, None, p_b, ds_b)
            q_prep(2 * nxt, 0)
            q_prep(2 * nxt + 1, 1)

    def send_q(g):
        for n in (0, 1):
            r_opp(g, n).start()
        for n in (0, 1):
            r_near(g, n).start()

    def relay_q(g):
        with jax.named_scope('relay_q'):
            got(rb.at[g, 2], rb_r.at[g])
            for n in (0, 1):
                half = pl.ds(2 * n, 2)
                rb[g, 2, half] = rb[g, 2, half] + pq[g, pl.ds(turn(b, 1 + 2 * n) * 4 + 2 * n, 2)]
        for n in (0, 1):
            r_on(g, n).start()

    def mid_q(g):
        with jax.named_scope('mid_q'):
            got(rb.at[g, pl.ds(0, 2)], rf_r.at[g])
            sa[g] = pq[g, pl.ds(b * 4, 4)] + rb[g, 0] + rb[g, 1]
        for d in D3:
            r_a(g, d).start()

    def send_k(g):
        r_d(g).start()

    def sum_k(g):
        with jax.named_scope('sum_k'):
            got(rd.at[g], rd_r.at[g])
            sz[g] = pk[g, core] + rd[g]

    def mid_k(g):
        sum_k(g)
        for d in D3:
            r_z(g, d).start()

    def mid_k_by(g):
        sum_k(g)
        for n in (0, 1):
            k_opp(g, n).start()
        for n in (0, 1):
            k_near(g, n).start()

    def relay_k(g):
        with jax.named_scope('relay_k'):
            got(rz.at[g, 2], rz_r.at[g])
            for n in (0, 1):
                rz[g, 2, n] = rz[g, 2, n] + sz[g, turn(z, 1 + 2 * n), n]
        for n in (0, 1):
            k_on(g, n).start()

    def end_q(g):
        with jax.named_scope('end_q'):
            got(ra.at[g], ra_r.at[g])
            dq = sa[g, a] + ra[g, 0] + ra[g, 1] + ra[g, 2]
            dq_ref[rows_g(g), :] = (dq * SCALE).astype(BF16)

    def out_k(g, dkv):
        dk_ref[rows_g(g), :] = (dkv[0] * SCALE).astype(BF16)
        dv_ref[rows_g(g), :] = dkv[1].astype(BF16)

    def end_k(g):
        with jax.named_scope('end_k'):
            got(rz.at[g], rz_r.at[g])
            out_k(g, sz[g, z] + rz[g, 0] + rz[g, 1] + rz[g, 2])

    def end_k_by(g):
        with jax.named_scope('end_k_by'):
            got(rz.at[g, pl.ds(0, 2)], rzf_r.at[g])
            out_k(g, sz[g, z] + rz[g, 0] + rz[g, 1])

    def pass_q(g):
        with jax.named_scope('pass_q'):
            got(q_row(0, g, 0, 8), qn_r.at[g])
        for n in (0, 1):
            q_f(g, n).start()

    def next_q(g):
        with jax.named_scope('next_q'):
            got_a(g)
        for n in (0, 1):
            q_n(g, n).start()

    take_k(0)
    pass_k(1)
    next_q(6)
    with jax.named_scope('first_q'):
        got(q_row(0, 7, 0, 12), q7_r.at[0])
    q_prep(14, 0)
    q_prep(15, 1)
    start_a(5)
    with jax.named_scope('first'):
        a_vpu(a_mm(14, 0), None, p_a, ds_a)
        a_vpu(a_mm(15, 0), None, p_b, ds_b)

    def group(i):
        late = lax.div(i + 4, 8)
        return 7 - i + late - 4 * (lax.div(i + 5, 8) - late)

    def at(events, j):
        for when, act in events.items():
            pl.when(j == when)(act)

    def runs(*acts):
        def run():
            for f, arg in acts:
                f(arg)
        return run

    ahead2 = {
        6: {1: runs((mid_k_by, 3), (relay_q, 4), (mid_q, 0))},
    }
    ahead4 = {
        0: {0: runs((take_k, 1), (pass_k, 2), (start_a, 0)),
            1: runs((take_k, 2), (pass_k, 3), (pass_q, 6), (next_q, 5), (start_a, 4)),
            2: runs((take_k, 3), (next_q, 0), (start_a, 3))},
        1: {1: runs((mid_k, 7), (pass_q, 0), (next_q, 3), (start_a, 1)), 2: runs((next_q, 2))},
        2: {1: runs((mid_k, 6), (pass_q, 3))},
        4: {1: runs((mid_k, 5), (mid_q, 6))},
        5: {0: runs((mid_k, 4), (relay_q, 0))},
    }
    behind = {
        0: runs((pass_q, 5), (next_q, 4), (start_a, 2)),
        1: runs((pass_q, 4), (next_q, 1), (relay_q, 7)),
        2: runs((pass_q, 2), (relay_q, 6), (mid_q, 7)),
        4: runs((pass_q, 1), (relay_q, 5)),
        5: runs((mid_q, 5)),
    }

    def fire(events, i, j):
        for when, acts in events.items():
            pl.when(i == when)(functools.partial(at, acts, j))

    def superstep(i, _):
        g = group(i)
        g1 = group(i + 1)
        single = lax.rem(g, 2) + 2 * (lax.div(i + 2, 8) - lax.div(i + 1, 8))

        def pair(j, _):
            fire(ahead2, i, j)
            with jax.named_scope('two'):
                two(2 * j, 2 * g)
            return 0

        def double(j, _):
            fire(ahead4, i, j)
            with jax.named_scope('four'):
                c = 2 * single + 4 * j
                two(c, 2 * g)
                two(c + 2, 2 * g)
            return 0
        lax.fori_loop(0, single, pair, 0)
        lax.fori_loop(0, lax.div(g - single, 2), double, 0)
        with jax.named_scope('take_q'):
            got(q_row(0, g1), qf_r.at[g1])
        with jax.named_scope('tail'):
            tail(g, g1)
        for when, act in behind.items():
            pl.when(i == when)(act)
        send_q(g)
        pl.when(i != 3)(functools.partial(send_k, g))
        return 0
    lax.fori_loop(0, NG - 1, superstep, 0)

    with jax.named_scope('two'):
        two(0, 2)
    finish_k(0, 0)
    finish_k(0, 1)
    send_k(0)
    mid_k_by(2)
    relay_q(3)
    mid_q(4)
    with jax.named_scope('tail'):
        tail(1)
    for d in D3:
        r_b(1, d).start()
    send_k(1)
    mid_k_by(0)
    relay_k(3)
    mid_k(1)
    relay_q(2)
    mid_q(3)
    for g in (7, 6, 5):
        end_k(g)
        end_q(g)
    end_q(0)
    end_k(4)
    relay_k(2)
    relay_k(0)
    with jax.named_scope('last_q'):
        got(rb.at[1], rb_r.at[1])
        sa[1] = pq[1, pl.ds(b * 4, 4)] + rb[1, 0] + rb[1, 1] + rb[1, 2]
    for d in D3:
        r_a(1, d).start()
    mid_q(2)
    end_q(4)
    end_k_by(3)
    end_k_by(2)
    end_q(3)
    end_k_by(0)
    end_k(1)
    end_q(2)
    end_q(1)

    got(ld.at[pl.ds(0, 15)], ld_s.at[0])
    got(qd.at[pl.ds(0, 3)], qa_s.at[0])
    got(qd.at[pl.ds(0, 12)], qb_s.at[0])
    got(kv.at[0, pl.ds(0, 3)], kz_s.at[0])
    got(kv.at[0], kd_s.at[0])
    got(pq.at[pl.ds(0, 6)], rb_s.at[0])
    got(sa.at[pl.ds(0, 6)], ra_s.at[0])
    got(rd, rd_s.at[0])
    got(rz, rz_s.at[0])


def put(*refs):
    sem = refs[6]
    copies = [pltpu.make_async_copy(refs[n], refs[3 + n], sem.at[n]) for n in range(3)]
    for c in copies:
        c.start()
    for c in copies:
        c.wait()


def local(q, k, v, o, dout, lse):
    flat = (ROWS, HD)
    vm = pl.BlockSpec(memory_space=pltpu.VMEM)
    V, DMA = pltpu.VMEM, pltpu.SemaphoreType.DMA
    scratch = [
        V((NQ, 2, ROWS, HD), BF16), V((2, 4, 2, ROWS, HD), BF16), V((NQ, 4, 8, 128), F32),
        V((NQ, ROWS, HD), BF16), V((2, BQ, BK), F32),
        V((NC, 2 * HD, BK), BF16), V((NC, 2 * HD, BK), BF16), V((2, HD, BQ), BF16), V((2, HD, BQ), BF16),
        *[V((BQ, BK), BF16)] * 6,
        V((2, HD, BQ), F32), V((NC, HD, BK), F32), V((NC, HD, BK), F32),
        V((NG, NQ, GR, HD), F32), V((NG, 3, 4, GR, HD), F32), V((NG, 4, GR, HD), F32), V((NG, 3, GR, HD), F32),
        V((NG, 2, 4, 2, GR, HD), F32), V((NG, 4, 2, GR, HD), F32), V((NG, 4, 2, GR, HD), F32),
        V((NG, 3, 2, GR, HD), F32), V((ROWS, HD), BF16), V((1, ROWS), F32),
        DMA((4,)), *[DMA((1,))] * 9,
        DMA((1,)), DMA((1,)), DMA((NG,)), DMA((4,)), DMA((1,)), DMA((NG,)), DMA((NG,)), DMA((KQ,)), DMA((KQ,)), *[DMA((NG,))] * 6,
    ]
    outs = pl.pallas_call(
        kernel,
        out_shape=[pltpu.VMEM(flat, BF16)] * 3,
        in_specs=[pl.BlockSpec(memory_space=pl.ANY)] * 6, out_specs=[vm] * 3,
        scratch_shapes=scratch,
        compiler_params=pltpu.CompilerParams(collective_id=0, has_side_effects=True, vmem_limit_bytes=62 << 20),
    )(*[t.reshape(flat) for t in (q, k, v, o, dout)], lse)
    outs = pl.pallas_call(
        put,
        out_shape=[jax.ShapeDtypeStruct(flat, BF16)] * 3,
        in_specs=[vm] * 3, out_specs=[pl.BlockSpec(memory_space=pl.ANY)] * 3,
        scratch_shapes=[DMA((3,))],
    )(*[pltpu.with_memory_space_constraint(t, pltpu.VMEM) for t in outs])
    return tuple(t.reshape(ROWS, 1, HD) for t in outs)


def solution(mesh):
    rows = P(('data', 'cp'))
    cols = P(None, ('data', 'cp'))
    return jax.shard_map(local, mesh=mesh, in_specs=(rows, rows, rows, rows, rows, cols),
                         out_specs=(rows, rows, rows), check_vma=False)
```

```python
import functools
import math

import jax
import jax.numpy as jnp
from jax import lax
from jax.experimental import pallas as pl
from jax.experimental.pallas import tpu as pltpu
from jax.sharding import PartitionSpec as P

F32, BF16 = jnp.float32, jnp.bfloat16
MESH = pl.DeviceIdType.MESH
ROWS, HD = 512, 128
L = 32
NC = ROWS // L
NG, GR = 8, 64
NQ, NK = 16, 8
BQ, BK = NQ * L, NK * L
KQ, KR = 4, 128
N4 = 4
D3, SIDES = (1, 2, 3), (0, 1)
SCALE = HD ** -0.5
LOG2E = math.log2(math.e)
SEQ = (7, 6, 0, 5, 4, 3, 2, 1)
END = 9
TAKE_K = (1, 2, 3)
PASS_K = (1, 2)
PASS_Q = (2, 9, 11, 19, 31, 32, 39)
NEXT_Q = (2, 3, 9, 11, 12, 19)
START_A = (1, 2, 3, 9, 11)
MID_K = (11, 31, 41, 51)
MID_K_BY = (61,)
RELAY_Q = (19, 39, 41, 49, 61)
MID_Q = (39, 49, 51, 61)


def dg(a, b, ca, cb):
    return lax.dot_general(a, b, (((ca,), (cb,)), ((), ())), preferred_element_type=F32)


def kernel(q_hbm, k_hbm, v_hbm, o_hbm, do_hbm, lse_hbm, dq_ref, dk_ref, dv_ref,
           qd, kv, ld, ex, thr, kt, vt, qt, dot, p_a, p_b, p_c, ds_a, ds_b, ds_c, dqt, dkt, dvt,
           pq, rb, sa, ra, pk, rd, sz, rz, o_in, lse_in,
           in_s, ld_s, qa_s, qb_s, kz_s, kd_s, rb_s, ra_s, rd_s, rz_s,
           lda_r, ldb_r, qa_r, q7a_r, q7_r, qn_r, qf_r, kz_r, kd_r, rb_r, rf_r, ra_r, rd_r, rz_r, rzf_r):
    me = lax.axis_index('cp')
    core = lax.rem(me, 2)
    x = lax.rem(lax.div(me, 2), 4)
    y = lax.rem(lax.div(me, 8), 4)
    z = lax.div(me, 32)
    a = x + core * (y - x)
    b = y + core * (x - y)
    step_a, step_b = 2 + 6 * core, 8 - 6 * core

    def dev_q(b_, a_):
        return z * 32 + b_ * step_b + a_ * step_a + core

    def dev_k(z_, c_):
        return z_ * 32 + y * 8 + x * 2 + c_

    def turn(i, d):
        return lax.rem(i + d, N4)

    def remote(src, dst, ss, rs, dev):
        return pltpu.make_async_remote_copy(src_ref=src, dst_ref=dst, send_sem=ss, recv_sem=rs,
                                            device_id={'cp': dev}, device_id_type=MESH)

    def side(i, n):
        return turn(i, 1 + 2 * n)

    def half(n, size=2):
        return pl.ds(2 * n, size)

    def row(b_, n=0, size=N4):
        return pl.ds(b_ * N4 + n, size)

    slot = b * N4 + a

    def rows_g(g):
        return pl.ds(pl.multiple_of(g * GR, GR), GR)

    def got(ref, sem):
        pltpu.make_async_copy(ref, ref, sem).wait()

    def own_a(src, ss, rs, d):
        return remote(src, src, ss, rs, dev_q(b, turn(a, d)))

    def to_b(src, ss, rs, d):
        return remote(src, src, ss, rs, dev_q(turn(b, d), a))

    def q_blk(n, g):
        return qd.at[b * N4 + turn(a, n), :, rows_g(g), :]

    def q_row(b_, g, n=0, size=N4):
        return qd.at[row(b_, n, size), :, rows_g(g), :]

    def q_n(g, n):
        return remote(q_row(b, g), q_row(b, g), qb_s, qn_r.at[g], dev_q(side(b, n), a))

    def q_f(g, n):
        r = q_row(side(b, 1 - n), g, 2 * n, 2)
        return remote(r, r, qb_s, qf_r.at[g], dev_q(side(b, n), a))

    def rows_p(j):
        return pl.ds(pl.multiple_of(j * KR, KR), KR)

    def k_z(j, d):
        r = kv.at[core, z, :, rows_p(j), :]
        return remote(r, r, kz_s, kz_r.at[j], dev_k(turn(z, d), core))

    def k_d(j, d=0):
        r = kv.at[core, turn(z, N4 - d), :, rows_p(j), :]
        return remote(r, r, kd_s, kd_r.at[j], dev_k(z, 1 - core))

    def r_b(g, d):
        return remote(pq.at[g, row(turn(b, d))], rb.at[g, d - 1], rb_s, rb_r.at[g], dev_q(turn(b, d), a))

    def r_opp(g, n):
        return remote(pq.at[g, row(turn(b, 2), 2 * n, 2)], rb.at[g, 2, half(n)], rb_s, rb_r.at[g], dev_q(side(b, n), a))

    def r_near(g, n):
        return remote(pq.at[g, row(side(b, n), 2 - 2 * n, 2)], rb.at[g, n, half(1 - n)], rb_s, rf_r.at[g],
                      dev_q(side(b, n), a))

    def r_on(g, n):
        return remote(rb.at[g, 2, half(n)], rb.at[g, n, half(n)], rb_s, rf_r.at[g], dev_q(side(b, n), a))

    def r_a(g, d):
        return remote(sa.at[g, turn(a, d)], ra.at[g, d - 1], ra_s, ra_r.at[g], dev_q(b, turn(a, d)))

    def r_d(g):
        return remote(pk.at[g, 1 - core], rd.at[g], rd_s, rd_r.at[g], dev_k(z, 1 - core))

    def r_z(g, d):
        return remote(sz.at[g, turn(z, d)], rz.at[g, d - 1], rz_s, rz_r.at[g], dev_k(turn(z, d), core))

    def k_opp(g, n):
        return remote(sz.at[g, turn(z, 2), n], rz.at[g, 2, n], rz_s, rz_r.at[g], dev_k(side(z, n), core))

    def k_near(g, n):
        return remote(sz.at[g, side(z, n), 1 - n], rz.at[g, n, 1 - n], rz_s, rzf_r.at[g], dev_k(side(z, n), core))

    def k_on(g, n):
        return remote(rz.at[g, 2, n], rz.at[g, n, n], rz_s, rzf_r.at[g], dev_k(side(z, n), core))

    def start(copy, g, which=D3):
        for n in which:
            copy(g, n).start()

    barrier = pltpu.get_barrier_semaphore()
    peers = [dev_q(b, turn(a, d)) for d in D3] + [dev_q(turn(b, d), a) for d in D3]
    peers += [dev_k(turn(z, d), core) for d in D3] + [dev_k(z, 1 - core)]
    for p in peers:
        pl.semaphore_signal(barrier, inc=1, device_id={'cp': p}, device_id_type=MESH)
    ins = [(do_hbm, qd.at[slot, 1], 0), (q_hbm, qd.at[slot, 0], 0), (k_hbm, kv.at[core, z, 0], 1),
           (v_hbm, kv.at[core, z, 1], 1), (o_hbm, o_in, 2), (lse_hbm, lse_in, 3)]
    for src, dst, n in ins:
        pltpu.make_async_copy(src, dst, in_s.at[n]).start()
    ld[slot] = jnp.zeros(ld.shape[1:], F32)
    for ref, n in ((qd.at[slot], 0), (kv.at[core, z], 1), (o_in, 2), (lse_in, 3)):
        got(ref, in_s.at[n])

    def split(t):
        hi = t.astype(BF16).astype(F32)
        mid = (t - hi).astype(BF16).astype(F32)
        return hi, mid, t - hi - mid

    with jax.named_scope('own_ld'):
        for j in range(N4):
            rows_j = rows_p(j)
            d_j = jnp.sum(qd[slot, 1, rows_j, :].astype(F32) * o_in[rows_j, :].astype(F32), axis=1, keepdims=True)
            d_j = jnp.broadcast_to(d_j, (KR, KR)).T[:1]
            for n, t in enumerate(split(lse_in[:, rows_j] * (-1.0 / SCALE)) + split(-d_j)):
                ld[slot, j, pl.ds(n, 1), :] = t
    with jax.named_scope('barrier'):
        pl.semaphore_wait(barrier, len(peers))

    def start_a(g):
        for d in D3:
            own_a(q_blk(0, g), qa_s, qa_r.at[g], d).start()

    for d in D3:
        own_a(ld.at[slot], ld_s, lda_r, d).start()
    for d in D3:
        own_a(q_blk(0, NG - 1), qa_s, q7a_r.at[a], d).start()
    start(k_z, 0)
    k_d(0).start()
    for d in D3:
        to_b(ld.at[slot], ld_s, ldb_r, d).start()
    for d in D3:
        to_b(q_blk(0, NG - 1), qb_s, q7_r, d).start()

    def start_k(j, _):
        start(k_z, j)
        k_d(j).start()
        return 0
    lax.fori_loop(1, KQ, start_k, 0)
    qi = lax.broadcasted_iota(jnp.int32, (BQ, 1), 0)
    ki = lax.broadcasted_iota(jnp.int32, (1, BK), 1)
    qpos = (qi & (L - 1)) * 128 + dev_q(qi >> 7, (qi >> 5) & 3)
    kpos = (ki & (L - 1)) * 128 + dev_k((ki >> 5) & 3, ki >> 7)
    thr[0] = jnp.full((BQ, BK), jnp.inf, F32)
    thr[1] = jnp.where(kpos <= qpos, jnp.inf, -jnp.inf).astype(F32)
    ex[...] = jnp.zeros_like(ex)
    ri = lax.broadcasted_iota(jnp.int32, (HD, BK), 0)
    for c in range(NC):
        kt[c, HD:] = jnp.where(ri < 3, 1.0, 0.0).astype(BF16)
        vt[c, HD:] = jnp.where((ri >= 3) & (ri < 6), 1.0, 0.0).astype(BF16)

    def got_a(g):
        got(q_row(0, g, 0, 3), qa_r.at[g])

    def prep_e(i, _):
        for n in range(N4):
            for j in range(N4):
                ex[N4 * i + n, pl.ds(j * KR, KR), pl.ds(0, 8)] = ld[N4 * i + n, j].T.astype(BF16)
        return 0

    def pass_k(j):
        with jax.named_scope('pass_k'):
            got(kv.at[0, pl.ds(0, 3), :, rows_p(0), :], kz_r.at[j])
        start(k_d, j)

    with jax.named_scope('w_lda'):
        got(ld.at[pl.ds(0, 3)], lda_r)
    for n in D3:
        for d in D3:
            to_b(ld.at[b * N4 + turn(a, n)], ld_s, ldb_r, d).start()
    for p in (0, 1, 3, 2):
        @pl.when(a != p)
        def _():
            r = qd.at[b * N4 + p, :, rows_g(NG - 1), :]
            with jax.named_scope('got_a7'):
                got(r, q7a_r.at[p])
            for d in D3:
                to_b(r, qb_s, q7_r, d).start()
    start_a(6)
    dkt[...] = jnp.zeros_like(dkt)
    dvt[...] = jnp.zeros_like(dvt)
    dqt[...] = jnp.zeros_like(dqt)
    pass_k(0)
    with jax.named_scope('w_ldb'):
        got(ld.at[pl.ds(0, 12)], ldb_r)
    with jax.named_scope('prep_e'):
        lax.fori_loop(0, NQ // N4, prep_e, 0)

    def rows_q(which, r):
        return qd[:, which, pl.ds(pl.multiple_of(r * L, L), L), :].reshape(BQ, HD)

    def rows_k(which, c):
        return kv[:, :, which, pl.ds(pl.multiple_of(c * L, L), L), :].reshape(BK, HD)

    def rows_e(r):
        return ex[:, pl.ds(pl.multiple_of(r * L, L), L), :].reshape(BQ, HD)

    def take_k(j):
        with jax.named_scope('take_k'):
            got(kv.at[0, :, :, rows_p(0), :], kd_r.at[j])
        with jax.named_scope('prep_k'):
            for n in range(KR // L):
                c = j * (KR // L) + n
                kt[c, :HD] = rows_k(0, c).T
                vt[c, :HD] = rows_k(1, c).T

    def a_mm(r, c):
        e = rows_e(r)
        return (dg(jnp.concatenate([rows_q(0, r), e], axis=1), kt[c], 1, 0),
                dg(jnp.concatenate([rows_q(1, r), e], axis=1), vt[c], 1, 0))

    def a_vpu(sdp, diag, p_s, ds_s):
        s, dp = sdp
        t = s * (SCALE * LOG2E)
        if diag is not None:
            t = jnp.minimum(t, thr[diag])
        p = jnp.exp2(t)
        p_s[...] = p.astype(BF16)
        ds_s[...] = (p * dp).astype(BF16)

    def b_mm(c, h, p_s, ds_s):
        p, ds = p_s[...], ds_s[...]
        dqt[h] += dg(kt[c, :HD], ds, 1, 1)
        return dg(dot[h], p, 1, 0), dg(qt[h], ds, 1, 0)

    def q_prep(r, h):
        qt[h] = rows_q(0, r).T
        dot[h] = rows_q(1, r).T

    def finish_q(g, h):
        pq[g, :, pl.ds(h * L, L), :] = dqt[h].T.reshape(NQ, L, HD)
        dqt[h] = jnp.zeros((HD, BQ), F32)

    def finish_k(g, h):
        r = 2 * g + h
        pk[g, :, :, 0, pl.ds(h * L, L), :] = dkt[r].T.reshape(2, N4, L, HD)
        pk[g, :, :, 1, pl.ds(h * L, L), :] = dvt[r].T.reshape(2, N4, L, HD)

    def one(c, r0, d0):
        sdp = a_mm(r0, c + 1)
        dv, dk = b_mm(c, 0, p_a, ds_a)
        a_vpu(sdp, d0, p_a, ds_a)
        sdp = a_mm(r0 + 1, c + 1)
        dv1, dk1 = b_mm(c, 1, p_b, ds_b)
        a_vpu(sdp, None, p_b, ds_b)
        dvt[c] += dv + dv1
        dkt[c] += dk + dk1

    def two(c, r0):
        one(c, r0, None)
        one(c + 1, r0, lax.div(c + 2, r0))

    def tail(g, nxt=None):
        r0, r1 = 2 * g, 2 * g + 1
        sdp = a_mm(r1, r1)
        dv, dk = b_mm(r0, 0, p_a, ds_a)
        a_vpu(sdp, 1, p_c, ds_c)
        dv1, dk1 = b_mm(r0, 1, p_b, ds_b)
        dvt[r0] += dv + dv1
        dkt[r0] += dk + dk1
        finish_q(g, 0)
        finish_k(g, 0)
        if nxt is not None:
            sdp = a_mm(2 * nxt, 0)
        dv, dk = b_mm(r1, 1, p_c, ds_c)
        if nxt is not None:
            a_vpu(sdp, lax.div(7 - nxt, 7), p_a, ds_a)
        dvt[r1] += dv
        dkt[r1] += dk
        if nxt is not None:
            sdp = a_mm(2 * nxt + 1, 0)
        finish_q(g, 1)
        finish_k(g, 1)
        if nxt is not None:
            a_vpu(sdp, None, p_b, ds_b)
            q_prep(2 * nxt, 0)
            q_prep(2 * nxt + 1, 1)

    def send_q(g):
        start(r_opp, g, SIDES)
        start(r_near, g, SIDES)

    def relay_q(g):
        with jax.named_scope('relay_q'):
            got(rb.at[g, 2], rb_r.at[g])
            for n in SIDES:
                rb[g, 2, half(n)] = rb[g, 2, half(n)] + pq[g, row(side(b, n), 2 * n, 2)]
        start(r_on, g, SIDES)

    def mid_q(g):
        with jax.named_scope('mid_q'):
            got(rb.at[g, half(0)], rf_r.at[g])
            sa[g] = pq[g, row(b)] + rb[g, 0] + rb[g, 1]
        start(r_a, g)

    def last_q(g):
        with jax.named_scope('last_q'):
            got(rb.at[g], rb_r.at[g])
            sa[g] = pq[g, row(b)] + rb[g, 0] + rb[g, 1] + rb[g, 2]
        start(r_a, g)

    def send_k(g):
        r_d(g).start()

    def sum_k(g):
        with jax.named_scope('sum_k'):
            got(rd.at[g], rd_r.at[g])
            sz[g] = pk[g, core] + rd[g]

    def mid_k(g):
        sum_k(g)
        start(r_z, g)

    def mid_k_by(g):
        sum_k(g)
        start(k_opp, g, SIDES)
        start(k_near, g, SIDES)

    def relay_k(g):
        with jax.named_scope('relay_k'):
            got(rz.at[g, 2], rz_r.at[g])
            for n in SIDES:
                rz[g, 2, n] = rz[g, 2, n] + sz[g, side(z, n), n]
        start(k_on, g, SIDES)

    def end_q(g):
        with jax.named_scope('end_q'):
            got(ra.at[g], ra_r.at[g])
            dq = sa[g, a] + ra[g, 0] + ra[g, 1] + ra[g, 2]
            dq_ref[rows_g(g), :] = (dq * SCALE).astype(BF16)

    def out_k(g, dkv):
        dk_ref[rows_g(g), :] = (dkv[0] * SCALE).astype(BF16)
        dv_ref[rows_g(g), :] = dkv[1].astype(BF16)

    def end_k(g):
        with jax.named_scope('end_k'):
            got(rz.at[g], rz_r.at[g])
            out_k(g, sz[g, z] + rz[g, 0] + rz[g, 1] + rz[g, 2])

    def end_k_by(g):
        with jax.named_scope('end_k_by'):
            got(rz.at[g, half(0)], rzf_r.at[g])
            out_k(g, sz[g, z] + rz[g, 0] + rz[g, 1])

    def pass_q(g):
        with jax.named_scope('pass_q'):
            got(q_row(0, g, 0, 2 * N4), qn_r.at[g])
        start(q_f, g, SIDES)

    def next_q(g):
        with jax.named_scope('next_q'):
            got_a(g)
        start(q_n, g, SIDES)

    take_k(0)
    pass_k(1)
    next_q(SEQ[1])
    with jax.named_scope('first_q'):
        got(q_row(0, NG - 1, 0, 12), q7_r)
    q_prep(NC - 2, 0)
    q_prep(NC - 1, 1)
    start_a(SEQ[2])
    with jax.named_scope('first'):
        a_vpu(a_mm(NC - 2, 0), None, p_a, ds_a)
        a_vpu(a_mm(NC - 1, 0), None, p_b, ds_b)

    def group(i):
        late = lax.div(i + 5, NG)
        return NG - 1 - i + late - 5 * (lax.div(i + 6, NG) - late)

    plan = {}
    for act, args, when in (
        (take_k, (1, 2, 3), TAKE_K),
        (pass_k, (2, 3), PASS_K),
        (pass_q, SEQ[1:], PASS_Q),
        (next_q, SEQ[2:], NEXT_Q),
        (start_a, SEQ[3:], START_A),
        (mid_k, (7, 6, 5, 4), MID_K),
        (mid_k_by, SEQ[5:], MID_K_BY),
        (relay_q, SEQ, RELAY_Q),
        (mid_q, SEQ, MID_Q),
    ):
        for arg, t in zip(args, when):
            plan.setdefault(t, []).append((act, arg))
    early = (pass_q, next_q, start_a)

    def fire(i, j, acts):
        for n in range(NG - 1):
            places = {t % 10: e for t, e in plan.items() if t // 10 == n}
            places = {t: [e for e in es if acts is None or (e[0] in early) == acts] for t, es in places.items()}
            if j is END:
                places = {t: es for t, es in places.items() if t == END and es}
            else:
                places = {t: es for t, es in places.items() if t != END and es}
            if places:
                pl.when(i == n)(functools.partial(at, j, places))

    def at(j, places):
        for t, es in places.items():
            def run(es=es):
                for act, arg in es:
                    act(arg)
            if j is END:
                run()
            else:
                pl.when(j == t)(run)

    def superstep(i, _):
        g = group(i)
        g1 = group(i + 1)
        single = lax.rem(g, 2) + 2 * (lax.div(i + 2, NG) - lax.div(i + 1, NG))

        def pair(j, _):
            fire(i, j, None)
            with jax.named_scope('two'):
                two(2 * j, 2 * g)
            return 0

        def double(j, _):
            fire(i, j + single, None)
            with jax.named_scope('four'):
                c = 2 * single + N4 * j
                two(c, 2 * g)
                two(c + 2, 2 * g)
            return 0
        lax.fori_loop(0, single, pair, 0)
        lax.fori_loop(0, lax.div(g - single, 2), double, 0)
        with jax.named_scope('take_q'):
            got(q_row(0, g1), qf_r.at[g1])
        with jax.named_scope('tail'):
            tail(g, g1)
        fire(i, END, True)
        send_q(g)
        pl.when(i != 2)(functools.partial(send_k, g))
        fire(i, END, False)
        return 0
    lax.fori_loop(0, NG - 1, superstep, 0)

    with jax.named_scope('two'):
        two(0, 2)
    finish_k(0, 0)
    finish_k(0, 1)
    send_k(0)
    mid_k_by(2)
    relay_q(3)
    with jax.named_scope('tail'):
        tail(1)
    start(r_b, 1)
    send_k(1)
    mid_k_by(0)
    relay_k(3)
    mid_k(1)
    relay_q(2)
    mid_q(4)
    mid_q(3)
    for g in (7, 6, 5):
        end_k(g)
        end_q(g)
    end_q(0)
    end_k(4)
    relay_k(2)
    relay_k(0)
    last_q(1)
    mid_q(2)
    end_q(4)
    end_k_by(3)
    end_k_by(2)
    end_q(3)
    end_k_by(0)
    end_k(1)
    end_q(2)
    end_q(1)

    got(ld.at[pl.ds(0, 15)], ld_s)
    got(qd.at[pl.ds(0, 3)], qa_s)
    got(qd.at[pl.ds(0, 12)], qb_s)
    got(kv.at[0, pl.ds(0, 3)], kz_s)
    got(kv.at[0], kd_s)
    got(pq.at[pl.ds(0, 6)], rb_s)
    got(sa.at[pl.ds(0, 6)], ra_s)
    got(rd, rd_s)
    got(rz, rz_s)


def put(*refs):
    sem = refs[6]
    copies = [pltpu.make_async_copy(refs[n], refs[3 + n], sem.at[n]) for n in range(3)]
    for c in copies:
        c.start()
    for c in copies:
        c.wait()


def local(q, k, v, o, dout, lse):
    flat = (ROWS, HD)
    vm = pl.BlockSpec(memory_space=pltpu.VMEM)
    V, DMA = pltpu.VMEM, pltpu.SemaphoreType.DMA
    scratch = [
        V((NQ, 2, ROWS, HD), BF16), V((2, 4, 2, ROWS, HD), BF16), V((NQ, 4, 8, 128), F32),
        V((NQ, ROWS, HD), BF16), V((2, BQ, BK), F32),
        V((NC, 2 * HD, BK), BF16), V((NC, 2 * HD, BK), BF16), V((2, HD, BQ), BF16), V((2, HD, BQ), BF16),
        *[V((BQ, BK), BF16)] * 6,
        V((2, HD, BQ), F32), V((NC, HD, BK), F32), V((NC, HD, BK), F32),
        V((NG, NQ, GR, HD), F32), V((NG, 3, 4, GR, HD), F32), V((NG, 4, GR, HD), F32), V((NG, 3, GR, HD), F32),
        V((NG, 2, 4, 2, GR, HD), F32), V((NG, 4, 2, GR, HD), F32), V((NG, 4, 2, GR, HD), F32),
        V((NG, 3, 2, GR, HD), F32), V((ROWS, HD), BF16), V((1, ROWS), F32),
        DMA((N4,)), *[DMA] * 9,
        DMA, DMA, DMA((NG,)), DMA((N4,)), DMA, DMA((NG,)), DMA((NG,)), DMA((KQ,)), DMA((KQ,)), *[DMA((NG,))] * 6,
    ]
    outs = pl.pallas_call(
        kernel,
        out_shape=[pltpu.VMEM(flat, BF16)] * 3,
        in_specs=[pl.BlockSpec(memory_space=pl.ANY)] * 6, out_specs=[vm] * 3,
        scratch_shapes=scratch,
        compiler_params=pltpu.CompilerParams(collective_id=0, has_side_effects=True, vmem_limit_bytes=62 << 20),
    )(*[t.reshape(flat) for t in (q, k, v, o, dout)], lse)
    outs = pl.pallas_call(
        put,
        out_shape=[jax.ShapeDtypeStruct(flat, BF16)] * 3,
        in_specs=[vm] * 3, out_specs=[pl.BlockSpec(memory_space=pl.ANY)] * 3,
        scratch_shapes=[DMA((3,))],
    )(*[pltpu.with_memory_space_constraint(t, pltpu.VMEM) for t in outs])
    return tuple(t.reshape(ROWS, 1, HD) for t in outs)


def solution(mesh):
    rows = P(('data', 'cp'))
    cols = P(None, ('data', 'cp'))
    return jax.shard_map(local, mesh=mesh, in_specs=(rows, rows, rows, rows, rows, cols),
                         out_specs=(rows, rows, rows), check_vma=False)
```

```python
import functools
import math

import jax
import jax.numpy as jnp
from jax import lax
from jax.experimental import pallas as pl
from jax.experimental.pallas import tpu as pltpu
from jax.sharding import PartitionSpec as P

F32, BF16 = jnp.float32, jnp.bfloat16
MESH = pl.DeviceIdType.MESH
ROWS, HD = 512, 128
L = 32
NC = ROWS // L
NG, GR = 8, 64
NQ, NK = 16, 8
BQ, BK = NQ * L, NK * L
KQ, KR = 4, 128
N4 = 4
TERMS = 24
D3, SIDES = (1, 2, 3), (0, 1)
SCALE = HD ** -0.5
LOG2E = math.log2(math.e)
SEQ = (7, 6, 0, 5, 1, 4, 3, 2)
END = 9
TAKE_K = (1, 2, 3)
PASS_K = (1, 2)
PASS_Q = (3, 9, 11, 19, 31, 32)
NEXT_Q = (2, 3, 9, 11, 12)
START_A = (1, 2, 3, 9)
MID_K = (11, 31, 49, 61)
RELAY_Q = (19, 39, 49, 51, 59)
MID_Q = (39, 59, 60, 61)


def dg(a, b, ca, cb):
    return lax.dot_general(a, b, (((ca,), (cb,)), ((), ())), preferred_element_type=F32)


def kernel(q_hbm, k_hbm, v_hbm, o_hbm, do_hbm, lse_hbm, dq_ref, dk_ref, dv_ref,
           qd, kv, ld, ex, thr, kt, vt, qt, dot, p_a, p_b, p_c, ds_a, ds_b, ds_c, dqt, dkt, dvt,
           pq, rb, sa, ra, pk, rd, sz, rz, o_in, lse_in,
           in_s, ld_s, qa_s, qb_s, kz_s, kd_s, rb_s, ra_s, rd_s, rz_s,
           lda_r, ldb_r, qa_r, q7a_r, q7_r, qn_r, qf_r, kz_r, kd_r, rb_r, rf_r, ra_r, rd_r, rz_r, rzf_r):
    me = lax.axis_index('cp')
    core = lax.rem(me, 2)
    x = lax.rem(lax.div(me, 2), 4)
    y = lax.rem(lax.div(me, 8), 4)
    z = lax.div(me, 32)
    a = x + core * (y - x)
    b = y + core * (x - y)
    step_a, step_b = 2 + 6 * core, 8 - 6 * core

    def dev_q(b_, a_):
        return z * 32 + b_ * step_b + a_ * step_a + core

    def dev_k(z_, c_):
        return z_ * 32 + y * 8 + x * 2 + c_

    def turn(i, d):
        return lax.rem(i + d, N4)

    def remote(src, dst, ss, rs, dev):
        return pltpu.make_async_remote_copy(src_ref=src, dst_ref=dst, send_sem=ss, recv_sem=rs,
                                            device_id={'cp': dev}, device_id_type=MESH)

    def side(i, n):
        return turn(i, 1 + 2 * n)

    def half(n, size=2):
        return pl.ds(2 * n, size)

    def row(b_, n=0, size=N4):
        return pl.ds(b_ * N4 + n, size)

    slot = b * N4 + a

    def rows_g(g):
        return pl.ds(pl.multiple_of(g * GR, GR), GR)

    def got(ref, sem):
        pltpu.make_async_copy(ref, ref, sem).wait()

    def own_a(src, ss, rs, d):
        return remote(src, src, ss, rs, dev_q(b, turn(a, d)))

    def to_b(src, ss, rs, d):
        return remote(src, src, ss, rs, dev_q(turn(b, d), a))

    def q_blk(n, g):
        return qd.at[b * N4 + turn(a, n), :, rows_g(g), :]

    def q_row(b_, g, n=0, size=N4):
        return qd.at[row(b_, n, size), :, rows_g(g), :]

    def q_n(g, n):
        return remote(q_row(b, g), q_row(b, g), qb_s, qn_r.at[g], dev_q(side(b, n), a))

    def q_f(g, n):
        r = q_row(side(b, 1 - n), g, 2 * n, 2)
        return remote(r, r, qb_s, qf_r.at[g], dev_q(side(b, n), a))

    def rows_p(j):
        return pl.ds(pl.multiple_of(j * KR, KR), KR)

    def k_z(j, d):
        r = kv.at[core, z, :, rows_p(j), :]
        return remote(r, r, kz_s, kz_r.at[j], dev_k(turn(z, d), core))

    def k_d(j, d=0):
        r = kv.at[core, turn(z, N4 - d), :, rows_p(j), :]
        return remote(r, r, kd_s, kd_r.at[j], dev_k(z, 1 - core))

    def r_b(g, d):
        return remote(pq.at[g, row(turn(b, d))], rb.at[g, d - 1], rb_s, rb_r.at[g], dev_q(turn(b, d), a))

    def r_opp(g, n):
        return remote(pq.at[g, row(turn(b, 2), 2 * n, 2)], rb.at[g, 2, half(n)], rb_s, rb_r.at[g], dev_q(side(b, n), a))

    def r_near(g, n):
        return remote(pq.at[g, row(side(b, n), 2 - 2 * n, 2)], rb.at[g, n, half(1 - n)], rb_s, rf_r.at[g],
                      dev_q(side(b, n), a))

    def r_on(g, n):
        return remote(rb.at[g, 2, half(n)], rb.at[g, n, half(n)], rb_s, rf_r.at[g], dev_q(side(b, n), a))

    def r_a(g, d):
        return remote(sa.at[g, turn(a, d)], ra.at[g, d - 1], ra_s, ra_r.at[g], dev_q(b, turn(a, d)))

    def r_d(g):
        return remote(pk.at[g, 1 - core], rd.at[g], rd_s, rd_r.at[g], dev_k(z, 1 - core))

    def r_z(g, d):
        return remote(sz.at[g, turn(z, d)], rz.at[g, d - 1], rz_s, rz_r.at[g], dev_k(turn(z, d), core))

    def k_opp(g, n):
        return remote(sz.at[g, turn(z, 2), n], rz.at[g, 2, n], rz_s, rz_r.at[g], dev_k(side(z, n), core))

    def k_near(g, n):
        return remote(sz.at[g, side(z, n), 1 - n], rz.at[g, n, 1 - n], rz_s, rzf_r.at[g], dev_k(side(z, n), core))

    def k_on(g, n):
        return remote(rz.at[g, 2, n], rz.at[g, n, n], rz_s, rzf_r.at[g], dev_k(side(z, n), core))

    def start(copy, g, which=D3):
        for n in which:
            copy(g, n).start()

    barrier = pltpu.get_barrier_semaphore()
    peers = [dev_q(b, turn(a, d)) for d in D3] + [dev_q(turn(b, d), a) for d in D3]
    peers += [dev_k(turn(z, d), core) for d in D3] + [dev_k(z, 1 - core)]
    for p in peers:
        pl.semaphore_signal(barrier, inc=1, device_id={'cp': p}, device_id_type=MESH)
    ins = [(do_hbm, qd.at[slot, 1], 0), (q_hbm, qd.at[slot, 0], 0), (k_hbm, kv.at[core, z, 0], 1),
           (v_hbm, kv.at[core, z, 1], 1), (o_hbm, o_in, 2), (lse_hbm, lse_in, 3)]
    for src, dst, n in ins:
        pltpu.make_async_copy(src, dst, in_s.at[n]).start()
    for ref, n in ((qd.at[slot], 0), (kv.at[core, z], 1), (o_in, 2), (lse_in, 3)):
        got(ref, in_s.at[n])

    with jax.named_scope('own_ld'):
        for j in range(N4):
            rows_j = rows_p(j)
            d_j = jnp.sum(qd[slot, 1, rows_j, :].astype(F32) * o_in[rows_j, :].astype(F32), axis=1, keepdims=True)
            ld[slot, pl.ds(j, 1), :] = lse_in[:, rows_j] * (-1.0 / SCALE)
            ld[slot, pl.ds(N4 + j, 1), :] = -jnp.broadcast_to(d_j, (KR, KR)).T[:1]
    with jax.named_scope('barrier'):
        pl.semaphore_wait(barrier, len(peers))

    def start_a(g):
        for d in D3:
            own_a(q_blk(0, g), qa_s, qa_r.at[g], d).start()

    for d in D3:
        own_a(ld.at[slot], ld_s, lda_r, d).start()
    start(k_z, 0)
    for d in D3:
        own_a(q_blk(0, NG - 1), qa_s, q7a_r.at[a], d).start()
    k_d(0).start()
    for d in D3:
        to_b(ld.at[slot], ld_s, ldb_r, d).start()
    for d in D3:
        to_b(q_blk(0, NG - 1), qb_s, q7_r, d).start()

    start_a(SEQ[1])
    start_a(SEQ[2])

    def start_k(j, _):
        start(k_z, j)
        k_d(j).start()
        return 0
    lax.fori_loop(1, KQ, start_k, 0)
    qi = lax.broadcasted_iota(jnp.int32, (BQ, 1), 0)
    ki = lax.broadcasted_iota(jnp.int32, (1, BK), 1)
    qpos = (qi & (L - 1)) * 128 + dev_q(qi >> 7, (qi >> 5) & 3)
    kpos = (ki & (L - 1)) * 128 + dev_k((ki >> 5) & 3, ki >> 7)
    thr[0] = jnp.full((BQ, BK), jnp.inf, F32)
    thr[1] = jnp.where(kpos <= qpos, jnp.inf, -jnp.inf).astype(F32)
    ex[...] = jnp.zeros_like(ex)
    ri = lax.broadcasted_iota(jnp.int32, (HD, BK), 0)
    of_d = ((ri >> 2) & 1) == 1
    for c in range(NC):
        kt[c, HD:] = jnp.where((ri < TERMS) & ~of_d, 1.0, 0.0).astype(BF16)
        vt[c, HD:] = jnp.where((ri < TERMS) & of_d, 1.0, 0.0).astype(BF16)

    def got_a(g):
        got(q_row(0, g, 0, 3), qa_r.at[g])

    def prep_e(i, _):
        for n in range(N4):
            t = ld[N4 * i + n]
            hi = t.astype(BF16).astype(F32)
            mid = (t - hi).astype(BF16).astype(F32)
            terms = jnp.concatenate([hi, mid, t - hi - mid], axis=0).T
            quarter = lax.broadcasted_iota(jnp.int32, terms.shape, 1) & 3
            for j in range(N4):
                ex[N4 * i + n, rows_p(j), pl.ds(0, TERMS)] = jnp.where(quarter == j, terms, 0.0).astype(BF16)
        return 0

    def pass_k(j):
        with jax.named_scope('pass_k'):
            got(kv.at[0, pl.ds(0, 3), :, rows_p(0), :], kz_r.at[j])
        start(k_d, j)

    with jax.named_scope('w_lda'):
        got(ld.at[pl.ds(0, 3)], lda_r)
    for n in D3:
        for d in D3:
            to_b(ld.at[b * N4 + turn(a, n)], ld_s, ldb_r, d).start()
    for p in (0, 1, 3, 2):
        @pl.when(a != p)
        def _():
            r = qd.at[b * N4 + p, :, rows_g(NG - 1), :]
            with jax.named_scope('got_a7'):
                got(r, q7a_r.at[p])
            for d in D3:
                to_b(r, qb_s, q7_r, d).start()
    dkt[...] = jnp.zeros_like(dkt)
    dvt[...] = jnp.zeros_like(dvt)
    dqt[...] = jnp.zeros_like(dqt)
    pass_k(0)
    with jax.named_scope('w_ldb'):
        got(ld.at[pl.ds(0, 12)], ldb_r)
    with jax.named_scope('prep_e'):
        lax.fori_loop(0, NQ // N4, prep_e, 0)

    def rows_q(which, r):
        return qd[:, which, pl.ds(pl.multiple_of(r * L, L), L), :].reshape(BQ, HD)

    def rows_k(which, c):
        return kv[:, :, which, pl.ds(pl.multiple_of(c * L, L), L), :].reshape(BK, HD)

    def rows_e(r):
        return ex[:, pl.ds(pl.multiple_of(r * L, L), L), :].reshape(BQ, HD)

    def take_k(j):
        with jax.named_scope('take_k'):
            got(kv.at[0, :, :, rows_p(0), :], kd_r.at[j])
        with jax.named_scope('prep_k'):
            for n in range(KR // L):
                c = j * (KR // L) + n
                kt[c, :HD] = rows_k(0, c).T
                vt[c, :HD] = rows_k(1, c).T

    def a_mm(r, c):
        e = rows_e(r)
        return (dg(jnp.concatenate([rows_q(0, r), e], axis=1), kt[c], 1, 0),
                dg(jnp.concatenate([rows_q(1, r), e], axis=1), vt[c], 1, 0))

    def a_vpu(sdp, diag, p_s, ds_s):
        s, dp = sdp
        t = s * (SCALE * LOG2E)
        if diag is not None:
            t = jnp.minimum(t, thr[diag])
        p = jnp.exp2(t)
        p_s[...] = p.astype(BF16)
        ds_s[...] = (p * dp).astype(BF16)

    def b_mm(c, h, p_s, ds_s):
        p, ds = p_s[...], ds_s[...]
        dqt[h] += dg(kt[c, :HD], ds, 1, 1)
        return dg(dot[h], p, 1, 0), dg(qt[h], ds, 1, 0)

    def q_prep(r, h):
        qt[h] = rows_q(0, r).T
        dot[h] = rows_q(1, r).T

    def finish_q(g, h):
        pq[g, :, pl.ds(h * L, L), :] = dqt[h].T.reshape(NQ, L, HD)
        dqt[h] = jnp.zeros((HD, BQ), F32)

    def finish_k(g, h):
        r = 2 * g + h
        pk[g, :, :, 0, pl.ds(h * L, L), :] = dkt[r].T.reshape(2, N4, L, HD)
        pk[g, :, :, 1, pl.ds(h * L, L), :] = dvt[r].T.reshape(2, N4, L, HD)

    def one(c, r0, d0):
        sdp = a_mm(r0, c + 1)
        dv, dk = b_mm(c, 0, p_a, ds_a)
        a_vpu(sdp, d0, p_a, ds_a)
        sdp = a_mm(r0 + 1, c + 1)
        dv1, dk1 = b_mm(c, 1, p_b, ds_b)
        a_vpu(sdp, None, p_b, ds_b)
        dvt[c] += dv + dv1
        dkt[c] += dk + dk1

    def two(c, r0):
        one(c, r0, None)
        one(c + 1, r0, lax.div(c + 2, r0))

    def tail(g, nxt=None):
        r0, r1 = 2 * g, 2 * g + 1
        sdp = a_mm(r1, r1)
        dv, dk = b_mm(r0, 0, p_a, ds_a)
        a_vpu(sdp, 1, p_c, ds_c)
        dv1, dk1 = b_mm(r0, 1, p_b, ds_b)
        dvt[r0] += dv + dv1
        dkt[r0] += dk + dk1
        finish_q(g, 0)
        finish_k(g, 0)
        if nxt is not None:
            sdp = a_mm(2 * nxt, 0)
        dv, dk = b_mm(r1, 1, p_c, ds_c)
        if nxt is not None:
            a_vpu(sdp, lax.div(7 - nxt, 7), p_a, ds_a)
        dvt[r1] += dv
        dkt[r1] += dk
        if nxt is not None:
            sdp = a_mm(2 * nxt + 1, 0)
        finish_q(g, 1)
        finish_k(g, 1)
        if nxt is not None:
            a_vpu(sdp, None, p_b, ds_b)
            q_prep(2 * nxt, 0)
            q_prep(2 * nxt + 1, 1)

    def send_q(g):
        start(r_opp, g, SIDES)
        start(r_near, g, SIDES)

    def relay_q(g):
        with jax.named_scope('relay_q'):
            got(rb.at[g, 2], rb_r.at[g])
            for n in SIDES:
                rb[g, 2, half(n)] = rb[g, 2, half(n)] + pq[g, row(side(b, n), 2 * n, 2)]
        start(r_on, g, SIDES)

    def mid_q(g):
        with jax.named_scope('mid_q'):
            got(rb.at[g, half(0)], rf_r.at[g])
            sa[g] = pq[g, row(b)] + rb[g, 0] + rb[g, 1]
        start(r_a, g)

    def last_q(g):
        with jax.named_scope('last_q'):
            got(rb.at[g], rb_r.at[g])
            sa[g] = pq[g, row(b)] + rb[g, 0] + rb[g, 1] + rb[g, 2]
        start(r_a, g)

    def send_k(g):
        r_d(g).start()

    def sum_k(g):
        with jax.named_scope('sum_k'):
            got(rd.at[g], rd_r.at[g])
            sz[g] = pk[g, core] + rd[g]

    def mid_k(g):
        sum_k(g)
        start(r_z, g)

    def mid_k_by(g):
        sum_k(g)
        start(k_opp, g, SIDES)
        start(k_near, g, SIDES)

    def relay_k(g):
        with jax.named_scope('relay_k'):
            got(rz.at[g, 2], rz_r.at[g])
            for n in SIDES:
                rz[g, 2, n] = rz[g, 2, n] + sz[g, side(z, n), n]
        start(k_on, g, SIDES)

    def end_q(g):
        with jax.named_scope('end_q'):
            got(ra.at[g], ra_r.at[g])
            dq = sa[g, a] + ra[g, 0] + ra[g, 1] + ra[g, 2]
            dq_ref[rows_g(g), :] = (dq * SCALE).astype(BF16)

    def out_k(g, dkv):
        dk_ref[rows_g(g), :] = (dkv[0] * SCALE).astype(BF16)
        dv_ref[rows_g(g), :] = dkv[1].astype(BF16)

    def end_k(g):
        with jax.named_scope('end_k'):
            got(rz.at[g], rz_r.at[g])
            out_k(g, sz[g, z] + rz[g, 0] + rz[g, 1] + rz[g, 2])

    def end_k_by(g):
        with jax.named_scope('end_k_by'):
            got(rz.at[g, half(0)], rzf_r.at[g])
            out_k(g, sz[g, z] + rz[g, 0] + rz[g, 1])

    def pass_q(g):
        with jax.named_scope('pass_q'):
            got(q_row(0, g, 0, 2 * N4), qn_r.at[g])
        start(q_f, g, SIDES)

    def next_q(g):
        with jax.named_scope('next_q'):
            got_a(g)
        start(q_n, g, SIDES)

    take_k(0)
    got_a(SEQ[1])
    for d in D3:
        to_b(q_row(b, SEQ[1]), qb_s, qf_r.at[SEQ[1]], d).start()
    with jax.named_scope('first_q'):
        got(q_row(0, NG - 1, 0, 12), q7_r)
    q_prep(NC - 2, 0)
    q_prep(NC - 1, 1)
    next_q(SEQ[2])
    start_a(SEQ[3])
    with jax.named_scope('first'):
        a_vpu(a_mm(NC - 2, 0), None, p_a, ds_a)
        a_vpu(a_mm(NC - 1, 0), None, p_b, ds_b)
    pass_k(1)

    def group(i):
        return SEQ[0] + sum((SEQ[n] - SEQ[n - 1]) * lax.div(i + NG - n, NG) for n in range(1, NG))

    plan = {}
    for act, args, when in (
        (take_k, (1, 2, 3), TAKE_K),
        (pass_k, (2, 3), PASS_K),
        (pass_q, SEQ[2:], PASS_Q),
        (next_q, SEQ[3:], NEXT_Q),
        (start_a, SEQ[4:], START_A),
        (mid_k, (7, 6, 5, 4), MID_K),
        (relay_q, SEQ, RELAY_Q),
        (mid_q, SEQ, MID_Q),
    ):
        for arg, t in zip(args, when):
            plan.setdefault(t, []).append((act, arg))
    early = (pass_q, next_q, start_a)

    def fire(i, j, acts):
        for n in range(NG - 1):
            places = {t % 10: e for t, e in plan.items() if t // 10 == n}
            places = {t: [e for e in es if acts is None or (e[0] in early) == acts] for t, es in places.items()}
            if j is END:
                places = {t: es for t, es in places.items() if t == END and es}
            else:
                places = {t: es for t, es in places.items() if t != END and es}
            if places:
                pl.when(i == n)(functools.partial(at, j, places))

    def at(j, places):
        for t, es in places.items():
            def run(es=es):
                for act, arg in es:
                    act(arg)
            if j is END:
                run()
            else:
                pl.when(j == t)(run)

    def superstep(i, _):
        g = group(i)
        g1 = group(i + 1)
        single = lax.rem(g, 2)

        def pair(j, _):
            fire(i, j, None)
            with jax.named_scope('two'):
                two(2 * j, 2 * g)
            return 0

        def four(j):
            c = 2 * single + N4 * j
            two(c, 2 * g)
            two(c + 2, 2 * g)

        def double(j, _):
            fire(i, j + single, None)
            with jax.named_scope('four'):
                four(j)
            return 0

        def last():
            with jax.named_scope('take_q'):
                pl.when(i == 0)(lambda: got(q_row(0, g1, 0, 12), qf_r.at[g1]))
                pl.when(i > 0)(lambda: got(q_row(0, g1), qf_r.at[g1]))

        fours = lax.div(g - single, 2)
        lax.fori_loop(0, single, pair, 0)
        lax.fori_loop(0, fours - 1, double, 0)

        @pl.when(fours > 0)
        def _():
            fire(i, fours - 1 + single, None)
            last()
            with jax.named_scope('fourtail'):
                four(fours - 1)
                tail(g, g1)

        @pl.when(fours == 0)
        def _():
            last()
            with jax.named_scope('tail'):
                tail(g, g1)
        fire(i, END, True)
        pl.when(i <= N4)(functools.partial(send_q, g))
        pl.when(i > N4)(functools.partial(start, r_b, g))
        pl.when((i != SEQ.index(0)) & (i != SEQ.index(1)))(functools.partial(send_k, g))
        fire(i, END, False)
        return 0
    lax.fori_loop(0, NG - 1, superstep, 0)

    def close(g):
        with jax.named_scope('two'):
            two(2 * g, N4)
        for h in SIDES:
            finish_k(g, h)
        send_k(g)

    close(0)
    mid_k_by(3)
    close(1)
    mid_k_by(0)
    mid_q(1)
    last_q(4)
    with jax.named_scope('tail'):
        tail(2)
    start(r_b, 2)
    send_k(2)
    mid_k_by(1)
    mid_k(2)
    relay_k(3)
    relay_k(0)
    last_q(3)
    relay_k(1)
    for g in (7, 6, 5):
        end_k(g)
        end_q(g)
    end_q(0)
    end_q(1)
    end_k(4)
    last_q(2)
    end_k_by(3)
    end_q(4)
    end_q(3)
    end_k_by(0)
    end_k_by(1)
    end_k(2)
    end_q(2)

    got(ld.at[pl.ds(0, 15)], ld_s)
    got(qd.at[pl.ds(0, 3)], qa_s)
    got(qd.at[pl.ds(0, 12)], qb_s)
    got(kv.at[0, pl.ds(0, 3)], kz_s)
    got(kv.at[0], kd_s)
    got(pq.at[pl.ds(0, 6)], rb_s)
    got(sa.at[pl.ds(0, 6)], ra_s)
    got(rd, rd_s)
    got(rz, rz_s)


def put(*refs):
    sem = refs[6]
    copies = [pltpu.make_async_copy(refs[n], refs[3 + n], sem.at[n]) for n in range(3)]
    for c in copies:
        c.start()
    for c in copies:
        c.wait()


def local(q, k, v, o, dout, lse):
    flat = (ROWS, HD)
    vm = pl.BlockSpec(memory_space=pltpu.VMEM)
    V, DMA = pltpu.VMEM, pltpu.SemaphoreType.DMA
    scratch = [
        V((NQ, 2, ROWS, HD), BF16), V((2, 4, 2, ROWS, HD), BF16), V((NQ, 8, 128), F32),
        V((NQ, ROWS, HD), BF16), V((2, BQ, BK), F32),
        V((NC, 2 * HD, BK), BF16), V((NC, 2 * HD, BK), BF16), V((2, HD, BQ), BF16), V((2, HD, BQ), BF16),
        *[V((BQ, BK), BF16)] * 6,
        V((2, HD, BQ), F32), V((NC, HD, BK), F32), V((NC, HD, BK), F32),
        V((NG, NQ, GR, HD), F32), V((NG, 3, 4, GR, HD), F32), V((NG, 4, GR, HD), F32), V((NG, 3, GR, HD), F32),
        V((NG, 2, 4, 2, GR, HD), F32), V((NG, 4, 2, GR, HD), F32), V((NG, 4, 2, GR, HD), F32),
        V((NG, 3, 2, GR, HD), F32), V((ROWS, HD), BF16), V((1, ROWS), F32),
        DMA((N4,)), *[DMA] * 9,
        DMA, DMA, DMA((NG,)), DMA((N4,)), DMA, DMA((NG,)), DMA((NG,)), DMA((KQ,)), DMA((KQ,)), *[DMA((NG,))] * 6,
    ]
    outs = pl.pallas_call(
        kernel,
        out_shape=[pltpu.VMEM(flat, BF16)] * 3,
        in_specs=[pl.BlockSpec(memory_space=pl.ANY)] * 6, out_specs=[vm] * 3,
        scratch_shapes=scratch,
        compiler_params=pltpu.CompilerParams(collective_id=0, has_side_effects=True, vmem_limit_bytes=62 << 20),
    )(*[t.reshape(flat) for t in (q, k, v, o, dout)], lse)
    outs = pl.pallas_call(
        put,
        out_shape=[jax.ShapeDtypeStruct(flat, BF16)] * 3,
        in_specs=[vm] * 3, out_specs=[pl.BlockSpec(memory_space=pl.ANY)] * 3,
        scratch_shapes=[DMA((3,))],
    )(*[pltpu.with_memory_space_constraint(t, pltpu.VMEM) for t in outs])
    return tuple(t.reshape(ROWS, 1, HD) for t in outs)


def solution(mesh):
    rows = P(('data', 'cp'))
    cols = P(None, ('data', 'cp'))
    return jax.shard_map(local, mesh=mesh, in_specs=(rows, rows, rows, rows, rows, cols),
                         out_specs=(rows, rows, rows), check_vma=False)
```

```python
import functools
import math

import jax
import jax.numpy as jnp
from jax import lax
from jax.experimental import pallas as pl
from jax.experimental.pallas import tpu as pltpu
from jax.sharding import PartitionSpec as P

F32, BF16 = jnp.float32, jnp.bfloat16
MESH = pl.DeviceIdType.MESH
ROWS, HD = 512, 128
L = 32
NC = ROWS // L
NG, GR = 8, 64
NQ, NK = 16, 8
BQ, BK = NQ * L, NK * L
KQ, KR = 4, 128
N4 = 4
TERMS = 24
D3, SIDES = (1, 2, 3), (0, 1)
SCALE = HD ** -0.5
LOG2E = math.log2(math.e)
SEQ = (7, 6, 0, 5, 1, 4, 3, 2)
END = 9
TAKE_K = (1, 2, 3)
PASS_K = (1, 2)
PASS_Q = (3, 10, 11, 19, 31, 32)
NEXT_Q = (2, 3, 9, 11, 12)
START_A = (1, 2, 3, 10)
MID_K = (11, 31, 50, 61)
RELAY_Q = (19, 40, 49, 51, 59)
MID_Q = (40, 59, 60, 61)


def dg(a, b, ca, cb):
    return lax.dot_general(a, b, (((ca,), (cb,)), ((), ())), preferred_element_type=F32)


def kernel(q_hbm, k_hbm, v_hbm, o_hbm, do_hbm, lse_hbm, dq_ref, dk_ref, dv_ref,
           qd, kv, ld, ex, thr, kt, vt, qt, dot, p_a, p_b, p_c, ds_a, ds_b, ds_c, dqt, dkt, dvt,
           pq, rb, sa, ra, pk, rd, sz, rz, o_in, lse_in,
           in_s, ld_s, qa_s, qb_s, kz_s, kd_s, rb_s, ra_s, rd_s, rz_s,
           lda_r, ldb_r, qa_r, q7a_r, q7_r, qn_r, qf_r, kz_r, kd_r, rb_r, rf_r, ra_r, rd_r, rz_r, rzf_r):
    me = lax.axis_index('cp')
    core = lax.rem(me, 2)
    x = lax.rem(lax.div(me, 2), 4)
    y = lax.rem(lax.div(me, 8), 4)
    z = lax.div(me, 32)
    a = x + core * (y - x)
    b = y + core * (x - y)
    step_a, step_b = 2 + 6 * core, 8 - 6 * core

    def dev_q(b_, a_):
        return z * 32 + b_ * step_b + a_ * step_a + core

    def dev_k(z_, c_):
        return z_ * 32 + y * 8 + x * 2 + c_

    def turn(i, d):
        return lax.rem(i + d, N4)

    def remote(src, dst, ss, rs, dev):
        return pltpu.make_async_remote_copy(src_ref=src, dst_ref=dst, send_sem=ss, recv_sem=rs,
                                            device_id={'cp': dev}, device_id_type=MESH)

    def side(i, n):
        return turn(i, 1 + 2 * n)

    def half(n, size=2):
        return pl.ds(2 * n, size)

    def row(b_, n=0, size=N4):
        return pl.ds(b_ * N4 + n, size)

    slot = b * N4 + a

    def rows_g(g):
        return pl.ds(pl.multiple_of(g * GR, GR), GR)

    def got(ref, sem):
        pltpu.make_async_copy(ref, ref, sem).wait()

    def own_a(src, ss, rs, d):
        return remote(src, src, ss, rs, dev_q(b, turn(a, d)))

    def to_b(src, ss, rs, d):
        return remote(src, src, ss, rs, dev_q(turn(b, d), a))

    def q_blk(n, g):
        return qd.at[b * N4 + turn(a, n), :, rows_g(g), :]

    def q_row(b_, g, n=0, size=N4):
        return qd.at[row(b_, n, size), :, rows_g(g), :]

    def q_n(g, n):
        return remote(q_row(b, g), q_row(b, g), qb_s, qn_r.at[g], dev_q(side(b, n), a))

    def q_f(g, n):
        r = q_row(side(b, 1 - n), g, 2 * n, 2)
        return remote(r, r, qb_s, qf_r.at[g], dev_q(side(b, n), a))

    def rows_p(j):
        return pl.ds(pl.multiple_of(j * KR, KR), KR)

    def k_z(j, d):
        r = kv.at[core, z, :, rows_p(j), :]
        return remote(r, r, kz_s, kz_r.at[j], dev_k(turn(z, d), core))

    def k_d(j, d=0):
        r = kv.at[core, turn(z, N4 - d), :, rows_p(j), :]
        return remote(r, r, kd_s, kd_r.at[j], dev_k(z, 1 - core))

    def r_b(g, d):
        return remote(pq.at[g, row(turn(b, d))], rb.at[g, d - 1], rb_s, rb_r.at[g], dev_q(turn(b, d), a))

    def r_opp(g, n):
        return remote(pq.at[g, row(turn(b, 2), 2 * n, 2)], rb.at[g, 2, half(n)], rb_s, rb_r.at[g], dev_q(side(b, n), a))

    def r_near(g, n):
        return remote(pq.at[g, row(side(b, n), 2 - 2 * n, 2)], rb.at[g, n, half(1 - n)], rb_s, rf_r.at[g],
                      dev_q(side(b, n), a))

    def r_on(g, n):
        return remote(rb.at[g, 2, half(n)], rb.at[g, n, half(n)], rb_s, rf_r.at[g], dev_q(side(b, n), a))

    def r_a(g, d):
        return remote(sa.at[g, turn(a, d)], ra.at[g, d - 1], ra_s, ra_r.at[g], dev_q(b, turn(a, d)))

    def r_d(g):
        return remote(pk.at[g, 1 - core], rd.at[g], rd_s, rd_r.at[g], dev_k(z, 1 - core))

    def r_z(g, d):
        return remote(sz.at[g, turn(z, d)], rz.at[g, d - 1], rz_s, rz_r.at[g], dev_k(turn(z, d), core))

    def k_opp(g, n):
        return remote(sz.at[g, turn(z, 2), n], rz.at[g, 2, n], rz_s, rz_r.at[g], dev_k(side(z, n), core))

    def k_near(g, n):
        return remote(sz.at[g, side(z, n), 1 - n], rz.at[g, n, 1 - n], rz_s, rzf_r.at[g], dev_k(side(z, n), core))

    def k_on(g, n):
        return remote(rz.at[g, 2, n], rz.at[g, n, n], rz_s, rzf_r.at[g], dev_k(side(z, n), core))

    def start(copy, g, which=D3):
        for n in which:
            copy(g, n).start()

    barrier = pltpu.get_barrier_semaphore()
    peers = [dev_q(b, turn(a, d)) for d in D3] + [dev_q(turn(b, d), a) for d in D3]
    peers += [dev_k(turn(z, d), core) for d in D3] + [dev_k(z, 1 - core)]
    for p in peers:
        pl.semaphore_signal(barrier, inc=1, device_id={'cp': p}, device_id_type=MESH)
    ins = [(do_hbm, qd.at[slot, 1], 0), (q_hbm, qd.at[slot, 0], 0), (k_hbm, kv.at[core, z, 0], 1),
           (v_hbm, kv.at[core, z, 1], 1), (o_hbm, o_in, 2), (lse_hbm, lse_in, 3)]
    for src, dst, n in ins:
        pltpu.make_async_copy(src, dst, in_s.at[n]).start()
    for ref, n in ((qd.at[slot], 0), (kv.at[core, z], 1), (o_in, 2), (lse_in, 3)):
        got(ref, in_s.at[n])

    with jax.named_scope('own_ld'):
        for j in range(N4):
            rows_j = rows_p(j)
            d_j = jnp.sum(qd[slot, 1, rows_j, :].astype(F32) * o_in[rows_j, :].astype(F32), axis=1, keepdims=True)
            ld[slot, pl.ds(j, 1), :] = lse_in[:, rows_j] * (-1.0 / SCALE)
            ld[slot, pl.ds(N4 + j, 1), :] = -jnp.broadcast_to(d_j, (KR, KR)).T[:1]
    with jax.named_scope('barrier'):
        pl.semaphore_wait(barrier, len(peers))

    def start_a(g):
        for d in D3:
            own_a(q_blk(0, g), qa_s, qa_r.at[g], d).start()

    for d in D3:
        own_a(ld.at[slot], ld_s, lda_r, d).start()
    start(k_z, 0)
    for d in D3:
        own_a(q_blk(0, NG - 1), qa_s, q7a_r.at[a], d).start()
    k_d(0).start()
    for d in D3:
        to_b(ld.at[slot], ld_s, ldb_r, d).start()
    for d in D3:
        to_b(q_blk(0, NG - 1), qb_s, q7_r, d).start()

    start_a(SEQ[1])
    start_a(SEQ[2])

    def start_k(j, _):
        start(k_z, j)
        k_d(j).start()
        return 0
    lax.fori_loop(1, KQ, start_k, 0)
    qi = lax.broadcasted_iota(jnp.int32, (BQ, 1), 0)
    ki = lax.broadcasted_iota(jnp.int32, (1, BK), 1)
    qpos = (qi & (L - 1)) * 128 + dev_q(qi >> 7, (qi >> 5) & 3)
    kpos = (ki & (L - 1)) * 128 + dev_k((ki >> 5) & 3, ki >> 7)
    thr[0] = jnp.full((BQ, BK), jnp.inf, F32)
    thr[1] = jnp.where(kpos <= qpos, jnp.inf, -jnp.inf).astype(F32)
    ex[...] = jnp.zeros_like(ex)
    ri = lax.broadcasted_iota(jnp.int32, (HD, BK), 0)
    of_d = ((ri >> 2) & 1) == 1
    for c in range(NC):
        kt[c, HD:] = jnp.where((ri < TERMS) & ~of_d, 1.0, 0.0).astype(BF16)
        vt[c, HD:] = jnp.where((ri < TERMS) & of_d, 1.0, 0.0).astype(BF16)

    def got_a(g):
        got(q_row(0, g, 0, 3), qa_r.at[g])

    def prep_e(i, _):
        for n in range(N4):
            t = ld[N4 * i + n]
            hi = t.astype(BF16).astype(F32)
            mid = (t - hi).astype(BF16).astype(F32)
            terms = jnp.concatenate([hi, mid, t - hi - mid], axis=0).T
            quarter = lax.broadcasted_iota(jnp.int32, terms.shape, 1) & 3
            for j in range(N4):
                ex[N4 * i + n, rows_p(j), pl.ds(0, TERMS)] = jnp.where(quarter == j, terms, 0.0).astype(BF16)
        return 0

    def pass_k(j):
        with jax.named_scope('pass_k'):
            got(kv.at[0, pl.ds(0, 3), :, rows_p(0), :], kz_r.at[j])
        start(k_d, j)

    with jax.named_scope('w_lda'):
        got(ld.at[pl.ds(0, 3)], lda_r)
    for n in D3:
        for d in D3:
            to_b(ld.at[b * N4 + turn(a, n)], ld_s, ldb_r, d).start()
    for p in (0, 1, 3, 2):
        @pl.when(a != p)
        def _():
            r = qd.at[b * N4 + p, :, rows_g(NG - 1), :]
            with jax.named_scope('got_a7'):
                got(r, q7a_r.at[p])
            for d in D3:
                to_b(r, qb_s, q7_r, d).start()
    dkt[...] = jnp.zeros_like(dkt)
    dvt[...] = jnp.zeros_like(dvt)
    dqt[...] = jnp.zeros_like(dqt)
    pass_k(0)
    with jax.named_scope('w_ldb'):
        got(ld.at[pl.ds(0, 12)], ldb_r)
    with jax.named_scope('prep_e'):
        lax.fori_loop(0, NQ // N4, prep_e, 0)

    def rows_q(which, r):
        return qd[:, which, pl.ds(pl.multiple_of(r * L, L), L), :].reshape(BQ, HD)

    def rows_k(which, c):
        return kv[:, :, which, pl.ds(pl.multiple_of(c * L, L), L), :].reshape(BK, HD)

    def rows_e(r):
        return ex[:, pl.ds(pl.multiple_of(r * L, L), L), :].reshape(BQ, HD)

    def take_k(j):
        with jax.named_scope('take_k'):
            got(kv.at[0, :, :, rows_p(0), :], kd_r.at[j])
        with jax.named_scope('prep_k'):
            for n in range(KR // L):
                c = j * (KR // L) + n
                kt[c, :HD] = rows_k(0, c).T
                vt[c, :HD] = rows_k(1, c).T

    def a_mm(r, c):
        e = rows_e(r)
        return (dg(jnp.concatenate([rows_q(0, r), e], axis=1), kt[c], 1, 0),
                dg(jnp.concatenate([rows_q(1, r), e], axis=1), vt[c], 1, 0))

    def a_vpu(sdp, diag, p_s, ds_s):
        s, dp = sdp
        t = s * (SCALE * LOG2E)
        if diag is not None:
            t = jnp.minimum(t, thr[diag])
        p = jnp.exp2(t)
        p_s[...] = p.astype(BF16)
        ds_s[...] = (p * dp).astype(BF16)

    def b_mm(c, h, p_s, ds_s):
        p, ds = p_s[...], ds_s[...]
        dqt[h] += dg(kt[c, :HD], ds, 1, 1)
        return dg(dot[h], p, 1, 0), dg(qt[h], ds, 1, 0)

    def q_prep(r, h):
        qt[h] = rows_q(0, r).T
        dot[h] = rows_q(1, r).T

    def finish_q(g, h):
        pq[g, :, pl.ds(h * L, L), :] = dqt[h].T.reshape(NQ, L, HD)
        dqt[h] = jnp.zeros((HD, BQ), F32)

    def finish_k(g, h):
        r = 2 * g + h
        pk[g, :, :, 0, pl.ds(h * L, L), :] = dkt[r].T.reshape(2, N4, L, HD)
        pk[g, :, :, 1, pl.ds(h * L, L), :] = dvt[r].T.reshape(2, N4, L, HD)

    def one(c, r0, d0):
        sdp = a_mm(r0, c + 1)
        dv, dk = b_mm(c, 0, p_a, ds_a)
        a_vpu(sdp, d0, p_a, ds_a)
        sdp = a_mm(r0 + 1, c + 1)
        dv1, dk1 = b_mm(c, 1, p_b, ds_b)
        a_vpu(sdp, None, p_b, ds_b)
        dvt[c] += dv + dv1
        dkt[c] += dk + dk1

    def two(c, r0):
        one(c, r0, None)
        one(c + 1, r0, lax.div(c + 2, r0))

    def tail(g, nxt=None):
        r0, r1 = 2 * g, 2 * g + 1
        sdp = a_mm(r1, r1)
        dv, dk = b_mm(r0, 0, p_a, ds_a)
        a_vpu(sdp, 1, p_c, ds_c)
        dv1, dk1 = b_mm(r0, 1, p_b, ds_b)
        dvt[r0] += dv + dv1
        dkt[r0] += dk + dk1
        finish_q(g, 0)
        finish_k(g, 0)
        if nxt is not None:
            sdp = a_mm(2 * nxt, 0)
        dv, dk = b_mm(r1, 1, p_c, ds_c)
        if nxt is not None:
            a_vpu(sdp, lax.div(7 - nxt, 7), p_a, ds_a)
        dvt[r1] += dv
        dkt[r1] += dk
        if nxt is not None:
            sdp = a_mm(2 * nxt + 1, 0)
        finish_q(g, 1)
        finish_k(g, 1)
        if nxt is not None:
            a_vpu(sdp, None, p_b, ds_b)
            q_prep(2 * nxt, 0)
            q_prep(2 * nxt + 1, 1)

    def send_q(g):
        start(r_opp, g, SIDES)
        start(r_near, g, SIDES)

    def relay_q(g):
        with jax.named_scope('relay_q'):
            got(rb.at[g, 2], rb_r.at[g])
            for n in SIDES:
                rb[g, 2, half(n)] = rb[g, 2, half(n)] + pq[g, row(side(b, n), 2 * n, 2)]
        start(r_on, g, SIDES)

    def mid_q(g):
        with jax.named_scope('mid_q'):
            got(rb.at[g, half(0)], rf_r.at[g])
            sa[g] = pq[g, row(b)] + rb[g, 0] + rb[g, 1]
        start(r_a, g)

    def last_q(g):
        with jax.named_scope('last_q'):
            got(rb.at[g], rb_r.at[g])
            sa[g] = pq[g, row(b)] + rb[g, 0] + rb[g, 1] + rb[g, 2]
        start(r_a, g)

    def send_k(g):
        r_d(g).start()

    def sum_k(g):
        with jax.named_scope('sum_k'):
            got(rd.at[g], rd_r.at[g])
            sz[g] = pk[g, core] + rd[g]

    def mid_k(g):
        sum_k(g)
        start(r_z, g)

    def mid_k_by(g):
        sum_k(g)
        start(k_opp, g, SIDES)
        start(k_near, g, SIDES)

    def relay_k(g):
        with jax.named_scope('relay_k'):
            got(rz.at[g, 2], rz_r.at[g])
            for n in SIDES:
                rz[g, 2, n] = rz[g, 2, n] + sz[g, side(z, n), n]
        start(k_on, g, SIDES)

    def end_q(g):
        with jax.named_scope('end_q'):
            got(ra.at[g], ra_r.at[g])
            dq = sa[g, a] + ra[g, 0] + ra[g, 1] + ra[g, 2]
            dq_ref[rows_g(g), :] = (dq * SCALE).astype(BF16)

    def out_k(g, dkv):
        dk_ref[rows_g(g), :] = (dkv[0] * SCALE).astype(BF16)
        dv_ref[rows_g(g), :] = dkv[1].astype(BF16)

    def end_k(g):
        with jax.named_scope('end_k'):
            got(rz.at[g], rz_r.at[g])
            out_k(g, sz[g, z] + rz[g, 0] + rz[g, 1] + rz[g, 2])

    def end_k_by(g):
        with jax.named_scope('end_k_by'):
            got(rz.at[g, half(0)], rzf_r.at[g])
            out_k(g, sz[g, z] + rz[g, 0] + rz[g, 1])

    def pass_q(g):
        with jax.named_scope('pass_q'):
            got(q_row(0, g, 0, 2 * N4), qn_r.at[g])
        start(q_f, g, SIDES)

    def next_q(g):
        with jax.named_scope('next_q'):
            got_a(g)
        start(q_n, g, SIDES)

    take_k(0)
    got_a(SEQ[1])
    for d in D3:
        to_b(q_row(b, SEQ[1]), qb_s, qf_r.at[SEQ[1]], d).start()
    with jax.named_scope('first_q'):
        got(q_row(0, NG - 1, 0, 12), q7_r)
    q_prep(NC - 2, 0)
    q_prep(NC - 1, 1)
    next_q(SEQ[2])
    start_a(SEQ[3])
    with jax.named_scope('first'):
        a_vpu(a_mm(NC - 2, 0), None, p_a, ds_a)
        a_vpu(a_mm(NC - 1, 0), None, p_b, ds_b)
    pass_k(1)

    def group(i):
        return SEQ[0] + sum((SEQ[n] - SEQ[n - 1]) * lax.div(i + NG - n, NG) for n in range(1, NG))

    plan = {}
    for act, args, when in (
        (take_k, (1, 2, 3), TAKE_K),
        (pass_k, (2, 3), PASS_K),
        (pass_q, SEQ[2:], PASS_Q),
        (next_q, SEQ[3:], NEXT_Q),
        (start_a, SEQ[4:], START_A),
        (mid_k, (7, 6, 5, 4), MID_K),
        (relay_q, SEQ, RELAY_Q),
        (mid_q, SEQ, MID_Q),
    ):
        for arg, t in zip(args, when):
            plan.setdefault(t, []).append((act, arg))
    early = (pass_q, next_q, start_a, relay_q)

    def fire(i, j, acts):
        for n in range(NG - 1):
            places = {t % 10: e for t, e in plan.items() if t // 10 == n}
            places = {t: [e for e in es if acts is None or (e[0] in early) == acts] for t, es in places.items()}
            if j is END:
                places = {t: es for t, es in places.items() if t == END and es}
            else:
                places = {t: es for t, es in places.items() if t != END and es}
            if places:
                pl.when(i == n)(functools.partial(at, j, places))

    def at(j, places):
        for t, es in places.items():
            def run(es=es):
                for act, arg in es:
                    act(arg)
            if j is END:
                run()
            else:
                pl.when(j == t)(run)

    def superstep(i, _):
        g = group(i)
        g1 = group(i + 1)
        single = lax.rem(g, 2)

        def pair(j, _):
            fire(i, j, None)
            with jax.named_scope('two'):
                two(2 * j, 2 * g)
            return 0

        def four(j):
            c = 2 * single + N4 * j
            two(c, 2 * g)
            two(c + 2, 2 * g)

        def double(j, _):
            fire(i, j + single, None)
            with jax.named_scope('four'):
                four(j)
            return 0

        def last():
            with jax.named_scope('take_q'):
                pl.when(i == 0)(lambda: got(q_row(0, g1, 0, 12), qf_r.at[g1]))
                pl.when(i > 0)(lambda: got(q_row(0, g1), qf_r.at[g1]))

        fours = lax.div(g - single, 2)
        lax.fori_loop(0, single, pair, 0)
        lax.fori_loop(0, fours - 1, double, 0)

        @pl.when(fours > 0)
        def _():
            fire(i, fours - 1 + single, None)
            last()
            with jax.named_scope('fourtail'):
                four(fours - 1)
                tail(g, g1)

        @pl.when(fours == 0)
        def _():
            last()
            with jax.named_scope('tail'):
                tail(g, g1)
        fire(i, END, True)
        pl.when(i <= N4)(functools.partial(send_q, g))
        pl.when(i > N4)(functools.partial(start, r_b, g))
        pl.when((i != SEQ.index(0)) & (i != SEQ.index(1)))(functools.partial(send_k, g))
        fire(i, END, False)
        return 0
    lax.fori_loop(0, NG - 1, superstep, 0)

    def close(g):
        with jax.named_scope('two'):
            two(2 * g, N4)
        for h in SIDES:
            finish_k(g, h)
        send_k(g)

    close(0)
    mid_k_by(3)
    close(1)
    mid_q(1)
    mid_k_by(0)
    with jax.named_scope('tail'):
        tail(2)
    start(r_b, 2)
    send_k(2)
    mid_k_by(1)
    mid_k(2)
    relay_k(3)
    relay_k(1)
    relay_k(0)
    last_q(4)
    last_q(3)
    for g in (7, 6, 5):
        end_k(g)
        end_q(g)
    end_q(0)
    end_q(1)
    end_k(4)
    last_q(2)
    end_q(4)
    end_k_by(3)
    end_q(3)
    end_k_by(0)
    end_k(2)
    end_k_by(1)
    end_q(2)

    got(ld.at[pl.ds(0, 15)], ld_s)
    got(qd.at[pl.ds(0, 3)], qa_s)
    got(qd.at[pl.ds(0, 12)], qb_s)
    got(kv.at[0, pl.ds(0, 3)], kz_s)
    got(kv.at[0], kd_s)
    got(pq.at[pl.ds(0, 6)], rb_s)
    got(sa.at[pl.ds(0, 6)], ra_s)
    got(rd, rd_s)
    got(rz, rz_s)


def put(*refs):
    sem = refs[6]
    copies = [pltpu.make_async_copy(refs[n], refs[3 + n], sem.at[n]) for n in range(3)]
    for c in copies:
        c.start()
    for c in copies:
        c.wait()


def local(q, k, v, o, dout, lse):
    flat = (ROWS, HD)
    vm = pl.BlockSpec(memory_space=pltpu.VMEM)
    V, DMA = pltpu.VMEM, pltpu.SemaphoreType.DMA
    scratch = [
        V((NQ, 2, ROWS, HD), BF16), V((2, 4, 2, ROWS, HD), BF16), V((NQ, 8, 128), F32),
        V((NQ, ROWS, HD), BF16), V((2, BQ, BK), F32),
        V((NC, 2 * HD, BK), BF16), V((NC, 2 * HD, BK), BF16), V((2, HD, BQ), BF16), V((2, HD, BQ), BF16),
        *[V((BQ, BK), BF16)] * 6,
        V((2, HD, BQ), F32), V((NC, HD, BK), F32), V((NC, HD, BK), F32),
        V((NG, NQ, GR, HD), F32), V((NG, 3, 4, GR, HD), F32), V((NG, 4, GR, HD), F32), V((NG, 3, GR, HD), F32),
        V((NG, 2, 4, 2, GR, HD), F32), V((NG, 4, 2, GR, HD), F32), V((NG, 4, 2, GR, HD), F32),
        V((NG, 3, 2, GR, HD), F32), V((ROWS, HD), BF16), V((1, ROWS), F32),
        DMA((N4,)), *[DMA] * 9,
        DMA, DMA, DMA((NG,)), DMA((N4,)), DMA, DMA((NG,)), DMA((NG,)), DMA((KQ,)), DMA((KQ,)), *[DMA((NG,))] * 6,
    ]
    outs = pl.pallas_call(
        kernel,
        out_shape=[pltpu.VMEM(flat, BF16)] * 3,
        in_specs=[pl.BlockSpec(memory_space=pl.ANY)] * 6, out_specs=[vm] * 3,
        scratch_shapes=scratch,
        compiler_params=pltpu.CompilerParams(collective_id=0, has_side_effects=True, vmem_limit_bytes=62 << 20),
    )(*[t.reshape(flat) for t in (q, k, v, o, dout)], lse)
    outs = pl.pallas_call(
        put,
        out_shape=[jax.ShapeDtypeStruct(flat, BF16)] * 3,
        in_specs=[vm] * 3, out_specs=[pl.BlockSpec(memory_space=pl.ANY)] * 3,
        scratch_shapes=[DMA((3,))],
    )(*[pltpu.with_memory_space_constraint(t, pltpu.VMEM) for t in outs])
    return tuple(t.reshape(ROWS, 1, HD) for t in outs)


def solution(mesh):
    rows = P(('data', 'cp'))
    cols = P(None, ('data', 'cp'))
    return jax.shard_map(local, mesh=mesh, in_specs=(rows, rows, rows, rows, rows, cols),
                         out_specs=(rows, rows, rows), check_vma=False)
```

```python
import functools
import math

import jax
import jax.numpy as jnp
from jax import lax
from jax.experimental import pallas as pl
from jax.experimental.pallas import tpu as pltpu
from jax.sharding import PartitionSpec as P

F32, BF16 = jnp.float32, jnp.bfloat16
MESH = pl.DeviceIdType.MESH
ROWS, HD = 512, 128
L = 32
NC = ROWS // L
NG, GR = 8, 64
NQ, NK = 16, 8
BQ, BK = NQ * L, NK * L
KQ, KR = 4, 128
N4 = 4
TERMS = 24
D3, SIDES = (1, 2, 3), (0, 1)
SCALE = HD ** -0.5
LOG2E = math.log2(math.e)
SEQ = (7, 6, 0, 5, 1, 4, 3, 2)
END = 9
TAKE_K = (1, 2, 3)
PASS_K = (1, 2)
PASS_Q = (9, 10, 11, 19, 31, 32)
NEXT_Q = (2, 3, 9, 11, 12)
START_A = (1, 2, 3, 10)
MID_K = (11, 31, 51, 61)
RELAY_Q = (19, 40, 49, 51, 59)
MID_Q = (40, 59, 60, 61)


def dg(a, b, ca, cb):
    return lax.dot_general(a, b, (((ca,), (cb,)), ((), ())), preferred_element_type=F32)


def kernel(q_hbm, k_hbm, v_hbm, o_hbm, do_hbm, lse_hbm, dq_ref, dk_ref, dv_ref,
           qd, kv, ld, ex, thr, kt, vt, qt, dot, p_a, p_b, p_c, ds_a, ds_b, ds_c, dqt, dkt, dvt,
           pq, rb, sa, ra, pk, rd, sz, rz, o_in, lse_in,
           in_s, ld_s, qa_s, qb_s, kz_s, kd_s, rb_s, ra_s, rd_s, rz_s,
           lda_r, ldb_r, qa_r, q7a_r, q7_r, qn_r, qf_r, kz_r, kd_r, rb_r, rf_r, ra_r, rd_r, rz_r, rzf_r):
    me = lax.axis_index('cp')
    core = lax.rem(me, 2)
    x = lax.rem(lax.div(me, 2), 4)
    y = lax.rem(lax.div(me, 8), 4)
    z = lax.div(me, 32)
    a = x + core * (y - x)
    b = y + core * (x - y)
    step_a, step_b = 2 + 6 * core, 8 - 6 * core

    def dev_q(b_, a_):
        return z * 32 + b_ * step_b + a_ * step_a + core

    def dev_k(z_, c_):
        return z_ * 32 + y * 8 + x * 2 + c_

    def turn(i, d):
        return lax.rem(i + d, N4)

    def remote(src, dst, ss, rs, dev):
        return pltpu.make_async_remote_copy(src_ref=src, dst_ref=dst, send_sem=ss, recv_sem=rs,
                                            device_id={'cp': dev}, device_id_type=MESH)

    def side(i, n):
        return turn(i, 1 + 2 * n)

    def half(n, size=2):
        return pl.ds(2 * n, size)

    def row(b_, n=0, size=N4):
        return pl.ds(b_ * N4 + n, size)

    slot = b * N4 + a

    def rows_g(g):
        return pl.ds(pl.multiple_of(g * GR, GR), GR)

    def got(ref, sem):
        pltpu.make_async_copy(ref, ref, sem).wait()

    def own_a(src, ss, rs, d):
        return remote(src, src, ss, rs, dev_q(b, turn(a, d)))

    def to_b(src, ss, rs, d):
        return remote(src, src, ss, rs, dev_q(turn(b, d), a))

    def q_blk(n, g):
        return qd.at[b * N4 + turn(a, n), :, rows_g(g), :]

    def q_row(b_, g, n=0, size=N4):
        return qd.at[row(b_, n, size), :, rows_g(g), :]

    def q_n(g, n):
        return remote(q_row(b, g), q_row(b, g), qb_s, qn_r.at[g], dev_q(side(b, n), a))

    def q_f(g, n):
        r = q_row(side(b, 1 - n), g, 2 * n, 2)
        return remote(r, r, qb_s, qf_r.at[g], dev_q(side(b, n), a))

    def rows_p(j):
        return pl.ds(pl.multiple_of(j * KR, KR), KR)

    def k_z(j, d):
        r = kv.at[core, z, :, rows_p(j), :]
        return remote(r, r, kz_s, kz_r.at[j], dev_k(turn(z, d), core))

    def k_d(j, d=0):
        r = kv.at[core, turn(z, N4 - d), :, rows_p(j), :]
        return remote(r, r, kd_s, kd_r.at[j], dev_k(z, 1 - core))

    def r_b(g, d):
        return remote(pq.at[g, row(turn(b, d))], rb.at[g, d - 1], rb_s, rb_r.at[g], dev_q(turn(b, d), a))

    def r_opp(g, n):
        return remote(pq.at[g, row(turn(b, 2), 2 * n, 2)], rb.at[g, 2, half(n)], rb_s, rb_r.at[g], dev_q(side(b, n), a))

    def r_near(g, n):
        return remote(pq.at[g, row(side(b, n), 2 - 2 * n, 2)], rb.at[g, n, half(1 - n)], rb_s, rf_r.at[g],
                      dev_q(side(b, n), a))

    def r_on(g, n):
        return remote(rb.at[g, 2, half(n)], rb.at[g, n, half(n)], rb_s, rf_r.at[g], dev_q(side(b, n), a))

    def r_a(g, d):
        return remote(sa.at[g, turn(a, d)], ra.at[g, d - 1], ra_s, ra_r.at[g], dev_q(b, turn(a, d)))

    def r_d(g):
        return remote(pk.at[g, 1 - core], rd.at[g], rd_s, rd_r.at[g], dev_k(z, 1 - core))

    def r_z(g, d):
        return remote(sz.at[g, turn(z, d)], rz.at[g, d - 1], rz_s, rz_r.at[g], dev_k(turn(z, d), core))

    def k_opp(g, n):
        return remote(sz.at[g, turn(z, 2), n], rz.at[g, 2, n], rz_s, rz_r.at[g], dev_k(side(z, n), core))

    def k_near(g, n):
        return remote(sz.at[g, side(z, n), 1 - n], rz.at[g, n, 1 - n], rz_s, rzf_r.at[g], dev_k(side(z, n), core))

    def k_on(g, n):
        return remote(rz.at[g, 2, n], rz.at[g, n, n], rz_s, rzf_r.at[g], dev_k(side(z, n), core))

    def start(copy, g, which=D3):
        for n in which:
            copy(g, n).start()

    barrier = pltpu.get_barrier_semaphore()
    peers = [dev_q(b, turn(a, d)) for d in D3] + [dev_q(turn(b, d), a) for d in D3]
    peers += [dev_k(turn(z, d), core) for d in D3] + [dev_k(z, 1 - core)]
    for p in peers:
        pl.semaphore_signal(barrier, inc=1, device_id={'cp': p}, device_id_type=MESH)
    ins = [(do_hbm, qd.at[slot, 1], 0), (q_hbm, qd.at[slot, 0], 0), (k_hbm, kv.at[core, z, 0], 1),
           (v_hbm, kv.at[core, z, 1], 1), (o_hbm, o_in, 2), (lse_hbm, lse_in, 3)]
    for src, dst, n in ins:
        pltpu.make_async_copy(src, dst, in_s.at[n]).start()
    for ref, n in ((qd.at[slot], 0), (kv.at[core, z], 1), (o_in, 2), (lse_in, 3)):
        got(ref, in_s.at[n])

    with jax.named_scope('own_ld'):
        for j in range(N4):
            rows_j = rows_p(j)
            d_j = jnp.sum(qd[slot, 1, rows_j, :].astype(F32) * o_in[rows_j, :].astype(F32), axis=1, keepdims=True)
            ld[slot, pl.ds(j, 1), :] = lse_in[:, rows_j] * (-1.0 / SCALE)
            ld[slot, pl.ds(N4 + j, 1), :] = -jnp.broadcast_to(d_j, (KR, KR)).T[:1]
    with jax.named_scope('barrier'):
        pl.semaphore_wait(barrier, len(peers))

    def start_a(g):
        for d in D3:
            own_a(q_blk(0, g), qa_s, qa_r.at[g], d).start()

    for d in D3:
        own_a(ld.at[slot], ld_s, lda_r, d).start()
    start(k_z, 0)
    for d in D3:
        own_a(q_blk(0, NG - 1), qa_s, q7a_r.at[a], d).start()
    k_d(0).start()
    for d in D3:
        to_b(ld.at[slot], ld_s, ldb_r, d).start()
    for d in D3:
        to_b(q_blk(0, NG - 1), qb_s, q7_r, d).start()


    def start_k(j, _):
        start(k_z, j)
        k_d(j).start()
        return 0
    lax.fori_loop(1, KQ, start_k, 0)
    qi = lax.broadcasted_iota(jnp.int32, (BQ, 1), 0)
    ki = lax.broadcasted_iota(jnp.int32, (1, BK), 1)
    qpos = (qi & (L - 1)) * 128 + dev_q(qi >> 7, (qi >> 5) & 3)
    kpos = (ki & (L - 1)) * 128 + dev_k((ki >> 5) & 3, ki >> 7)
    thr[0] = jnp.full((BQ, BK), jnp.inf, F32)
    thr[1] = jnp.where(kpos <= qpos, jnp.inf, -jnp.inf).astype(F32)
    ex[...] = jnp.zeros_like(ex)
    ri = lax.broadcasted_iota(jnp.int32, (HD, BK), 0)
    of_d = ((ri >> 2) & 1) == 1
    for c in range(NC):
        kt[c, HD:] = jnp.where((ri < TERMS) & ~of_d, 1.0, 0.0).astype(BF16)
        vt[c, HD:] = jnp.where((ri < TERMS) & of_d, 1.0, 0.0).astype(BF16)

    def got_a(g):
        got(q_row(0, g, 0, 3), qa_r.at[g])

    def prep_e(i, _):
        for n in range(N4):
            t = ld[N4 * i + n]
            hi = t.astype(BF16).astype(F32)
            mid = (t - hi).astype(BF16).astype(F32)
            terms = jnp.concatenate([hi, mid, t - hi - mid], axis=0).T
            quarter = lax.broadcasted_iota(jnp.int32, terms.shape, 1) & 3
            for j in range(N4):
                ex[N4 * i + n, rows_p(j), pl.ds(0, TERMS)] = jnp.where(quarter == j, terms, 0.0).astype(BF16)
        return 0

    def pass_k(j):
        with jax.named_scope('pass_k'):
            got(kv.at[0, pl.ds(0, 3), :, rows_p(0), :], kz_r.at[j])
        start(k_d, j)

    with jax.named_scope('w_lda'):
        got(ld.at[pl.ds(0, 3)], lda_r)
    for n in D3:
        for d in D3:
            to_b(ld.at[b * N4 + turn(a, n)], ld_s, ldb_r, d).start()
    for p in (0, 1, 3, 2):
        @pl.when(a != p)
        def _():
            r = qd.at[b * N4 + p, :, rows_g(NG - 1), :]
            with jax.named_scope('got_a7'):
                got(r, q7a_r.at[p])
            for d in D3:
                to_b(r, qb_s, q7_r, d).start()
    start_a(SEQ[1])
    start_a(SEQ[2])
    dkt[...] = jnp.zeros_like(dkt)
    dvt[...] = jnp.zeros_like(dvt)
    dqt[...] = jnp.zeros_like(dqt)
    pass_k(0)
    with jax.named_scope('w_ldb'):
        got(ld.at[pl.ds(0, 12)], ldb_r)
    with jax.named_scope('prep_e'):
        lax.fori_loop(0, NQ // N4, prep_e, 0)

    def rows_q(which, r):
        return qd[:, which, pl.ds(pl.multiple_of(r * L, L), L), :].reshape(BQ, HD)

    def rows_k(which, c):
        return kv[:, :, which, pl.ds(pl.multiple_of(c * L, L), L), :].reshape(BK, HD)

    def rows_e(r):
        return ex[:, pl.ds(pl.multiple_of(r * L, L), L), :].reshape(BQ, HD)

    def take_k(j):
        with jax.named_scope('take_k'):
            got(kv.at[0, :, :, rows_p(0), :], kd_r.at[j])
        with jax.named_scope('prep_k'):
            for n in range(KR // L):
                c = j * (KR // L) + n
                kt[c, :HD] = rows_k(0, c).T
                vt[c, :HD] = rows_k(1, c).T

    def a_mm(r, c):
        e = rows_e(r)
        return (dg(jnp.concatenate([rows_q(0, r), e], axis=1), kt[c], 1, 0),
                dg(jnp.concatenate([rows_q(1, r), e], axis=1), vt[c], 1, 0))

    def a_vpu(sdp, diag, p_s, ds_s):
        s, dp = sdp
        t = s * (SCALE * LOG2E)
        if diag is not None:
            t = jnp.minimum(t, thr[diag])
        p = jnp.exp2(t)
        p_s[...] = p.astype(BF16)
        ds_s[...] = (p * dp).astype(BF16)

    def b_mm(c, h, p_s, ds_s):
        p, ds = p_s[...], ds_s[...]
        dqt[h] += dg(kt[c, :HD], ds, 1, 1)
        return dg(dot[h], p, 1, 0), dg(qt[h], ds, 1, 0)

    def q_prep(r, h):
        qt[h] = rows_q(0, r).T
        dot[h] = rows_q(1, r).T

    def finish_q(g, h):
        pq[g, :, pl.ds(h * L, L), :] = dqt[h].T.reshape(NQ, L, HD)
        dqt[h] = jnp.zeros((HD, BQ), F32)

    def finish_k(g, h):
        r = 2 * g + h
        pk[g, :, :, 0, pl.ds(h * L, L), :] = dkt[r].T.reshape(2, N4, L, HD)
        pk[g, :, :, 1, pl.ds(h * L, L), :] = dvt[r].T.reshape(2, N4, L, HD)

    def one(c, r0, d0):
        sdp = a_mm(r0, c + 1)
        dv, dk = b_mm(c, 0, p_a, ds_a)
        a_vpu(sdp, d0, p_a, ds_a)
        sdp = a_mm(r0 + 1, c + 1)
        dv1, dk1 = b_mm(c, 1, p_b, ds_b)
        a_vpu(sdp, None, p_b, ds_b)
        dvt[c] += dv + dv1
        dkt[c] += dk + dk1

    def two(c, r0):
        one(c, r0, None)
        one(c + 1, r0, lax.div(c + 2, r0))

    def tail(g, nxt=None):
        r0, r1 = 2 * g, 2 * g + 1
        sdp = a_mm(r1, r1)
        dv, dk = b_mm(r0, 0, p_a, ds_a)
        a_vpu(sdp, 1, p_c, ds_c)
        dv1, dk1 = b_mm(r0, 1, p_b, ds_b)
        dvt[r0] += dv + dv1
        dkt[r0] += dk + dk1
        finish_q(g, 0)
        finish_k(g, 0)
        if nxt is not None:
            sdp = a_mm(2 * nxt, 0)
        dv, dk = b_mm(r1, 1, p_c, ds_c)
        if nxt is not None:
            a_vpu(sdp, lax.div(7 - nxt, 7), p_a, ds_a)
        dvt[r1] += dv
        dkt[r1] += dk
        if nxt is not None:
            sdp = a_mm(2 * nxt + 1, 0)
        finish_q(g, 1)
        finish_k(g, 1)
        if nxt is not None:
            a_vpu(sdp, None, p_b, ds_b)
            q_prep(2 * nxt, 0)
            q_prep(2 * nxt + 1, 1)

    def send_q(g):
        start(r_opp, g, SIDES)
        start(r_near, g, SIDES)

    def relay_q(g):
        with jax.named_scope('relay_q'):
            got(rb.at[g, 2], rb_r.at[g])
            for n in SIDES:
                rb[g, 2, half(n)] = rb[g, 2, half(n)] + pq[g, row(side(b, n), 2 * n, 2)]
        start(r_on, g, SIDES)

    def mid_q(g):
        with jax.named_scope('mid_q'):
            got(rb.at[g, half(0)], rf_r.at[g])
            sa[g] = pq[g, row(b)] + rb[g, 0] + rb[g, 1]
        start(r_a, g)

    def last_q(g):
        with jax.named_scope('last_q'):
            got(rb.at[g], rb_r.at[g])
            sa[g] = pq[g, row(b)] + rb[g, 0] + rb[g, 1] + rb[g, 2]
        start(r_a, g)

    def send_k(g):
        r_d(g).start()

    def sum_k(g):
        with jax.named_scope('sum_k'):
            got(rd.at[g], rd_r.at[g])
            sz[g] = pk[g, core] + rd[g]

    def mid_k(g):
        sum_k(g)
        start(r_z, g)

    def mid_k_by(g):
        sum_k(g)
        start(k_opp, g, SIDES)
        start(k_near, g, SIDES)

    def relay_k(g):
        with jax.named_scope('relay_k'):
            got(rz.at[g, 2], rz_r.at[g])
            for n in SIDES:
                rz[g, 2, n] = rz[g, 2, n] + sz[g, side(z, n), n]
        start(k_on, g, SIDES)

    def end_q(g):
        with jax.named_scope('end_q'):
            got(ra.at[g], ra_r.at[g])
            dq = sa[g, a] + ra[g, 0] + ra[g, 1] + ra[g, 2]
            dq_ref[rows_g(g), :] = (dq * SCALE).astype(BF16)

    def out_k(g, dkv):
        dk_ref[rows_g(g), :] = (dkv[0] * SCALE).astype(BF16)
        dv_ref[rows_g(g), :] = dkv[1].astype(BF16)

    def end_k(g):
        with jax.named_scope('end_k'):
            got(rz.at[g], rz_r.at[g])
            out_k(g, sz[g, z] + rz[g, 0] + rz[g, 1] + rz[g, 2])

    def end_k_by(g):
        with jax.named_scope('end_k_by'):
            got(rz.at[g, half(0)], rzf_r.at[g])
            out_k(g, sz[g, z] + rz[g, 0] + rz[g, 1])

    def pass_q(g):
        with jax.named_scope('pass_q'):
            got(q_row(0, g, 0, 2 * N4), qn_r.at[g])
        start(q_f, g, SIDES)

    def next_q(g):
        with jax.named_scope('next_q'):
            got_a(g)
        start(q_n, g, SIDES)

    take_k(0)
    got_a(SEQ[1])
    for d in D3:
        to_b(q_row(b, SEQ[1]), qb_s, qf_r.at[SEQ[1]], d).start()
    with jax.named_scope('first_q'):
        got(q_row(0, NG - 1, 0, 12), q7_r)
    pass_k(1)
    q_prep(NC - 2, 0)
    q_prep(NC - 1, 1)
    next_q(SEQ[2])
    start_a(SEQ[3])
    with jax.named_scope('first'):
        a_vpu(a_mm(NC - 2, 0), None, p_a, ds_a)
        a_vpu(a_mm(NC - 1, 0), None, p_b, ds_b)

    def group(i):
        return SEQ[0] + sum((SEQ[n] - SEQ[n - 1]) * lax.div(i + NG - n, NG) for n in range(1, NG))

    plan = {}
    for act, args, when in (
        (take_k, (1, 2, 3), TAKE_K),
        (pass_k, (2, 3), PASS_K),
        (pass_q, SEQ[2:], PASS_Q),
        (next_q, SEQ[3:], NEXT_Q),
        (start_a, SEQ[4:], START_A),
        (mid_k, (7, 6, 5, 4), MID_K),
        (relay_q, SEQ, RELAY_Q),
        (mid_q, SEQ, MID_Q),
    ):
        for arg, t in zip(args, when):
            plan.setdefault(t, []).append((act, arg))
    early = (pass_q, next_q, start_a, relay_q)

    def fire(i, j, acts):
        for n in range(NG - 1):
            places = {t % 10: e for t, e in plan.items() if t // 10 == n}
            places = {t: [e for e in es if acts is None or (e[0] in early) == acts] for t, es in places.items()}
            if j is END:
                places = {t: es for t, es in places.items() if t == END and es}
            else:
                places = {t: es for t, es in places.items() if t != END and es}
            if places:
                pl.when(i == n)(functools.partial(at, j, places))

    def at(j, places):
        for t, es in places.items():
            def run(es=es):
                for act, arg in es:
                    act(arg)
            if j is END:
                run()
            else:
                pl.when(j == t)(run)

    def superstep(i, _):
        g = group(i)
        g1 = group(i + 1)
        single = lax.rem(g, 2)

        def pair(j, _):
            fire(i, j, None)
            with jax.named_scope('two'):
                two(2 * j, 2 * g)
            return 0

        def four(j):
            c = 2 * single + N4 * j
            two(c, 2 * g)
            two(c + 2, 2 * g)

        def double(j, _):
            fire(i, j + single, None)
            with jax.named_scope('four'):
                four(j)
            return 0

        def last():
            with jax.named_scope('take_q'):
                pl.when(i == 0)(lambda: got(q_row(0, g1, 0, 12), qf_r.at[g1]))
                pl.when(i > 0)(lambda: got(q_row(0, g1), qf_r.at[g1]))

        fours = lax.div(g - single, 2)
        lax.fori_loop(0, single, pair, 0)
        lax.fori_loop(0, fours - 1, double, 0)

        @pl.when(fours > 0)
        def _():
            fire(i, fours - 1 + single, None)
            last()
            with jax.named_scope('fourtail'):
                four(fours - 1)
                tail(g, g1)

        @pl.when(fours == 0)
        def _():
            last()
            with jax.named_scope('tail'):
                tail(g, g1)
        fire(i, END, True)
        pl.when(i <= N4)(functools.partial(send_q, g))
        pl.when(i > N4)(functools.partial(start, r_b, g))
        pl.when((i != SEQ.index(0)) & (i != SEQ.index(1)))(functools.partial(send_k, g))
        fire(i, END, False)
        return 0
    lax.fori_loop(0, NG - 1, superstep, 0)

    def close(g):
        with jax.named_scope('two'):
            two(2 * g, N4)
        for h in SIDES:
            finish_k(g, h)
        send_k(g)

    close(0)
    mid_k_by(3)
    close(1)
    mid_q(1)
    mid_k_by(0)
    with jax.named_scope('tail'):
        tail(2)
    start(r_b, 2)
    send_k(2)
    mid_k_by(1)
    mid_k(2)
    relay_k(3)
    relay_k(1)
    relay_k(0)
    last_q(4)
    last_q(3)
    for g in (7, 6, 5):
        end_k(g)
        end_q(g)
    end_q(0)
    end_q(1)
    end_k(4)
    last_q(2)
    end_q(4)
    end_k_by(3)
    end_q(3)
    end_k_by(0)
    end_k(2)
    end_k_by(1)
    end_q(2)

    got(ld.at[pl.ds(0, 15)], ld_s)
    got(qd.at[pl.ds(0, 3)], qa_s)
    got(qd.at[pl.ds(0, 12)], qb_s)
    got(kv.at[0, pl.ds(0, 3)], kz_s)
    got(kv.at[0], kd_s)
    got(pq.at[pl.ds(0, 6)], rb_s)
    got(sa.at[pl.ds(0, 6)], ra_s)
    got(rd, rd_s)
    got(rz, rz_s)


def put(*refs):
    sem = refs[6]
    copies = [pltpu.make_async_copy(refs[n], refs[3 + n], sem.at[n]) for n in range(3)]
    for c in copies:
        c.start()
    for c in copies:
        c.wait()


def local(q, k, v, o, dout, lse):
    flat = (ROWS, HD)
    vm = pl.BlockSpec(memory_space=pltpu.VMEM)
    V, DMA = pltpu.VMEM, pltpu.SemaphoreType.DMA
    scratch = [
        V((NQ, 2, ROWS, HD), BF16), V((2, 4, 2, ROWS, HD), BF16), V((NQ, 8, 128), F32),
        V((NQ, ROWS, HD), BF16), V((2, BQ, BK), F32),
        V((NC, 2 * HD, BK), BF16), V((NC, 2 * HD, BK), BF16), V((2, HD, BQ), BF16), V((2, HD, BQ), BF16),
        *[V((BQ, BK), BF16)] * 6,
        V((2, HD, BQ), F32), V((NC, HD, BK), F32), V((NC, HD, BK), F32),
        V((NG, NQ, GR, HD), F32), V((NG, 3, 4, GR, HD), F32), V((NG, 4, GR, HD), F32), V((NG, 3, GR, HD), F32),
        V((NG, 2, 4, 2, GR, HD), F32), V((NG, 4, 2, GR, HD), F32), V((NG, 4, 2, GR, HD), F32),
        V((NG, 3, 2, GR, HD), F32), V((ROWS, HD), BF16), V((1, ROWS), F32),
        DMA((N4,)), *[DMA] * 9,
        DMA, DMA, DMA((NG,)), DMA((N4,)), DMA, DMA((NG,)), DMA((NG,)), DMA((KQ,)), DMA((KQ,)), *[DMA((NG,))] * 6,
    ]
    outs = pl.pallas_call(
        kernel,
        out_shape=[pltpu.VMEM(flat, BF16)] * 3,
        in_specs=[pl.BlockSpec(memory_space=pl.ANY)] * 6, out_specs=[vm] * 3,
        scratch_shapes=scratch,
        compiler_params=pltpu.CompilerParams(collective_id=0, has_side_effects=True, vmem_limit_bytes=62 << 20),
    )(*[t.reshape(flat) for t in (q, k, v, o, dout)], lse)
    outs = pl.pallas_call(
        put,
        out_shape=[jax.ShapeDtypeStruct(flat, BF16)] * 3,
        in_specs=[vm] * 3, out_specs=[pl.BlockSpec(memory_space=pl.ANY)] * 3,
        scratch_shapes=[DMA((3,))],
    )(*[pltpu.with_memory_space_constraint(t, pltpu.VMEM) for t in outs])
    return tuple(t.reshape(ROWS, 1, HD) for t in outs)


def solution(mesh):
    rows = P(('data', 'cp'))
    cols = P(None, ('data', 'cp'))
    return jax.shard_map(local, mesh=mesh, in_specs=(rows, rows, rows, rows, rows, cols),
                         out_specs=(rows, rows, rows), check_vma=False)
```

```python
import functools
import math

import jax
import jax.numpy as jnp
from jax import lax
from jax.experimental import pallas as pl
from jax.experimental.pallas import tpu as pltpu
from jax.sharding import PartitionSpec as P

F32, BF16 = jnp.float32, jnp.bfloat16
MESH = pl.DeviceIdType.MESH
ROWS, HD = 512, 128
L = 32
NC = ROWS // L
NG, GR = 8, 64
NQ, NK = 16, 8
BQ, BK = NQ * L, NK * L
KQ, KR = 4, 128
N4 = 4
TERMS = 24
D3, SIDES = (1, 2, 3), (0, 1)
SCALE = HD ** -0.5
LOG2E = math.log2(math.e)
SEQ = (7, 6, 0, 5, 1, 4, 3, 2)
END = 9
TAKE_K = (1, 2, 3)
PASS_K = (1, 2)
PASS_Q = (9, 10, 11, 19, 31, 32)
NEXT_Q = (2, 3, 9, 11, 12)
START_A = (1, 2, 3, 10)
MID_K = (11, 31, 51, 61)
RELAY_Q = (19, 40, 49, 51, 59)
MID_Q = (40, 59, 60, 61)


def dg(a, b, ca, cb):
    return lax.dot_general(a, b, (((ca,), (cb,)), ((), ())), preferred_element_type=F32)


def kernel(q_hbm, k_hbm, v_hbm, o_hbm, do_hbm, lse_hbm, dq_ref, dk_ref, dv_ref,
           qd, kv, ld, ex, thr, kt, vt, qt, dot, p_a, p_b, p_c, ds_a, ds_b, ds_c, dqt, dkt, dvt,
           pq, rb, sa, ra, pk, rd, sz, rz, o_in, lse_in,
           in_s, ld_s, qa_s, qb_s, kz_s, kd_s, rb_s, ra_s, rd_s, rz_s,
           lda_r, ldb_r, qa_r, q7a_r, q7_r, qn_r, qf_r, kz_r, kd_r, rb_r, rf_r, ra_r, rd_r, rz_r, rzf_r):
    me = lax.axis_index('cp')
    core = lax.rem(me, 2)
    x = lax.rem(lax.div(me, 2), 4)
    y = lax.rem(lax.div(me, 8), 4)
    z = lax.div(me, 32)
    a = x + core * (y - x)
    b = y + core * (x - y)
    step_a, step_b = 2 + 6 * core, 8 - 6 * core

    def dev_q(b_, a_):
        return z * 32 + b_ * step_b + a_ * step_a + core

    def dev_k(z_, c_):
        return z_ * 32 + y * 8 + x * 2 + c_

    def turn(i, d):
        return lax.rem(i + d, N4)

    def remote(src, dst, ss, rs, dev):
        return pltpu.make_async_remote_copy(src_ref=src, dst_ref=dst, send_sem=ss, recv_sem=rs,
                                            device_id={'cp': dev}, device_id_type=MESH)

    def side(i, n):
        return turn(i, 1 + 2 * n)

    def half(n, size=2):
        return pl.ds(2 * n, size)

    def row(b_, n=0, size=N4):
        return pl.ds(b_ * N4 + n, size)

    slot = b * N4 + a

    def rows_g(g):
        return pl.ds(pl.multiple_of(g * GR, GR), GR)

    def got(ref, sem):
        pltpu.make_async_copy(ref, ref, sem).wait()

    def own_a(src, ss, rs, d):
        return remote(src, src, ss, rs, dev_q(b, turn(a, d)))

    def to_b(src, ss, rs, d):
        return remote(src, src, ss, rs, dev_q(turn(b, d), a))

    def q_blk(n, g):
        return qd.at[b * N4 + turn(a, n), :, rows_g(g), :]

    def q_row(b_, g, n=0, size=N4):
        return qd.at[row(b_, n, size), :, rows_g(g), :]

    def q_n(g, n):
        return remote(q_row(b, g), q_row(b, g), qb_s, qn_r.at[g], dev_q(side(b, n), a))

    def q_f(g, n):
        r = q_row(side(b, 1 - n), g, 2 * n, 2)
        return remote(r, r, qb_s, qf_r.at[g], dev_q(side(b, n), a))

    def rows_p(j):
        return pl.ds(pl.multiple_of(j * KR, KR), KR)

    def k_z(j, d):
        r = kv.at[core, z, :, rows_p(j), :]
        return remote(r, r, kz_s, kz_r.at[j], dev_k(turn(z, d), core))

    def k_d(j, d=0):
        r = kv.at[core, turn(z, N4 - d), :, rows_p(j), :]
        return remote(r, r, kd_s, kd_r.at[j], dev_k(z, 1 - core))

    def r_b(g, d):
        return remote(pq.at[g, row(turn(b, d))], rb.at[g, d - 1], rb_s, rb_r.at[g], dev_q(turn(b, d), a))

    def r_opp(g, n):
        return remote(pq.at[g, row(turn(b, 2), 2 * n, 2)], rb.at[g, 2, half(n)], rb_s, rb_r.at[g], dev_q(side(b, n), a))

    def r_near(g, n):
        return remote(pq.at[g, row(side(b, n), 2 - 2 * n, 2)], rb.at[g, n, half(1 - n)], rb_s, rf_r.at[g],
                      dev_q(side(b, n), a))

    def r_on(g, n):
        return remote(rb.at[g, 2, half(n)], rb.at[g, n, half(n)], rb_s, rf_r.at[g], dev_q(side(b, n), a))

    def r_a(g, d):
        return remote(sa.at[g, turn(a, d)], ra.at[g, d - 1], ra_s, ra_r.at[g], dev_q(b, turn(a, d)))

    def r_d(g):
        return remote(pk.at[g, 1 - core], rd.at[g], rd_s, rd_r.at[g], dev_k(z, 1 - core))

    def r_z(g, d):
        return remote(sz.at[g, turn(z, d)], rz.at[g, d - 1], rz_s, rz_r.at[g], dev_k(turn(z, d), core))

    def k_opp(g, n):
        return remote(sz.at[g, turn(z, 2), n], rz.at[g, 2, n], rz_s, rz_r.at[g], dev_k(side(z, n), core))

    def k_near(g, n):
        return remote(sz.at[g, side(z, n), 1 - n], rz.at[g, n, 1 - n], rz_s, rzf_r.at[g], dev_k(side(z, n), core))

    def k_on(g, n):
        return remote(rz.at[g, 2, n], rz.at[g, n, n], rz_s, rzf_r.at[g], dev_k(side(z, n), core))

    def start(copy, g, which=D3):
        for n in which:
            copy(g, n).start()

    barrier = pltpu.get_barrier_semaphore()
    peers = [dev_q(b, turn(a, d)) for d in D3] + [dev_q(turn(b, d), a) for d in D3]
    peers += [dev_k(turn(z, d), core) for d in D3] + [dev_k(z, 1 - core)]
    for p in peers:
        pl.semaphore_signal(barrier, inc=1, device_id={'cp': p}, device_id_type=MESH)
    ins = [(do_hbm, qd.at[slot, 1], 0), (q_hbm, qd.at[slot, 0], 0), (k_hbm, kv.at[core, z, 0], 1),
           (v_hbm, kv.at[core, z, 1], 1), (o_hbm, o_in, 2), (lse_hbm, lse_in, 3)]
    for src, dst, n in ins:
        pltpu.make_async_copy(src, dst, in_s.at[n]).start()
    for ref, n in ((qd.at[slot], 0), (kv.at[core, z], 1), (o_in, 2), (lse_in, 3)):
        got(ref, in_s.at[n])

    with jax.named_scope('own_ld'):
        for j in range(N4):
            rows_j = rows_p(j)
            d_j = jnp.sum(qd[slot, 1, rows_j, :].astype(F32) * o_in[rows_j, :].astype(F32), axis=1, keepdims=True)
            ld[slot, pl.ds(j, 1), :] = lse_in[:, rows_j] * (-1.0 / SCALE)
            ld[slot, pl.ds(N4 + j, 1), :] = -jnp.broadcast_to(d_j, (KR, KR)).T[:1]
    with jax.named_scope('barrier'):
        pl.semaphore_wait(barrier, len(peers))

    def start_a(g):
        for d in D3:
            own_a(q_blk(0, g), qa_s, qa_r.at[g], d).start()

    for d in D3:
        own_a(ld.at[slot], ld_s, lda_r, d).start()
    start(k_z, 0)
    for d in D3:
        own_a(q_blk(0, NG - 1), qa_s, q7a_r.at[a], d).start()
    k_d(0).start()
    for d in D3:
        to_b(ld.at[slot], ld_s, ldb_r, d).start()
    for d in D3:
        to_b(q_blk(0, NG - 1), qb_s, q7_r, d).start()


    def start_k(j, _):
        start(k_z, j)
        k_d(j).start()
        return 0
    lax.fori_loop(1, KQ, start_k, 0)
    qi = lax.broadcasted_iota(jnp.int32, (BQ, 1), 0)
    ki = lax.broadcasted_iota(jnp.int32, (1, BK), 1)
    qpos = (qi & (L - 1)) * 128 + dev_q(qi >> 7, (qi >> 5) & 3)
    kpos = (ki & (L - 1)) * 128 + dev_k((ki >> 5) & 3, ki >> 7)
    thr[0] = jnp.full((BQ, BK), jnp.inf, F32)
    thr[1] = jnp.where(kpos <= qpos, jnp.inf, -jnp.inf).astype(F32)
    ex[...] = jnp.zeros_like(ex)
    ri = lax.broadcasted_iota(jnp.int32, (HD, BK), 0)
    of_d = ((ri >> 2) & 1) == 1
    for c in range(NC):
        kt[c, HD:] = jnp.where((ri < TERMS) & ~of_d, 1.0, 0.0).astype(BF16)
        vt[c, HD:] = jnp.where((ri < TERMS) & of_d, 1.0, 0.0).astype(BF16)

    def got_a(g):
        got(q_row(0, g, 0, 3), qa_r.at[g])

    def prep_e(i, _):
        for n in range(N4):
            t = ld[N4 * i + n]
            hi = t.astype(BF16).astype(F32)
            mid = (t - hi).astype(BF16).astype(F32)
            terms = jnp.concatenate([hi, mid, t - hi - mid], axis=0).T
            quarter = lax.broadcasted_iota(jnp.int32, terms.shape, 1) & 3
            for j in range(N4):
                ex[N4 * i + n, rows_p(j), pl.ds(0, TERMS)] = jnp.where(quarter == j, terms, 0.0).astype(BF16)
        return 0

    def pass_k(j):
        with jax.named_scope('pass_k'):
            got(kv.at[0, pl.ds(0, 3), :, rows_p(0), :], kz_r.at[j])
        start(k_d, j)

    with jax.named_scope('w_lda'):
        got(ld.at[pl.ds(0, 3)], lda_r)
    for n in D3:
        for d in D3:
            to_b(ld.at[b * N4 + turn(a, n)], ld_s, ldb_r, d).start()
    for p in (0, 1, 3, 2):
        @pl.when(a != p)
        def _():
            r = qd.at[b * N4 + p, :, rows_g(NG - 1), :]
            with jax.named_scope('got_a7'):
                got(r, q7a_r.at[p])
            for d in D3:
                to_b(r, qb_s, q7_r, d).start()
    start_a(SEQ[1])
    start_a(SEQ[2])
    dkt[...] = jnp.zeros_like(dkt)
    dvt[...] = jnp.zeros_like(dvt)
    dqt[...] = jnp.zeros_like(dqt)
    with jax.named_scope('w_ldb'):
        got(ld.at[pl.ds(0, 12)], ldb_r)
    with jax.named_scope('prep_e'):
        lax.fori_loop(0, NQ // N4, prep_e, 0)
    pass_k(0)

    def rows_q(which, r):
        return qd[:, which, pl.ds(pl.multiple_of(r * L, L), L), :].reshape(BQ, HD)

    def rows_k(which, c):
        return kv[:, :, which, pl.ds(pl.multiple_of(c * L, L), L), :].reshape(BK, HD)

    def rows_e(r):
        return ex[:, pl.ds(pl.multiple_of(r * L, L), L), :].reshape(BQ, HD)

    def take_k(j):
        with jax.named_scope('take_k'):
            got(kv.at[0, :, :, rows_p(0), :], kd_r.at[j])
        with jax.named_scope('prep_k'):
            for n in range(KR // L):
                c = j * (KR // L) + n
                kt[c, :HD] = rows_k(0, c).T
                vt[c, :HD] = rows_k(1, c).T

    def a_mm(r, c):
        e = rows_e(r)
        return (dg(jnp.concatenate([rows_q(0, r), e], axis=1), kt[c], 1, 0),
                dg(jnp.concatenate([rows_q(1, r), e], axis=1), vt[c], 1, 0))

    def a_vpu(sdp, diag, p_s, ds_s):
        s, dp = sdp
        t = s * (SCALE * LOG2E)
        if diag is not None:
            t = jnp.minimum(t, thr[diag])
        p = jnp.exp2(t)
        p_s[...] = p.astype(BF16)
        ds_s[...] = (p * dp).astype(BF16)

    def b_mm(c, h, p_s, ds_s):
        p, ds = p_s[...], ds_s[...]
        dqt[h] += dg(kt[c, :HD], ds, 1, 1)
        return dg(dot[h], p, 1, 0), dg(qt[h], ds, 1, 0)

    def q_prep(r, h):
        qt[h] = rows_q(0, r).T
        dot[h] = rows_q(1, r).T

    def finish_q(g, h):
        pq[g, :, pl.ds(h * L, L), :] = dqt[h].T.reshape(NQ, L, HD)
        dqt[h] = jnp.zeros((HD, BQ), F32)

    def finish_k(g, h):
        r = 2 * g + h
        pk[g, :, :, 0, pl.ds(h * L, L), :] = dkt[r].T.reshape(2, N4, L, HD)
        pk[g, :, :, 1, pl.ds(h * L, L), :] = dvt[r].T.reshape(2, N4, L, HD)

    def one(c, r0, d0):
        sdp = a_mm(r0, c + 1)
        dv, dk = b_mm(c, 0, p_a, ds_a)
        a_vpu(sdp, d0, p_a, ds_a)
        sdp = a_mm(r0 + 1, c + 1)
        dv1, dk1 = b_mm(c, 1, p_b, ds_b)
        a_vpu(sdp, None, p_b, ds_b)
        dvt[c] += dv + dv1
        dkt[c] += dk + dk1

    def two(c, r0):
        one(c, r0, None)
        one(c + 1, r0, lax.div(c + 2, r0))

    def tail(g, nxt=None):
        r0, r1 = 2 * g, 2 * g + 1
        sdp = a_mm(r1, r1)
        dv, dk = b_mm(r0, 0, p_a, ds_a)
        a_vpu(sdp, 1, p_c, ds_c)
        dv1, dk1 = b_mm(r0, 1, p_b, ds_b)
        dvt[r0] += dv + dv1
        dkt[r0] += dk + dk1
        finish_q(g, 0)
        finish_k(g, 0)
        if nxt is not None:
            sdp = a_mm(2 * nxt, 0)
        dv, dk = b_mm(r1, 1, p_c, ds_c)
        if nxt is not None:
            a_vpu(sdp, lax.div(7 - nxt, 7), p_a, ds_a)
        dvt[r1] += dv
        dkt[r1] += dk
        if nxt is not None:
            sdp = a_mm(2 * nxt + 1, 0)
        finish_q(g, 1)
        finish_k(g, 1)
        if nxt is not None:
            a_vpu(sdp, None, p_b, ds_b)
            q_prep(2 * nxt, 0)
            q_prep(2 * nxt + 1, 1)

    def send_q(g):
        start(r_opp, g, SIDES)
        start(r_near, g, SIDES)

    def relay_q(g):
        with jax.named_scope('relay_q'):
            got(rb.at[g, 2], rb_r.at[g])
            for n in SIDES:
                rb[g, 2, half(n)] = rb[g, 2, half(n)] + pq[g, row(side(b, n), 2 * n, 2)]
        start(r_on, g, SIDES)

    def mid_q(g):
        with jax.named_scope('mid_q'):
            got(rb.at[g, half(0)], rf_r.at[g])
            sa[g] = pq[g, row(b)] + rb[g, 0] + rb[g, 1]
        start(r_a, g)

    def last_q(g):
        with jax.named_scope('last_q'):
            got(rb.at[g], rb_r.at[g])
            sa[g] = pq[g, row(b)] + rb[g, 0] + rb[g, 1] + rb[g, 2]
        start(r_a, g)

    def send_k(g):
        r_d(g).start()

    def sum_k(g):
        with jax.named_scope('sum_k'):
            got(rd.at[g], rd_r.at[g])
            sz[g] = pk[g, core] + rd[g]

    def mid_k(g):
        sum_k(g)
        start(r_z, g)

    def mid_k_by(g):
        sum_k(g)
        start(k_opp, g, SIDES)
        start(k_near, g, SIDES)

    def relay_k(g):
        with jax.named_scope('relay_k'):
            got(rz.at[g, 2], rz_r.at[g])
            for n in SIDES:
                rz[g, 2, n] = rz[g, 2, n] + sz[g, side(z, n), n]
        start(k_on, g, SIDES)

    def end_q(g):
        with jax.named_scope('end_q'):
            got(ra.at[g], ra_r.at[g])
            dq = sa[g, a] + ra[g, 0] + ra[g, 1] + ra[g, 2]
            dq_ref[rows_g(g), :] = (dq * SCALE).astype(BF16)

    def out_k(g, dkv):
        dk_ref[rows_g(g), :] = (dkv[0] * SCALE).astype(BF16)
        dv_ref[rows_g(g), :] = dkv[1].astype(BF16)

    def end_k(g):
        with jax.named_scope('end_k'):
            got(rz.at[g], rz_r.at[g])
            out_k(g, sz[g, z] + rz[g, 0] + rz[g, 1] + rz[g, 2])

    def end_k_by(g):
        with jax.named_scope('end_k_by'):
            got(rz.at[g, half(0)], rzf_r.at[g])
            out_k(g, sz[g, z] + rz[g, 0] + rz[g, 1])

    def pass_q(g):
        with jax.named_scope('pass_q'):
            got(q_row(0, g, 0, 2 * N4), qn_r.at[g])
        start(q_f, g, SIDES)

    def next_q(g):
        with jax.named_scope('next_q'):
            got_a(g)
        start(q_n, g, SIDES)

    take_k(0)
    got_a(SEQ[1])
    for d in D3:
        to_b(q_row(b, SEQ[1]), qb_s, qf_r.at[SEQ[1]], d).start()
    with jax.named_scope('first_q'):
        got(q_row(0, NG - 1, 0, 12), q7_r)
    pass_k(1)
    q_prep(NC - 2, 0)
    q_prep(NC - 1, 1)
    next_q(SEQ[2])
    start_a(SEQ[3])
    with jax.named_scope('first'):
        a_vpu(a_mm(NC - 2, 0), None, p_a, ds_a)
        a_vpu(a_mm(NC - 1, 0), None, p_b, ds_b)

    def group(i):
        return SEQ[0] + sum((SEQ[n] - SEQ[n - 1]) * lax.div(i + NG - n, NG) for n in range(1, NG))

    plan = {}
    for act, args, when in (
        (take_k, (1, 2, 3), TAKE_K),
        (pass_k, (2, 3), PASS_K),
        (pass_q, SEQ[2:], PASS_Q),
        (next_q, SEQ[3:], NEXT_Q),
        (start_a, SEQ[4:], START_A),
        (mid_k, (7, 6, 5, 4), MID_K),
        (relay_q, SEQ, RELAY_Q),
        (mid_q, SEQ, MID_Q),
    ):
        for arg, t in zip(args, when):
            plan.setdefault(t, []).append((act, arg))
    early = (pass_q, next_q, start_a, relay_q)

    def fire(i, j, acts):
        for n in range(NG - 1):
            places = {t % 10: e for t, e in plan.items() if t // 10 == n}
            places = {t: [e for e in es if acts is None or (e[0] in early) == acts] for t, es in places.items()}
            if j is END:
                places = {t: es for t, es in places.items() if t == END and es}
            else:
                places = {t: es for t, es in places.items() if t != END and es}
            if places:
                pl.when(i == n)(functools.partial(at, j, places))

    def at(j, places):
        for t, es in places.items():
            def run(es=es):
                for act, arg in es:
                    act(arg)
            if j is END:
                run()
            else:
                pl.when(j == t)(run)

    def superstep(i, _):
        g = group(i)
        g1 = group(i + 1)
        single = lax.rem(g, 2)

        def pair(j, _):
            fire(i, j, None)
            with jax.named_scope('two'):
                two(2 * j, 2 * g)
            return 0

        def four(j):
            c = 2 * single + N4 * j
            two(c, 2 * g)
            two(c + 2, 2 * g)

        def double(j, _):
            fire(i, j + single, None)
            with jax.named_scope('four'):
                four(j)
            return 0

        def last():
            with jax.named_scope('take_q'):
                pl.when(i == 0)(lambda: got(q_row(0, g1, 0, 12), qf_r.at[g1]))
                pl.when(i > 0)(lambda: got(q_row(0, g1), qf_r.at[g1]))

        fours = lax.div(g - single, 2)
        lax.fori_loop(0, single, pair, 0)
        lax.fori_loop(0, fours - 1, double, 0)

        @pl.when(fours > 0)
        def _():
            fire(i, fours - 1 + single, None)
            last()
            with jax.named_scope('fourtail'):
                four(fours - 1)
                tail(g, g1)

        @pl.when(fours == 0)
        def _():
            last()
            with jax.named_scope('tail'):
                tail(g, g1)
        fire(i, END, True)
        pl.when(i <= N4)(functools.partial(send_q, g))
        pl.when(i > N4)(functools.partial(start, r_b, g))
        pl.when((i != SEQ.index(0)) & (i != SEQ.index(1)))(functools.partial(send_k, g))
        fire(i, END, False)
        return 0
    lax.fori_loop(0, NG - 1, superstep, 0)

    def close(g):
        with jax.named_scope('two'):
            two(2 * g, N4)
        for h in SIDES:
            finish_k(g, h)
        send_k(g)

    close(0)
    mid_k_by(3)
    close(1)
    mid_q(1)
    mid_k_by(0)
    with jax.named_scope('tail'):
        tail(2)
    start(r_b, 2)
    send_k(2)
    mid_k_by(1)
    mid_k(2)
    relay_k(3)
    relay_k(1)
    relay_k(0)
    last_q(4)
    last_q(3)
    for g in (7, 6, 5):
        end_k(g)
        end_q(g)
    end_q(0)
    end_q(1)
    end_k(4)
    last_q(2)
    end_q(4)
    end_k_by(3)
    end_q(3)
    end_k_by(0)
    end_k(2)
    end_k_by(1)
    got(ld.at[pl.ds(0, 15)], ld_s)
    got(qd.at[pl.ds(0, 3)], qa_s)
    got(qd.at[pl.ds(0, 12)], qb_s)
    got(kv.at[0, pl.ds(0, 3)], kz_s)
    got(kv.at[0], kd_s)
    got(rd, rd_s)
    end_q(2)

    got(pq.at[pl.ds(0, 6)], rb_s)
    got(sa.at[pl.ds(0, 6)], ra_s)
    got(rz, rz_s)


def put(*refs):
    sem = refs[6]
    copies = [pltpu.make_async_copy(refs[n], refs[3 + n], sem.at[n]) for n in range(3)]
    for c in copies:
        c.start()
    for c in copies:
        c.wait()


def local(q, k, v, o, dout, lse):
    flat = (ROWS, HD)
    vm = pl.BlockSpec(memory_space=pltpu.VMEM)
    V, DMA = pltpu.VMEM, pltpu.SemaphoreType.DMA
    scratch = [
        V((NQ, 2, ROWS, HD), BF16), V((2, 4, 2, ROWS, HD), BF16), V((NQ, 8, 128), F32),
        V((NQ, ROWS, HD), BF16), V((2, BQ, BK), F32),
        V((NC, 2 * HD, BK), BF16), V((NC, 2 * HD, BK), BF16), V((2, HD, BQ), BF16), V((2, HD, BQ), BF16),
        *[V((BQ, BK), BF16)] * 6,
        V((2, HD, BQ), F32), V((NC, HD, BK), F32), V((NC, HD, BK), F32),
        V((NG, NQ, GR, HD), F32), V((NG, 3, 4, GR, HD), F32), V((NG, 4, GR, HD), F32), V((NG, 3, GR, HD), F32),
        V((NG, 2, 4, 2, GR, HD), F32), V((NG, 4, 2, GR, HD), F32), V((NG, 4, 2, GR, HD), F32),
        V((NG, 3, 2, GR, HD), F32), V((ROWS, HD), BF16), V((1, ROWS), F32),
        DMA((N4,)), *[DMA] * 9,
        DMA, DMA, DMA((NG,)), DMA((N4,)), DMA, DMA((NG,)), DMA((NG,)), DMA((KQ,)), DMA((KQ,)), *[DMA((NG,))] * 6,
    ]
    outs = pl.pallas_call(
        kernel,
        out_shape=[pltpu.VMEM(flat, BF16)] * 3,
        in_specs=[pl.BlockSpec(memory_space=pl.ANY)] * 6, out_specs=[vm] * 3,
        scratch_shapes=scratch,
        compiler_params=pltpu.CompilerParams(collective_id=0, has_side_effects=True, vmem_limit_bytes=62 << 20),
    )(*[t.reshape(flat) for t in (q, k, v, o, dout)], lse)
    outs = pl.pallas_call(
        put,
        out_shape=[jax.ShapeDtypeStruct(flat, BF16)] * 3,
        in_specs=[vm] * 3, out_specs=[pl.BlockSpec(memory_space=pl.ANY)] * 3,
        scratch_shapes=[DMA((3,))],
    )(*[pltpu.with_memory_space_constraint(t, pltpu.VMEM) for t in outs])
    return tuple(t.reshape(ROWS, 1, HD) for t in outs)


def solution(mesh):
    rows = P(('data', 'cp'))
    cols = P(None, ('data', 'cp'))
    return jax.shard_map(local, mesh=mesh, in_specs=(rows, rows, rows, rows, rows, cols),
                         out_specs=(rows, rows, rows), check_vma=False)
```
